16 devices in a mesh: tp: 2 (over z), dp: 8 (over y, x, core).
Axes of the slice: x: 2, y: 2, z: 2, core: 2. Of those that a mesh axis runs over, the one named last changes fastest.
Arguments:
- w_in: float32 [1, 1408, 10368], P(None, None, 'tp')
- w_out: float32 [1, 7552, 1408], P(None, 'tp')
- g_in: float32 [8, 1, 1408, 10368], P('dp', None, None, 'tp')
- g_out: float32 [8, 1, 7552, 1408], P('dp', None, 'tp')
- m_in: bfloat16 [1, 1408, 10368], P(None, 'dp', 'tp')
- m_out: bfloat16 [1, 7552, 1408], P(None, 'tp', 'dp')
- r_in: float32 [1, 1408], P(None, 'dp')
- c_in: float32 [1, 10368], P(None, 'tp')
- r_out: float32 [1, 7552], P(None, 'tp')
- c_out: float32 [1, 1408], P(None, 'dp')
- learn_rate: float32 [], replicated
- weight_decay: float32 [], replicated
- beta_two: float32 [], replicated
Outputs:
- output 1: float32 [1, 1408, 10368], P(None, None, 'tp')
- output 2: float32 [1, 7552, 1408], P(None, 'tp')
- output 3: bfloat16 [1, 1408, 10368], P(None, 'dp', 'tp')
- output 4: bfloat16 [1, 7552, 1408], P(None, 'tp', 'dp')
- output 5: float32 [1, 1408], P(None, 'dp')
- output 6: float32 [1, 10368], P(None, 'tp')
- output 7: float32 [1, 7552], P(None, 'tp')
- output 8: float32 [1, 1408], P(None, 'dp')
All inputs are finite; a program needn't handle non-finite values.
Results may differ from the reference program's by a relative error of at most 0.00125668.
Values sent between devices are 32-bit elements.
A program may use at most 1 GiB of HBM per device.

```python
import math
import jax
import jax.numpy as jnp

LAYERS = 1
D = 1408
MLP = 6144
DP = 8

FIN = MLP + 3 * D
FOUT = MLP + D


def axis_scales(key, count):
    key_ramp, key_noise = jax.random.split(key)
    ramp_slope = jax.random.uniform(key_ramp, (LAYERS, 1), jnp.float32, 0.6, 1.0)
    ramp_vals = jnp.linspace(-1.0, 1.0, count, dtype=jnp.float32)[None, :]
    noise_vals = jax.random.normal(key_noise, (LAYERS, count), jnp.float32)
    return jnp.exp(ramp_slope * ramp_vals + 0.3 * noise_vals)


def draw_matrix(key, n_rows, n_cols):
    key_list = jax.random.split(key, 7)
    row_scale = axis_scales(key_list[0], n_rows)
    col_scale = axis_scales(key_list[1], n_cols)
    noise_rep = jax.random.normal(key_list[2], (DP, LAYERS, n_rows, n_cols), jnp.float32)
    grad_rep = noise_rep * (row_scale[:, :, None] * col_scale[:, None, :] / math.sqrt(DP))
    grad_sum = jnp.sum(grad_rep, axis=0)
    grad_sq = grad_sum * grad_sum
    row_noise = jax.random.normal(key_list[3], (LAYERS, n_rows), jnp.float32)
    col_noise = jax.random.normal(key_list[4], (LAYERS, n_cols), jnp.float32)
    row_old = 0.25 * jnp.mean(grad_sq, axis=2) * jnp.exp(0.5 * row_noise)
    col_old = 0.25 * jnp.mean(grad_sq, axis=1) * jnp.exp(0.5 * col_noise)
    weight = jax.random.normal(key_list[5], (LAYERS, n_rows, n_cols), jnp.float32) * n_rows ** -0.5
    moment = (0.1 * jax.random.normal(key_list[6], (LAYERS, n_rows, n_cols), jnp.float32)).astype(jnp.bfloat16)
    return weight, grad_rep, moment, row_old, col_old


def setup_inputs(seed: int = 0) -> dict:
    key_list = jax.random.split(jax.random.key(seed), 5)
    w_in, g_in, m_in, r_in, c_in = draw_matrix(key_list[0], D, FIN)
    w_out, g_out, m_out, r_out, c_out = draw_matrix(key_list[1], FOUT, D)
    learn_rate = jax.random.uniform(key_list[2], (), jnp.float32, 0.25, 0.75) * D ** -0.5
    weight_decay = jax.random.uniform(key_list[3], (), jnp.float32, 0.15, 0.45) * D ** 0.5
    beta_two = jax.random.uniform(key_list[4], (), jnp.float32, 0.8, 0.9)
    return dict(w_in=w_in, w_out=w_out, g_in=g_in, g_out=g_out, m_in=m_in, m_out=m_out, r_in=r_in, c_in=c_in, r_out=r_out, c_out=c_out, learn_rate=learn_rate, weight_decay=weight_decay, beta_two=beta_two)


def adafactor_matrix(weight, grad_rep, moment, row_old, col_old, learn_rate, weight_decay, beta_two):
    grad_sum = jnp.sum(grad_rep, axis=0)
    grad_sq = grad_sum * grad_sum + 1e-30
    row_new = beta_two * row_old + (1.0 - beta_two) * jnp.mean(grad_sq, axis=2)
    col_new = beta_two * col_old + (1.0 - beta_two) * jnp.mean(grad_sq, axis=1)
    row_avg = jnp.mean(row_new, axis=1)
    second = row_new[:, :, None] * col_new[:, None, :] / row_avg[:, None, None]
    update = grad_sum / jnp.sqrt(second)
    rms_val = jnp.sqrt(jnp.mean(update * update, axis=(1, 2)))
    update = update / jnp.maximum(1.0, rms_val)[:, None, None]
    mom_new = (0.9 * moment.astype(jnp.float32) + 0.1 * update).astype(jnp.bfloat16)
    w_new = weight - learn_rate * mom_new.astype(jnp.float32) - learn_rate * weight_decay * weight
    return w_new, mom_new, row_new, col_new


def reference(w_in, w_out, g_in, g_out, m_in, m_out, r_in, c_in, r_out, c_out, learn_rate, weight_decay, beta_two):
    in_result = adafactor_matrix(w_in, g_in, m_in, r_in, c_in, learn_rate, weight_decay, beta_two)
    out_result = adafactor_matrix(w_out, g_out, m_out, r_out, c_out, learn_rate, weight_decay, beta_two)
    return (in_result[0], out_result[0], in_result[1], out_result[1], in_result[2], in_result[3], out_result[2], out_result[3])
```

```python
import jax
import jax.numpy as jnp
from jax import lax
from jax.experimental import pallas as pl
from jax.experimental.pallas import tpu as pltpu
from jax.sharding import PartitionSpec as P

F32 = jnp.float32
LANES = 128
SUB = 8
DP = 8
BF16 = jnp.bfloat16
MESH = pl.DeviceIdType.MESH
NCH = 8
ORDER = (0, 4, 1, 5, 2, 6, 3, 7)


def chunk_rows(rows):
    tiles = rows // 8
    out, start = [], 0
    for part in ((tiles + 1) // 2, tiles // 2):
        for i in range(4):
            n = part // 4 + (1 if i < part % 4 else 0)
            out.append((8 * start, 8 * n))
            start += n
    return out


def lane_chunks(total, width=1024):
    out, s = [], 0
    while s < total:
        n = total - s if total - s < 2 * width else width
        if n > width + 256:
            n = width
        out.append((s, n))
        s += n
    return out


class Mat:
    def __init__(self, kloc, width, tp, row_is_r):
        self.k, self.width, self.sh = kloc, width, width // 8
        self.r = kloc // 8
        self.ktot = kloc * tp
        self.row_is_r = row_is_r
        self.ch = chunk_rows(self.r)
        self.tiles = (kloc + 127) // LANES
        self.kr = (self.tiles + 7) // 8 * 8
        self.nmax = max(n for _, n in self.ch)


def rcopy(src, dst, ss, rs, dev):
    return pltpu.make_async_remote_copy(src_ref=src, dst_ref=dst, send_sem=ss, recv_sem=rs, device_id=dev, device_id_type=MESH)


def main_kernel(mats, sh, *refs):
    it = iter(refs)
    lr_ref, wd_ref, b2_ref = next(it), next(it), next(it)
    for m in mats:
        m.g, m.w, m.mom, m.row_old, m.col_old = (next(it) for _ in range(5))
    for m in mats:
        (m.ag, m.mom_new, m.row_new, m.col_new, m.d2d, m.xy1, m.x2, m.y2) = (next(it) for _ in range(8))
    stage, wst, usq, ucol = next(it), next(it), next(it), next(it)
    ld_sem, w_sem = next(it), next(it)
    for m in mats:
        (m.p, m.gt, m.gn, m.mv, m.colacc, m.msg, m.slots, m.rp, m.rz, m.sc, m.slots2) = (next(it) for _ in range(11))
        (m.d2d_s, m.rs1_s, m.x2_s, m.y2_s, m.ex_s, m.msg_s, m.z_s, m.sc_s, m.agx_s, m.agy_s, m.agd_s, m.ags_s, m.loc_s) = (next(it) for _ in range(13))
    tp = lax.axis_index('tp')
    dp = lax.axis_index('dp')
    c = lax.rem(dp, 2)
    chip = lax.div(dp, 2)
    x = lax.rem(chip, 2)
    y = lax.div(chip, 2)
    jx, jy, jd = chip + 1 - 2 * x, chip + 2 - 4 * y, 3 - chip
    qx, qy, qd, qs = 2 * jx + c, 2 * jy + c, 2 * jd + c, dp + 1 - 2 * c
    sib, xn, yn = {'tp': tp, 'dp': qs}, {'tp': tp, 'dp': qx}, {'tp': tp, 'dp': qy}
    zn = {'tp': 1 - tp, 'dp': dp}
    me16 = tp * 8 + dp

    sends = []

    def start(cp):
        cp.start()
        sends.append(cp)

    def d2d_copy(m, i):
        r0, n = m.ch[i]
        return rcopy(m.g.at[pl.ds(4 * (1 - c), 4), pl.ds(r0, n), :], m.d2d.at[:, pl.ds(r0, n), :], m.d2d_s.at[0, i], m.d2d_s.at[1, i], sib)

    def load_pair(m, i, b):
        r0, n = m.ch[i]
        own = pltpu.make_async_copy(m.g.at[pl.ds(4 * c, 4), pl.ds(r0, n), :], stage.at[b, 0, :, pl.ds(0, n), :], ld_sem.at[b, 0])
        got = pltpu.make_async_copy(m.d2d.at[:, pl.ds(r0, n), :], stage.at[b, 1, :, pl.ds(0, n), :], ld_sem.at[b, 1])
        return own, got

    def start_loads(m, i, b):
        own, got = load_pair(m, i, b)
        own.start()
        d2d_copy(m, i).wait_recv()
        got.start()

    def pack_chunk(m, i, b):
        r0, n = m.ch[i]
        own, got = load_pair(m, i, b)
        own.wait()
        got.wait()

        def body(t, carry):
            rs = pl.multiple_of(t * SUB, SUB)
            rd = pl.multiple_of(r0 + t * SUB, SUB)
            xs = [stage[b, 0, k, pl.ds(rs, SUB), :] + stage[b, 1, k, pl.ds(rs, SUB), :] for k in range(4)]
            for j in range(4):
                parts = [xs[k][:, sh * (2 * j + cc):sh * (2 * j + cc + 1)] for cc in range(2) for k in range(4)]
                m.p[j, pl.ds(rd, SUB), :] = jnp.concatenate(parts, axis=1)
            return carry

        lax.fori_loop(0, n // SUB, body, 0)

    def pview(m, j, i):
        r0, n = m.ch[i]
        return m.p.at[j, pl.ds(r0, n), :]

    def hview(ref, m, i):
        r0, n = m.ch[i]
        return ref.at[pl.ds(r0, n), :]

    def rs1_copy(m, i):
        dev = xn if i < 4 else yn
        return rcopy(pview(m, jd, i), hview(m.xy1, m, i), m.rs1_s.at[0, i], m.rs1_s.at[1, i], dev)

    def x2_copy(m, i):
        return rcopy(pview(m, jx, i), hview(m.x2, m, i), m.x2_s.at[0, i], m.x2_s.at[1, i], xn)

    def y2_copy(m, i):
        return rcopy(pview(m, jy, i), hview(m.y2, m, i), m.y2_s.at[0, i], m.y2_s.at[1, i], yn)

    def rs_pack(m, send):
        for s, i in enumerate(ORDER):
            if s == 0:
                start_loads(m, i, 0)
            elif s > 1:
                pass
            if s > 0 and s + 1 < NCH:
                start_loads(m, ORDER[s + 1], (s + 1) % 2)
            pack_chunk(m, i, s % 2)
            if s == 0:
                start_loads(m, ORDER[1], 1)
            if send:
                start(rs1_copy(m, i))

    def rs_free(m, i):
        start(x2_copy(m, i) if i < 4 else y2_copy(m, i))

    def rs_dep(m, ids):
        def load(s):
            i = ids[s]
            r0, n = m.ch[i]
            return pltpu.make_async_copy(hview(m.xy1, m, i), stage.at[s % 2, 0, 0, pl.ds(0, n), :], ld_sem.at[s % 2, 0])

        for s, i in enumerate(ids):
            r0, n = m.ch[i]
            rs1_copy(m, i).wait_recv()
            load(s).start()
            load(s).wait()
            j = jy if i < 4 else jx

            def body(t, carry):
                rs = pl.multiple_of(t * SUB, SUB)
                rd = pl.multiple_of(r0 + t * SUB, SUB)
                m.p[j, pl.ds(rd, SUB), :] = m.p[j, pl.ds(rd, SUB), :] + stage[s % 2, 0, 0, pl.ds(rs, SUB), :]
                return carry

            lax.fori_loop(0, n // SUB, body, 0)
            start(y2_copy(m, i) if i < 4 else x2_copy(m, i))

    def acc_own(m, ids):
        base = (2 * c * (4 * m.r), (2 - c) * (4 * m.r))

        def loads(s):
            i = ids[s]
            r0, n = m.ch[i]
            b = s % 2
            return (pltpu.make_async_copy(hview(m.x2, m, i), stage.at[b, 0, 0, pl.ds(0, n), :], ld_sem.at[b, 0]),
                    pltpu.make_async_copy(hview(m.y2, m, i), stage.at[b, 0, 1, pl.ds(0, n), :], ld_sem.at[b, 1]))

        for s, i in enumerate(ids):
            r0, n = m.ch[i]
            b = s % 2
            x2_copy(m, i).wait_recv()
            y2_copy(m, i).wait_recv()
            la, lb = loads(s)
            la.start()
            lb.start()
            la.wait()
            lb.wait()

            def body(t, carry):
                rs = pl.multiple_of(t * SUB, SUB)
                rd = pl.multiple_of(r0 + t * SUB, SUB)
                v = m.p[chip, pl.ds(rd, SUB), :] + stage[b, 0, 0, pl.ds(rs, SUB), :] + stage[b, 0, 1, pl.ds(rs, SUB), :]
                for cc in range(2):
                    for k in range(4):
                        row = pl.multiple_of(base[cc] + k * m.r + r0 + t * SUB, SUB)
                        m.gt[pl.ds(row, SUB), 0:sh] = v[:, sh * (4 * cc + k):sh * (4 * cc + k + 1)]
                return carry

            lax.fori_loop(0, n // SUB, body, 0)

    def ex_copy(m):
        h = 4 * m.r
        return rcopy(m.gt.at[pl.ds(2 * h, h), :], m.gt.at[pl.ds(c * h, h), :], m.ex_s.at[0], m.ex_s.at[1], sib)

    def ex_wait(m):
        h = 4 * m.r
        rcopy(m.gt.at[pl.ds(2 * h, h), :], m.gt.at[pl.ds((1 - c) * h, h), :], m.ex_s.at[0], m.ex_s.at[1], sib).wait_recv()

    def to_gn(m):
        full = m.k // LANES

        def body(t, carry):
            o = pl.multiple_of(t * LANES, LANES)
            m.gn[:, pl.ds(o, LANES)] = m.gt[pl.ds(o, LANES), :].T[0:sh, :]
            return carry

        lax.fori_loop(0, full, body, 0)
        rest = m.k - full * LANES
        if rest:
            m.gn[:, full * LANES:m.k] = m.gt[full * LANES:full * LANES + LANES, :].T[0:sh, 0:rest]

    def from_gn(m):
        full = m.k // LANES
        pad = m.gt.shape[1] - sh

        def turn(v):
            return jnp.concatenate([v, jnp.zeros((pad, LANES), F32)], axis=0).T

        def body(t, carry):
            o = pl.multiple_of(t * LANES, LANES)
            m.gt[pl.ds(o, LANES), :] = turn(m.gn[:, pl.ds(o, LANES)])
            return carry

        lax.fori_loop(0, full, body, 0)
        rest = m.k - full * LANES
        if rest:
            v = jnp.concatenate([m.gn[:, full * LANES:m.k], jnp.zeros((sh, LANES - rest), F32)], axis=1)
            m.gt[full * LANES:m.k, :] = turn(v)[0:rest, :]

    def peers():
        out = []
        for d in range(1, 8):
            q = lax.rem(dp + d, 8)
            out.append((True, tp, q))
        for d in range(8):
            q = lax.rem(dp + d, 8)
            out.append((False, 1 - tp, q))
        return out

    def msg_copies(m, sending):
        out = []
        for n, (same, t, q) in enumerate(peers()):
            slot = me16 if sending else t * SUB + q
            dev = {'tp': t, 'dp': q}
            rsem = m.msg_s.at[1, slot]
            if same:
                out.append(rcopy(m.msg, m.slots.at[slot], m.msg_s.at[0, n], rsem, dev))
            else:
                out.append(rcopy(m.msg.at[pl.ds(m.kr, SUB), :], m.slots.at[slot, pl.ds(m.kr, SUB), :], m.msg_s.at[0, n], rsem, dev))
        return out

    def z_copy(m):
        return rcopy(m.rp, m.rz, m.z_s.at[0], m.z_s.at[1], zn)

    def sc_copies(m, sending):
        out = []
        for n, (same, t, q) in enumerate(peers()):
            slot = me16 if sending else t * SUB + q
            out.append(rcopy(m.sc, m.slots2.at[slot], m.sc_s.at[0, n], m.sc_s.at[1, slot], {'tp': t, 'dp': q}))
        return out

    def stats1(m):
        b2 = b2_ref[0, 0]
        m.colacc[...] = jnp.zeros_like(m.colacc)

        def body(t, carry):
            rr = pl.multiple_of(t * SUB, SUB)
            rsum = jnp.zeros((8, 1), F32)
            for s0, w in lane_chunks(m.k):
                g = m.gn[pl.ds(rr, SUB), s0:s0 + w]
                sq = g * g + 1e-30
                m.colacc[:, s0:s0 + w] = m.colacc[:, s0:s0 + w] + sq
                rsum = rsum + jnp.sum(sq, axis=1, keepdims=True)
            m.rp[pl.ds(rr, SUB), :] = jnp.broadcast_to(rsum, (SUB, LANES))
            return carry

        lax.fori_loop(0, sh // SUB, body, 0)
        for i in range(m.tiles):
            w = min(LANES, m.k - LANES * i)
            m.msg[i:i + 1, 0:w] = jnp.sum(m.colacc[:, LANES * i:LANES * i + w], axis=0, keepdims=True)
        mean_s = jnp.sum(m.rp[...] * (1.0 / m.ktot), axis=0, keepdims=True) * (1.0 / m.width)
        if m.row_is_r:
            old = jnp.sum(m.row_old[...], axis=0, keepdims=True) * (0.5 / m.width)
        else:
            old = jnp.sum(jnp.sum(m.col_old[...], axis=0, keepdims=True), axis=1, keepdims=True) * (0.125 / m.ktot)
        m.msg[m.kr:m.kr + SUB, :] = jnp.broadcast_to(b2 * old + (1.0 - b2) * mean_s, (SUB, LANES))
        m.slots[me16, :, :] = m.msg[...]
        for cp in msg_copies(m, True):
            start(cp)
        start(z_copy(m))

    def stats2(m):
        b2 = b2_ref[0, 0]
        for cp in msg_copies(m, False):
            cp.wait_recv()
        z_copy(m).wait_recv()
        tot = m.slots[tp * 8, 0:m.kr, :]
        for q in range(1, 8):
            tot = tot + m.slots[tp * 8 + q, 0:m.kr, :]
        m.col_new[...] = b2 * m.col_old[...] + (1.0 - b2) * (tot / float(m.width))
        m.row_new[...] = b2 * m.row_old[...] + (1.0 - b2) * ((m.rp[...] + m.rz[...]) / float(m.ktot))
        mean_r = m.slots[0, m.kr:m.kr + SUB, :]
        for q in range(1, 16):
            mean_r = mean_r + m.slots[q, m.kr:m.kr + SUB, :]
        mean_r = mean_r[:, 0:1]
        usq[...] = jnp.zeros_like(usq)
        ucol[...] = jnp.zeros_like(ucol)

        def body(t, carry):
            rr = pl.multiple_of(t * SUB, SUB)
            rv = m.row_new[pl.ds(rr, SUB), 0:1]
            acc = jnp.zeros((8, 1), F32)
            for i in range(m.tiles):
                s0, w = LANES * i, min(LANES, m.k - LANES * i)
                second = rv * m.col_new[i:i + 1, 0:w] / mean_r
                u = m.gn[pl.ds(rr, SUB), s0:s0 + w] / jnp.sqrt(second)
                m.gn[pl.ds(rr, SUB), s0:s0 + w] = u
                if w == LANES:
                    usq[...] = usq[...] + u * u
                else:
                    acc = acc + jnp.sum(u * u, axis=1, keepdims=True)
            ucol[...] = ucol[...] + jnp.broadcast_to(acc, (SUB, LANES))
            return carry

        lax.fori_loop(0, sh // SUB, body, 0)
        usum = jnp.sum(jnp.sum(usq[...], axis=1, keepdims=True), axis=0, keepdims=True)
        usum = usum + jnp.sum(ucol[:, 0:1], axis=0, keepdims=True)
        m.sc[...] = jnp.broadcast_to(usum, (SUB, LANES))
        m.slots2[me16, :, :] = m.sc[...]
        for cp in sc_copies(m, True):
            start(cp)

    def stats3(m):
        for cp in sc_copies(m, False):
            cp.wait_recv()
        tot = m.slots2[0, :, :]
        for q in range(1, 16):
            tot = tot + m.slots2[q, :, :]
        den = jnp.maximum(1.0, jnp.sqrt(tot / (float(m.width) * float(m.ktot))))[0:1, 0:1]
        mom_load(m).wait()

        def body(t, carry):
            rr = pl.multiple_of(t * 16, 16)
            for s0, w in lane_chunks(m.k):
                u = m.gn[pl.ds(rr, 16), s0:s0 + w] / den
                mn = (0.9 * m.mv[pl.ds(rr, 16), s0:s0 + w].astype(F32) + 0.1 * u).astype(BF16)
                m.mv[pl.ds(rr, 16), s0:s0 + w] = mn
                m.gn[pl.ds(rr, 16), s0:s0 + w] = mn.astype(F32)
            return carry

        lax.fori_loop(0, sh // 16, body, 0)
        mom_store(m).start()
        from_gn(m)

    def mom_load(m):
        return pltpu.make_async_copy(m.mom, m.mv, m.loc_s.at[0])

    def mom_store(m):
        return pltpu.make_async_copy(m.mv, m.mom_new, m.loc_s.at[1])

    def own_copy(m):
        return pltpu.make_async_copy(m.p.at[chip], m.ag.at[dp], m.loc_s.at[2])

    lane0 = jnp.minimum(lax.div(sh * dp, LANES), 8)
    off = sh * dp - lane0 * LANES

    def w_load(m, i, b):
        r0, n = m.ch[i]
        return pltpu.make_async_copy(m.w.at[:, pl.ds(r0, n), pl.ds(pl.multiple_of(lane0 * LANES, LANES), 384)], wst.at[b, :, pl.ds(0, n), :], w_sem.at[b])

    def new_weights(m):
        lr, wd = lr_ref[0, 0], wd_ref[0, 0]
        w_load(m, 0, 0).start()
        for i in range(NCH):
            r0, n = m.ch[i]
            b = i % 2
            if i + 1 < NCH:
                w_load(m, i + 1, 1 - b).start()
            w_load(m, i, b).wait()

            def body(t, carry):
                rs = pl.multiple_of(t * SUB, SUB)
                rd = pl.multiple_of(r0 + t * SUB, SUB)
                parts = []
                for k in range(8):
                    w = pltpu.roll(wst[b, k, pl.ds(rs, SUB), :], lax.rem(384 - off, 384), 1)[:, 0:sh]
                    mt = m.gt[pl.ds(pl.multiple_of(k * m.r + r0 + t * SUB, SUB), 8), 0:sh]
                    parts.append(w - lr * mt - lr * wd * w)
                m.p[chip, pl.ds(rd, SUB), :] = jnp.concatenate(parts, axis=1)
                return carry

            lax.fori_loop(0, n // SUB, body, 0)

    def agrow(m, q, i):
        r0, n = m.ch[i]
        return m.ag.at[q, pl.ds(r0, n), :]

    def ag_own(m, i):
        start(rcopy(pview(m, chip, i), agrow(m, dp, i), m.agx_s.at[0, i], m.agx_s.at[1, i], xn))
        start(rcopy(pview(m, chip, i), agrow(m, dp, i), m.agy_s.at[0, i], m.agy_s.at[1, i], yn))

    def ag_sib_own(m, i):
        start(rcopy(pview(m, chip, i), agrow(m, dp, i), m.ags_s.at[0, 0, i], m.ags_s.at[1, 0, i], sib))

    def ag_sib(m, which, q, i):
        start(rcopy(agrow(m, q, i), agrow(m, q, i), m.ags_s.at[0, which, i], m.ags_s.at[1, which, i], sib))

    def ag_xy(m, i):
        rcopy(agrow(m, qx, i), agrow(m, qx, i), m.agx_s.at[0, i], m.agx_s.at[1, i], xn).wait_recv()
        rcopy(agrow(m, qy, i), agrow(m, qy, i), m.agy_s.at[0, i], m.agy_s.at[1, i], yn).wait_recv()
        if i < 4:
            start(rcopy(agrow(m, qx, i), agrow(m, qx, i), m.agd_s.at[0, i], m.agd_s.at[1, i], yn))
        else:
            start(rcopy(agrow(m, qy, i), agrow(m, qy, i), m.agd_s.at[0, i], m.agd_s.at[1, i], xn))
        ag_sib(m, 1, qx, i)
        ag_sib(m, 2, qy, i)

    def ag_d(m, i):
        rcopy(agrow(m, qd, i), agrow(m, qd, i), m.agd_s.at[0, i], m.agd_s.at[1, i], xn).wait_recv()
        ag_sib(m, 3, qd, i)

    def ag_end(m):
        for which, q in enumerate((qs, qx + 1 - 2 * c, qy + 1 - 2 * c, qd + 1 - 2 * c)):
            for i in range(NCH):
                rcopy(agrow(m, q, i), agrow(m, q, i), m.ags_s.at[0, which, i], m.ags_s.at[1, which, i], sib).wait_recv()

    a, o = mats
    for m in mats:
        for i in ORDER:
            start(d2d_copy(m, i))
    rs_pack(a, True)
    for i in ORDER:
        rs_free(a, i)
    for m in mats:
        mom_load(m).start()
    rs_dep(a, ORDER)
    rs_pack(o, False)
    start(rs1_copy(o, 0))
    start(rs1_copy(o, 4))
    acc_own(a, ORDER)
    start(ex_copy(a))
    ex_wait(a)
    to_gn(a)
    stats1(a)
    for i in (1, 5, 2, 6):
        start(rs1_copy(o, i))
    stats2(a)
    for i in (3, 7):
        start(rs1_copy(o, i))
    for i in (0, 4):
        rs_free(o, i)
    stats3(a)
    for i in (1, 5, 2, 6, 3, 7):
        rs_free(o, i)
    new_weights(a)
    own_copy(a).start()
    rs_dep(o, ORDER)
    for i in range(2):
        ag_own(a, i)
    for i in range(NCH):
        ag_sib_own(a, i)
    acc_own(o, ORDER)
    start(ex_copy(o))
    ex_wait(o)
    to_gn(o)
    stats1(o)
    for i in range(2, 4):
        ag_own(a, i)
    stats2(o)
    for i in range(4, 6):
        ag_own(a, i)
    stats3(o)
    for i in range(6, 8):
        ag_own(a, i)
    new_weights(o)
    own_copy(o).start()
    for i in range(NCH):
        ag_sib_own(o, i)
    for i in range(NCH):
        ag_xy(a, i)
    for i in range(NCH):
        ag_own(o, i)
    for i in range(NCH):
        ag_d(a, i)
    for i in range(NCH):
        ag_xy(o, i)
    for i in range(NCH):
        ag_d(o, i)
    for m in mats:
        ag_end(m)
        own_copy(m).wait()
        mom_store(m).wait()
    for cp in sends:
        cp.wait_send()


def split_rows(rows, parts):
    tiles = rows // 8
    out, start = [], 0
    for i in range(parts):
        n = tiles // parts + (1 if i < tiles % parts else 0)
        out.append((8 * start, 8 * n))
        start += n
    return out


def unpack_kernel(sh, work, *refs):
    n_mats = 2
    srcs, dsts = refs[0:n_mats], refs[n_mats:2 * n_mats]
    src_v, dst_v, in_sem, out_sem = refs[2 * n_mats:]

    def load(s):
        m, r0, n = work[s]
        return pltpu.make_async_copy(srcs[m].at[:, pl.ds(r0, n), :], src_v.at[s % 2, :, pl.ds(0, n), :], in_sem.at[s % 2])

    def store(s):
        m, r0, n = work[s]
        return pltpu.make_async_copy(dst_v.at[s % 2, :, pl.ds(0, n), :], dsts[m].at[:, pl.ds(r0, n), :], out_sem.at[s % 2])

    load(0).start()
    for s, (m, r0, n) in enumerate(work):
        b = s % 2
        if s + 1 < len(work):
            load(s + 1).start()
        load(s).wait()
        if s >= 2:
            store(s - 2).wait()

        def body(t, carry):
            r = pl.multiple_of(t * SUB, SUB)
            xs = [src_v[b, q, pl.ds(r, SUB), :] for q in range(8)]
            for k in range(8):
                dst_v[b, k, pl.ds(r, SUB), :] = jnp.concatenate([xs[q][:, sh * k:sh * (k + 1)] for q in range(8)], axis=1)
            return carry

        lax.fori_loop(0, n // SUB, body, 0)
        store(s).start()
    for s in range(max(0, len(work) - 2), len(work)):
        store(s).wait()


def unpack(packed, sh):
    work = [(m, r0, n) for m, v in enumerate(packed) for r0, n in split_rows(v.shape[1], 14 if m == 0 else 10)]
    nmax = max(n for _, _, n in work)
    width = packed[0].shape[2]
    anyspec = pl.BlockSpec(memory_space=pl.ANY)
    return pl.pallas_call(
        lambda *refs: unpack_kernel(sh, work, *refs),
        in_specs=[anyspec] * 2,
        out_specs=[anyspec] * 2,
        out_shape=[jax.ShapeDtypeStruct(v.shape, F32) for v in packed],
        scratch_shapes=[pltpu.VMEM((2, 8, nmax, width), F32), pltpu.VMEM((2, 8, nmax, width), F32), pltpu.SemaphoreType.DMA((2,)), pltpu.SemaphoreType.DMA((2,))],
        compiler_params=pltpu.CompilerParams(vmem_limit_bytes=60000000),
        name='unpack',
    )(*packed)


def solution(mesh):
    tp_devs = mesh.shape['tp']

    def body(w_in, w_out, g_in, g_out, m_in, m_out, r_in, c_in, r_out, c_out, learn_rate, weight_decay, beta_two):
        width = w_in.shape[1]
        sh = width // 8
        mats = (Mat(w_in.shape[2], width, tp_devs, True), Mat(w_out.shape[1], width, tp_devs, False))
        a, o = mats

        def grouped(v, m):
            return v.reshape(8, m.r, width)

        def column(v):
            return jnp.broadcast_to(v.reshape(sh, 1), (sh, LANES))

        def row_tiles(v, m):
            return jnp.pad(v, ((0, 0), (0, LANES * m.kr - m.k))).reshape(m.kr, LANES)

        def flat(v, m):
            return v.reshape(1, LANES * m.kr)[:, 0:m.k]

        scal = [v.reshape(1, 1) for v in (learn_rate, weight_decay, beta_two)]
        args = list(scal)
        args += [grouped(g_in[0, 0].T, a), grouped(w_in[0].T, a), m_in[0], column(r_in), row_tiles(c_in, a)]
        args += [grouped(g_out[0, 0], o), grouped(w_out[0], o), m_out[0].T, column(c_out), row_tiles(r_out, o)]
        anyspec = pl.BlockSpec(memory_space=pl.ANY)
        vspec = pl.BlockSpec(memory_space=pltpu.VMEM)
        sspec = pl.BlockSpec(memory_space=pltpu.SMEM)
        in_specs = [sspec] * 3 + [anyspec, anyspec, anyspec, vspec, vspec] * 2
        out_shape, out_specs = [], []
        for m in mats:
            big = jax.ShapeDtypeStruct((m.r, width), F32)
            out_shape += [jax.ShapeDtypeStruct((8, m.r, width), F32), jax.ShapeDtypeStruct((sh, m.k), BF16),
                          jax.ShapeDtypeStruct((sh, LANES), F32), jax.ShapeDtypeStruct((m.kr, LANES), F32),
                          jax.ShapeDtypeStruct((4, m.r, width), F32), big, big, big]
            out_specs += [anyspec, anyspec, vspec, vspec, anyspec, anyspec, anyspec, anyspec]
        nmax = max(m.nmax for m in mats)
        dma = pltpu.SemaphoreType.DMA
        scratch = [pltpu.VMEM((2, 2, 4, nmax, width), F32), pltpu.VMEM((2, 8, nmax, 384), F32), pltpu.VMEM((SUB, LANES), F32), pltpu.VMEM((SUB, LANES), F32), dma((2, 2)), dma((2,))]
        for m in mats:
            gt_rows = 12 * m.r
            scratch += [pltpu.VMEM((4, m.r, width), F32), pltpu.VMEM((gt_rows, 256), F32), pltpu.VMEM((sh, LANES * m.tiles), F32),
                        pltpu.VMEM((sh, m.k), BF16), pltpu.VMEM((SUB, LANES * m.tiles), F32), pltpu.VMEM((m.kr + SUB, LANES), F32),
                        pltpu.VMEM((16, m.kr + SUB, LANES), F32), pltpu.VMEM((sh, LANES), F32), pltpu.VMEM((sh, LANES), F32),
                        pltpu.VMEM((SUB, LANES), F32), pltpu.VMEM((16, 8, LANES), F32)]
            scratch += [dma((2, NCH)), dma((2, NCH)), dma((2, NCH)), dma((2, NCH)), dma((2,)), dma((2, 16)), dma((2,)), dma((2, 16)),
                        dma((2, NCH)), dma((2, NCH)), dma((2, NCH)), dma((2, 4, NCH)), dma((3,))]
        outs = pl.pallas_call(
            lambda *refs: main_kernel(mats, sh, *refs),
            in_specs=in_specs,
            out_specs=out_specs,
            out_shape=out_shape,
            scratch_shapes=scratch,
            compiler_params=pltpu.CompilerParams(has_side_effects=True, vmem_limit_bytes=67043328),
            name='step',
        )(*args)
        ag_in, mom_in, row_in, col_in = outs[0:4]
        ag_out, mom_out, row_out, col_out = outs[8:12]
        flat_in, flat_out = unpack((ag_in, ag_out), sh)
        new_in = flat_in.reshape(a.k, width).T[None]
        new_out = flat_out.reshape(o.k, width)[None]
        return (new_in, new_out, mom_in[None], mom_out.T[None], row_in[:, 0][None], flat(col_in, a), flat(col_out, o), row_out[:, 0][None])

    free = None
    rows_tp, cols_tp = P(free, 'tp', free), P(free, free, 'tp')
    on_dp, on_tp, whole = P(free, 'dp'), P(free, 'tp'), P()
    state_in, state_out = P(free, 'dp', 'tp'), P(free, 'tp', 'dp')
    in_specs = (cols_tp, rows_tp, P('dp', free, free, 'tp'), P('dp', free, 'tp', free), state_in, state_out, on_dp, on_tp, on_tp, on_dp, whole, whole, whole)
    out_specs = (cols_tp, rows_tp, state_in, state_out, on_dp, on_tp, on_tp, on_dp)
    return jax.shard_map(body, mesh=mesh, in_specs=in_specs, out_specs=out_specs, check_vma=False)
```

```python
import jax
import jax.numpy as jnp
from jax import lax
from jax.experimental import pallas as pl
from jax.experimental.pallas import tpu as pltpu
from jax.sharding import PartitionSpec as P

F32 = jnp.float32
LANES = 128
SUB = 8
DP = 8
BF16 = jnp.bfloat16
MESH = pl.DeviceIdType.MESH
NCH = 8
ORDER = (0, 4, 1, 5, 2, 6, 3, 7)


def chunk_rows(rows):
    tiles = rows // SUB
    out, start = [], 0
    for part in ((tiles + 1) // 2, tiles // 2):
        sizes = [part // 9, part * 3 // 10, part * 7 // 20]
        for n in sizes + [part - sum(sizes)]:
            out.append((SUB * start, SUB * n))
            start += n
    return out


def lane_chunks(total, width=1024):
    out, s = [], 0
    while s < total:
        n = total - s if total - s < 2 * width else width
        if n > width + 256:
            n = width
        out.append((s, n))
        s += n
    return out


class Mat:
    def __init__(self, kloc, width, tp, row_is_r):
        self.k, self.width, self.sh = kloc, width, width // 8
        self.r = kloc // 8
        self.ktot = kloc * tp
        self.row_is_r = row_is_r
        self.ch = chunk_rows(self.r)
        self.tiles = (kloc + 127) // LANES
        self.kr = (self.tiles + 7) // 8 * 8
        self.nmax = max(n for _, n in self.ch)


def rcopy(src, dst, ss, rs, dev):
    return pltpu.make_async_remote_copy(src_ref=src, dst_ref=dst, send_sem=ss, recv_sem=rs, device_id=dev, device_id_type=MESH)


def main_kernel(mats, sh, *refs):
    it = iter(refs)
    lr_ref, wd_ref, b2_ref = next(it), next(it), next(it)
    for m in mats:
        m.g, m.w, m.mom, m.row_arg, m.col_arg = (next(it) for _ in range(5))
    for m in mats:
        (m.ag, m.mom_new, m.row_out, m.col_out, m.d2d, m.xy1, m.x2, m.y2) = (next(it) for _ in range(DP))
    stage, wst, usq, ucol = next(it), next(it), next(it), next(it)
    ld_sem, w_sem = next(it), next(it)
    for m in mats:
        (m.p, m.gt, m.gn, m.mv, m.colacc, m.msg, m.slots, m.rp, m.rz, m.sc, m.slots2, m.row_raw, m.col_raw, m.row_old, m.row_new, m.col_old, m.col_new) = (next(it) for _ in range(17))
        (m.d2d_s, m.rs1_s, m.x2_s, m.y2_s, m.ex_s, m.msg_s, m.z_s, m.sc_s, m.agx_s, m.agy_s, m.agd_s, m.ags_s, m.loc_s) = (next(it) for _ in range(13))
    tp = lax.axis_index('tp')
    dp = lax.axis_index('dp')
    c = lax.rem(dp, 2)
    chip = lax.div(dp, 2)
    x = lax.rem(chip, 2)
    y = lax.div(chip, 2)
    jx, jy, jd = chip + 1 - 2 * x, chip + 2 - 4 * y, 3 - chip
    qx, qy, qd, qs = 2 * jx + c, 2 * jy + c, 2 * jd + c, dp + 1 - 2 * c
    sib, xn, yn = {'tp': tp, 'dp': qs}, {'tp': tp, 'dp': qx}, {'tp': tp, 'dp': qy}
    zn = {'tp': 1 - tp, 'dp': dp}
    me16 = tp * 8 + dp

    sends = []

    def start(cp):
        cp.start()
        sends.append(cp)

    def d2d_copy(m, i):
        r0, n = m.ch[i]
        return rcopy(m.g.at[pl.ds(4 * (1 - c), 4), pl.ds(r0, n), :], m.d2d.at[:, pl.ds(r0, n), :], m.d2d_s.at[0, i], m.d2d_s.at[1, i], sib)

    def load_pair(m, i, b):
        r0, n = m.ch[i]
        own = pltpu.make_async_copy(m.g.at[pl.ds(4 * c, 4), pl.ds(r0, n), :], stage.at[b, 0, :, pl.ds(0, n), :], ld_sem.at[b, 0])
        got = pltpu.make_async_copy(m.d2d.at[:, pl.ds(r0, n), :], stage.at[b, 1, :, pl.ds(0, n), :], ld_sem.at[b, 1])
        return own, got

    def start_loads(m, i, b):
        own, got = load_pair(m, i, b)
        own.start()
        d2d_copy(m, i).wait_recv()
        got.start()

    def pack_chunk(m, i, b):
        r0, n = m.ch[i]
        own, got = load_pair(m, i, b)
        own.wait()
        got.wait()

        def body(t, carry):
            rs = pl.multiple_of(t * SUB, SUB)
            rd = pl.multiple_of(r0 + t * SUB, SUB)
            xs = [stage[b, 0, k, pl.ds(rs, SUB), :] + stage[b, 1, k, pl.ds(rs, SUB), :] for k in range(4)]
            for j in range(4):
                parts = [xs[k][:, sh * (2 * j + cc):sh * (2 * j + cc + 1)] for cc in range(2) for k in range(4)]
                m.p[j, pl.ds(rd, SUB), :] = jnp.concatenate(parts, axis=1)
            return carry

        lax.fori_loop(0, n // SUB, body, 0)

    def pview(m, j, i):
        r0, n = m.ch[i]
        return m.p.at[j, pl.ds(r0, n), :]

    def hview(ref, m, i):
        r0, n = m.ch[i]
        return ref.at[pl.ds(r0, n), :]

    def rs1_copy(m, i):
        dev = xn if i < 4 else yn
        return rcopy(pview(m, jd, i), hview(m.xy1, m, i), m.rs1_s.at[0, i], m.rs1_s.at[1, i], dev)

    def x2_copy(m, i):
        return rcopy(pview(m, jx, i), hview(m.x2, m, i), m.x2_s.at[0, i], m.x2_s.at[1, i], xn)

    def y2_copy(m, i):
        return rcopy(pview(m, jy, i), hview(m.y2, m, i), m.y2_s.at[0, i], m.y2_s.at[1, i], yn)

    def rs_pack(m, send):
        for s, i in enumerate(ORDER):
            if s == 0:
                start_loads(m, i, 0)
            elif s > 1:
                pass
            if s > 0 and s + 1 < NCH:
                start_loads(m, ORDER[s + 1], (s + 1) % 2)
            pack_chunk(m, i, s % 2)
            if s == 0:
                start_loads(m, ORDER[1], 1)
            if send:
                start(rs1_copy(m, i))

    def rs_free(m, i):
        start(x2_copy(m, i) if i < 4 else y2_copy(m, i))

    def rs_dep(m, ids):
        def load(s):
            i = ids[s]
            r0, n = m.ch[i]
            return pltpu.make_async_copy(hview(m.xy1, m, i), stage.at[s % 2, 0, 0, pl.ds(0, n), :], ld_sem.at[s % 2, 0])

        for s, i in enumerate(ids):
            r0, n = m.ch[i]
            rs1_copy(m, i).wait_recv()
            load(s).start()
            load(s).wait()
            j = jy if i < 4 else jx

            def body(t, carry):
                rs = pl.multiple_of(t * SUB, SUB)
                rd = pl.multiple_of(r0 + t * SUB, SUB)
                m.p[j, pl.ds(rd, SUB), :] = m.p[j, pl.ds(rd, SUB), :] + stage[s % 2, 0, 0, pl.ds(rs, SUB), :]
                return carry

            lax.fori_loop(0, n // SUB, body, 0)
            start(y2_copy(m, i) if i < 4 else x2_copy(m, i))

    def acc_own(m, ids):
        base = (2 * c * (4 * m.r), (2 - c) * (4 * m.r))

        def loads(s):
            i = ids[s]
            r0, n = m.ch[i]
            b = s % 2
            return (pltpu.make_async_copy(hview(m.x2, m, i), stage.at[b, 0, 0, pl.ds(0, n), :], ld_sem.at[b, 0]),
                    pltpu.make_async_copy(hview(m.y2, m, i), stage.at[b, 0, 1, pl.ds(0, n), :], ld_sem.at[b, 1]))

        for s, i in enumerate(ids):
            r0, n = m.ch[i]
            b = s % 2
            x2_copy(m, i).wait_recv()
            y2_copy(m, i).wait_recv()
            la, lb = loads(s)
            la.start()
            lb.start()
            la.wait()
            lb.wait()

            def body(t, carry):
                rs = pl.multiple_of(t * SUB, SUB)
                rd = pl.multiple_of(r0 + t * SUB, SUB)
                v = m.p[chip, pl.ds(rd, SUB), :] + stage[b, 0, 0, pl.ds(rs, SUB), :] + stage[b, 0, 1, pl.ds(rs, SUB), :]
                for cc in range(2):
                    for k in range(4):
                        row = pl.multiple_of(base[cc] + k * m.r + r0 + t * SUB, SUB)
                        m.gt[pl.ds(row, SUB), 0:sh] = v[:, sh * (4 * cc + k):sh * (4 * cc + k + 1)]
                return carry

            lax.fori_loop(0, n // SUB, body, 0)

    def ex_copy(m):
        h = 4 * m.r
        return rcopy(m.gt.at[pl.ds(2 * h, h), :], m.gt.at[pl.ds(c * h, h), :], m.ex_s.at[0], m.ex_s.at[1], sib)

    def ex_wait(m):
        h = 4 * m.r
        rcopy(m.gt.at[pl.ds(2 * h, h), :], m.gt.at[pl.ds((1 - c) * h, h), :], m.ex_s.at[0], m.ex_s.at[1], sib).wait_recv()

    def to_gn(m):
        full = m.k // LANES

        def body(t, carry):
            o = pl.multiple_of(t * LANES, LANES)
            m.gn[:, pl.ds(o, LANES)] = m.gt[pl.ds(o, LANES), :].T[0:sh, :]
            return carry

        lax.fori_loop(0, full, body, 0)
        rest = m.k - full * LANES
        if rest:
            m.gn[:, full * LANES:m.k] = m.gt[full * LANES:full * LANES + LANES, :].T[0:sh, 0:rest]

    def from_gn(m):
        full = m.k // LANES
        pad = m.gt.shape[1] - sh

        def turn(v):
            return jnp.concatenate([v, jnp.zeros((pad, LANES), F32)], axis=0).T

        def body(t, carry):
            o = pl.multiple_of(t * LANES, LANES)
            m.gt[pl.ds(o, LANES), :] = turn(m.gn[:, pl.ds(o, LANES)])
            return carry

        lax.fori_loop(0, full, body, 0)
        rest = m.k - full * LANES
        if rest:
            v = jnp.concatenate([m.gn[:, full * LANES:m.k], jnp.zeros((sh, LANES - rest), F32)], axis=1)
            m.gt[full * LANES:m.k, :] = turn(v)[0:rest, :]

    def vec_loads(m):
        return (pltpu.make_async_copy(m.row_arg, m.row_raw.at[pl.ds(0, 1), :], m.loc_s.at[3]),
                pltpu.make_async_copy(m.col_arg, m.col_raw.at[pl.ds(0, 1), :], m.loc_s.at[4]))

    def vec_stores(m):
        return (pltpu.make_async_copy(m.row_raw.at[pl.ds(0, 1), :], m.row_out, m.loc_s.at[3]),
                pltpu.make_async_copy(m.col_raw.at[pl.ds(0, 1), :], m.col_out, m.loc_s.at[4]))

    def vec_prepare(m):
        for cp in vec_loads(m):
            cp.wait()
        pad = m.gt.shape[1] - sh
        row = jnp.concatenate([m.row_raw[0:1, :], jnp.zeros((1, pad), F32)], axis=1)
        m.row_old[...] = jnp.broadcast_to(row, (LANES, sh + pad)).T[0:sh, :]
        m.col_old[...] = jnp.zeros_like(m.col_old)
        for t in range(m.tiles):
            w = min(LANES, m.k - LANES * t)
            m.col_old[t:t + 1, 0:w] = m.col_raw[0:1, LANES * t:LANES * t + w]

    def vec_finish(m):
        pad = m.gt.shape[1] - sh
        m.row_raw[...] = jnp.concatenate([m.row_new[...], jnp.zeros((pad, LANES), F32)], axis=0).T[0:SUB, 0:sh]
        for t in range(m.tiles):
            w = min(LANES, m.k - LANES * t)
            m.col_raw[0:1, LANES * t:LANES * t + w] = m.col_new[t:t + 1, 0:w]
        for cp in vec_stores(m):
            cp.start()

    def peers():
        out = []
        for d in range(1, 8):
            q = lax.rem(dp + d, 8)
            out.append((True, tp, q))
        for d in range(8):
            q = lax.rem(dp + d, 8)
            out.append((False, 1 - tp, q))
        return out

    def msg_copies(m, sending):
        out = []
        for n, (same, t, q) in enumerate(peers()):
            slot = me16 if sending else t * SUB + q
            dev = {'tp': t, 'dp': q}
            rsem = m.msg_s.at[1, slot]
            if same:
                out.append(rcopy(m.msg, m.slots.at[slot], m.msg_s.at[0, n], rsem, dev))
            else:
                out.append(rcopy(m.msg.at[pl.ds(m.kr, SUB), :], m.slots.at[slot, pl.ds(m.kr, SUB), :], m.msg_s.at[0, n], rsem, dev))
        return out

    def z_copy(m):
        return rcopy(m.rp, m.rz, m.z_s.at[0], m.z_s.at[1], zn)

    def sc_copies(m, sending):
        out = []
        for n, (same, t, q) in enumerate(peers()):
            slot = me16 if sending else t * SUB + q
            out.append(rcopy(m.sc, m.slots2.at[slot], m.sc_s.at[0, n], m.sc_s.at[1, slot], {'tp': t, 'dp': q}))
        return out

    def stats1(m):
        b2 = b2_ref[0, 0]
        m.colacc[...] = jnp.zeros_like(m.colacc)

        def body(t, carry):
            rr = pl.multiple_of(t * SUB, SUB)
            rsum = jnp.zeros((8, 1), F32)
            for s0, w in lane_chunks(m.k):
                g = m.gn[pl.ds(rr, SUB), s0:s0 + w]
                sq = g * g + 1e-30
                m.colacc[:, s0:s0 + w] = m.colacc[:, s0:s0 + w] + sq
                rsum = rsum + jnp.sum(sq, axis=1, keepdims=True)
            m.rp[pl.ds(rr, SUB), :] = jnp.broadcast_to(rsum, (SUB, LANES))
            return carry

        lax.fori_loop(0, sh // SUB, body, 0)
        for i in range(m.tiles):
            w = min(LANES, m.k - LANES * i)
            m.msg[i:i + 1, 0:w] = jnp.sum(m.colacc[:, LANES * i:LANES * i + w], axis=0, keepdims=True)
        mean_s = jnp.sum(m.rp[...] * (1.0 / m.ktot), axis=0, keepdims=True) * (1.0 / m.width)
        if m.row_is_r:
            old = jnp.sum(m.row_old[...], axis=0, keepdims=True) * (0.5 / m.width)
        else:
            old = jnp.sum(jnp.sum(m.col_old[...], axis=0, keepdims=True), axis=1, keepdims=True) * (0.125 / m.ktot)
        m.msg[m.kr:m.kr + SUB, :] = jnp.broadcast_to(b2 * old + (1.0 - b2) * mean_s, (SUB, LANES))
        m.slots[me16, :, :] = m.msg[...]
        for cp in msg_copies(m, True):
            start(cp)
        start(z_copy(m))

    def stats2(m):
        b2 = b2_ref[0, 0]
        for cp in msg_copies(m, False):
            cp.wait_recv()
        z_copy(m).wait_recv()
        tot = m.slots[tp * 8, 0:m.kr, :]
        for q in range(1, 8):
            tot = tot + m.slots[tp * 8 + q, 0:m.kr, :]
        m.col_new[...] = b2 * m.col_old[...] + (1.0 - b2) * (tot / float(m.width))
        m.row_new[...] = b2 * m.row_old[...] + (1.0 - b2) * ((m.rp[...] + m.rz[...]) / float(m.ktot))
        mean_r = m.slots[0, m.kr:m.kr + SUB, :]
        for q in range(1, 16):
            mean_r = mean_r + m.slots[q, m.kr:m.kr + SUB, :]
        mean_r = mean_r[:, 0:1]
        usq[...] = jnp.zeros_like(usq)
        ucol[...] = jnp.zeros_like(ucol)

        def body(t, carry):
            rr = pl.multiple_of(t * SUB, SUB)
            rv = m.row_new[pl.ds(rr, SUB), 0:1]
            acc = jnp.zeros((8, 1), F32)
            for i in range(m.tiles):
                s0, w = LANES * i, min(LANES, m.k - LANES * i)
                second = rv * m.col_new[i:i + 1, 0:w] / mean_r
                u = m.gn[pl.ds(rr, SUB), s0:s0 + w] / jnp.sqrt(second)
                m.gn[pl.ds(rr, SUB), s0:s0 + w] = u
                if w == LANES:
                    usq[...] = usq[...] + u * u
                else:
                    acc = acc + jnp.sum(u * u, axis=1, keepdims=True)
            ucol[...] = ucol[...] + jnp.broadcast_to(acc, (SUB, LANES))
            return carry

        lax.fori_loop(0, sh // SUB, body, 0)
        usum = jnp.sum(jnp.sum(usq[...], axis=1, keepdims=True), axis=0, keepdims=True)
        usum = usum + jnp.sum(ucol[:, 0:1], axis=0, keepdims=True)
        m.sc[...] = jnp.broadcast_to(usum, (SUB, LANES))
        m.slots2[me16, :, :] = m.sc[...]
        for cp in sc_copies(m, True):
            start(cp)

    def stats3(m):
        for cp in sc_copies(m, False):
            cp.wait_recv()
        tot = m.slots2[0, :, :]
        for q in range(1, 16):
            tot = tot + m.slots2[q, :, :]
        den = jnp.maximum(1.0, jnp.sqrt(tot / (float(m.width) * float(m.ktot))))[0:1, 0:1]
        mom_load(m).wait()

        def body(t, carry):
            rr = pl.multiple_of(t * 16, 16)
            for s0, w in lane_chunks(m.k):
                u = m.gn[pl.ds(rr, 16), s0:s0 + w] / den
                mn = (0.9 * m.mv[pl.ds(rr, 16), s0:s0 + w].astype(F32) + 0.1 * u).astype(BF16)
                m.mv[pl.ds(rr, 16), s0:s0 + w] = mn
                m.gn[pl.ds(rr, 16), s0:s0 + w] = mn.astype(F32)
            return carry

        lax.fori_loop(0, sh // 16, body, 0)
        mom_store(m).start()
        from_gn(m)

    def mom_load(m):
        return pltpu.make_async_copy(m.mom, m.mv, m.loc_s.at[0])

    def mom_store(m):
        return pltpu.make_async_copy(m.mv, m.mom_new, m.loc_s.at[1])

    def own_copy(m):
        return pltpu.make_async_copy(m.p.at[chip], m.ag.at[dp], m.loc_s.at[2])

    lane0 = jnp.minimum(lax.div(sh * dp, LANES), 8)
    off = sh * dp - lane0 * LANES

    def w_load(m, i, b):
        r0, n = m.ch[i]
        return pltpu.make_async_copy(m.w.at[:, pl.ds(r0, n), pl.ds(pl.multiple_of(lane0 * LANES, LANES), 384)], wst.at[b, :, pl.ds(0, n), :], w_sem.at[b])

    def new_weights(m):
        lr, wd = lr_ref[0, 0], wd_ref[0, 0]
        w_load(m, 0, 0).start()
        for i in range(NCH):
            r0, n = m.ch[i]
            b = i % 2
            if i + 1 < NCH:
                w_load(m, i + 1, 1 - b).start()
            w_load(m, i, b).wait()

            def body(t, carry):
                rs = pl.multiple_of(t * SUB, SUB)
                rd = pl.multiple_of(r0 + t * SUB, SUB)
                parts = []
                for k in range(8):
                    w = pltpu.roll(wst[b, k, pl.ds(rs, SUB), :], lax.rem(384 - off, 384), 1)[:, 0:sh]
                    mt = m.gt[pl.ds(pl.multiple_of(k * m.r + r0 + t * SUB, SUB), 8), 0:sh]
                    parts.append(w - lr * mt - lr * wd * w)
                m.p[chip, pl.ds(rd, SUB), :] = jnp.concatenate(parts, axis=1)
                return carry

            lax.fori_loop(0, n // SUB, body, 0)

    def agrow(m, q, i):
        r0, n = m.ch[i]
        return m.ag.at[q, pl.ds(r0, n), :]

    def ag_own(m, i):
        start(rcopy(pview(m, chip, i), agrow(m, dp, i), m.agx_s.at[0, i], m.agx_s.at[1, i], xn))
        start(rcopy(pview(m, chip, i), agrow(m, dp, i), m.agy_s.at[0, i], m.agy_s.at[1, i], yn))

    def ag_sib_own(m, i):
        start(rcopy(pview(m, chip, i), agrow(m, dp, i), m.ags_s.at[0, 0, i], m.ags_s.at[1, 0, i], sib))

    def ag_sib(m, which, q, i):
        start(rcopy(agrow(m, q, i), agrow(m, q, i), m.ags_s.at[0, which, i], m.ags_s.at[1, which, i], sib))

    def ag_xy(m, i):
        rcopy(agrow(m, qx, i), agrow(m, qx, i), m.agx_s.at[0, i], m.agx_s.at[1, i], xn).wait_recv()
        rcopy(agrow(m, qy, i), agrow(m, qy, i), m.agy_s.at[0, i], m.agy_s.at[1, i], yn).wait_recv()
        if i < 4:
            start(rcopy(agrow(m, qx, i), agrow(m, qx, i), m.agd_s.at[0, i], m.agd_s.at[1, i], yn))
        else:
            start(rcopy(agrow(m, qy, i), agrow(m, qy, i), m.agd_s.at[0, i], m.agd_s.at[1, i], xn))
        ag_sib(m, 1, qx, i)
        ag_sib(m, 2, qy, i)

    def ag_d(m, i):
        rcopy(agrow(m, qd, i), agrow(m, qd, i), m.agd_s.at[0, i], m.agd_s.at[1, i], xn).wait_recv()
        ag_sib(m, 3, qd, i)

    def ag_end(m):
        for which, q in enumerate((qs, qx + 1 - 2 * c, qy + 1 - 2 * c, qd + 1 - 2 * c)):
            for i in range(NCH):
                rcopy(agrow(m, q, i), agrow(m, q, i), m.ags_s.at[0, which, i], m.ags_s.at[1, which, i], sib).wait_recv()

    a, o = mats
    for m in mats:
        for i in ORDER:
            start(d2d_copy(m, i))
    rs_pack(a, True)
    for i in ORDER:
        rs_free(a, i)
    for m in mats:
        mom_load(m).start()
        for cp in vec_loads(m):
            cp.start()
    rs_dep(a, ORDER)
    rs_pack(o, False)
    for m in mats:
        vec_prepare(m)
    for i in ORDER[0:4]:
        start(rs1_copy(o, i))
    acc_own(a, ORDER)
    start(ex_copy(a))
    ex_wait(a)
    to_gn(a)
    stats1(a)
    for i in ORDER[4:6]:
        start(rs1_copy(o, i))
    stats2(a)
    for i in ORDER[6:]:
        start(rs1_copy(o, i))
    for i in ORDER[0:2]:
        rs_free(o, i)
    stats3(a)
    for i in ORDER[2:]:
        rs_free(o, i)
    new_weights(a)
    vec_finish(a)
    own_copy(a).start()
    rs_dep(o, ORDER)
    for i in range(2):
        ag_own(a, i)
    for i in range(NCH):
        ag_sib_own(a, i)
    acc_own(o, ORDER)
    start(ex_copy(o))
    ex_wait(o)
    to_gn(o)
    stats1(o)
    for i in range(2, 4):
        ag_own(a, i)
    stats2(o)
    for i in range(4, 6):
        ag_own(a, i)
    stats3(o)
    for i in range(6, 8):
        ag_own(a, i)
    new_weights(o)
    vec_finish(o)
    own_copy(o).start()
    for i in range(NCH):
        ag_sib_own(o, i)
    for i in range(NCH):
        ag_xy(a, i)
    for i in range(NCH):
        ag_own(o, i)
    for i in range(NCH):
        ag_d(a, i)
    for i in range(NCH):
        ag_xy(o, i)
    for i in range(NCH):
        ag_d(o, i)
    for m in mats:
        ag_end(m)
        own_copy(m).wait()
        mom_store(m).wait()
        for cp in vec_stores(m):
            cp.wait()
    for cp in sends:
        cp.wait_send()


def split_rows(rows, parts):
    tiles = rows // 8
    out, start = [], 0
    for i in range(parts):
        n = tiles // parts + (1 if i < tiles % parts else 0)
        out.append((8 * start, 8 * n))
        start += n
    return out


def unpack_kernel(sh, work, n_small, *refs):
    it = iter(refs)

    def take(n):
        return [next(it) for _ in range(n)]

    srcs, small = take(2), take(n_small)
    dsts, small_out = take(2), take(n_small)
    src_v, dst_v, in_sem, out_sem, small_sem = take(5)
    small_v = take(n_small)
    ins, outs = src_v.shape[0], dst_v.shape[0]

    def load(s):
        m, r0, n = work[s]
        return pltpu.make_async_copy(srcs[m].at[:, pl.ds(r0, n), :], src_v.at[s % ins, :, pl.ds(0, n), :], in_sem.at[s % ins])

    def store(s):
        m, r0, n = work[s]
        return pltpu.make_async_copy(dst_v.at[s % outs, :, pl.ds(0, n), :], dsts[m].at[:, pl.ds(r0, n), :], out_sem.at[s % outs])

    def small_in(k):
        return pltpu.make_async_copy(small[k], small_v[k], small_sem.at[0, k])

    def small_back(k):
        return pltpu.make_async_copy(small_v[k], small_out[k], small_sem.at[1, k])

    for s in range(ins - 1):
        load(s).start()
    for k in range(n_small):
        small_in(k).start()
    for s, (m, r0, n) in enumerate(work):
        bi, bo = s % ins, s % outs
        if s + ins - 1 < len(work):
            load(s + ins - 1).start()
        load(s).wait()
        if s >= outs:
            store(s - outs).wait()

        def body(t, carry):
            r = pl.multiple_of(t * SUB, SUB)
            xs = [src_v[bi, q, pl.ds(r, SUB), :] for q in range(DP)]
            for k in range(DP):
                dst_v[bo, k, pl.ds(r, SUB), :] = jnp.concatenate([v[:, sh * k:sh * (k + 1)] for v in xs], axis=1)
            return carry

        lax.fori_loop(0, n // SUB, body, 0)
        store(s).start()
        if s == ins:
            for k in range(n_small):
                small_in(k).wait()
                small_back(k).start()
    for s in range(len(work) - outs, len(work)):
        store(s).wait()
    for k in range(n_small):
        small_back(k).wait()


def unpack(packed, small, sh):
    work = [(m, r0, n) for m, v in enumerate(packed) for r0, n in split_rows(v.shape[1], 14 if m == 0 else 10)]
    nmax = max(n for _, _, n in work)
    width = packed[0].shape[2]
    anyspec = pl.BlockSpec(memory_space=pl.ANY)
    count = len(small)
    dma = pltpu.SemaphoreType.DMA
    return pl.pallas_call(
        lambda *refs: unpack_kernel(sh, work, count, *refs),
        in_specs=[anyspec] * (2 + count),
        out_specs=[anyspec] * (2 + count),
        out_shape=[jax.ShapeDtypeStruct(v.shape, v.dtype) for v in (*packed, *small)],
        scratch_shapes=[pltpu.VMEM((4, DP, nmax, width), F32), pltpu.VMEM((3, DP, nmax, width), F32), dma((4,)), dma((3,)), dma((2, count))]
        + [pltpu.VMEM(v.shape, v.dtype) for v in small],
        compiler_params=pltpu.CompilerParams(vmem_limit_bytes=67043328),
        name='unpack',
    )(*packed, *small)


def solution(mesh):
    tp_devs = mesh.shape['tp']

    def body(w_in, w_out, g_in, g_out, m_in, m_out, r_in, c_in, r_out, c_out, learn_rate, weight_decay, beta_two):
        width = w_in.shape[1]
        sh = width // 8
        mats = (Mat(w_in.shape[2], width, tp_devs, True), Mat(w_out.shape[1], width, tp_devs, False))
        a, o = mats

        def grouped(v, m):
            return v.reshape(8, m.r, width)

        scal = [v.reshape(1, 1) for v in (learn_rate, weight_decay, beta_two)]
        args = list(scal)
        args += [grouped(g_in[0, 0].T, a), grouped(w_in[0].T, a), m_in[0], r_in, c_in]
        args += [grouped(g_out[0, 0], o), grouped(w_out[0], o), m_out[0].T, c_out, r_out]
        anyspec = pl.BlockSpec(memory_space=pl.ANY)
        sspec = pl.BlockSpec(memory_space=pltpu.SMEM)
        in_specs = [sspec] * 3 + [anyspec] * 10
        out_shape, out_specs = [], []
        for m in mats:
            big = jax.ShapeDtypeStruct((m.r, width), F32)
            out_shape += [jax.ShapeDtypeStruct((8, m.r, width), F32), jax.ShapeDtypeStruct((sh, m.k), BF16),
                          jax.ShapeDtypeStruct((1, sh), F32), jax.ShapeDtypeStruct((1, m.k), F32),
                          jax.ShapeDtypeStruct((4, m.r, width), F32), big, big, big]
            out_specs += [anyspec] * 8
        nmax = max(m.nmax for m in mats)
        dma = pltpu.SemaphoreType.DMA
        scratch = [pltpu.VMEM((2, 2, 4, nmax, width), F32), pltpu.VMEM((2, 8, nmax, 384), F32), pltpu.VMEM((SUB, LANES), F32), pltpu.VMEM((SUB, LANES), F32), dma((2, 2)), dma((2,))]
        for m in mats:
            gt_rows = 12 * m.r
            scratch += [pltpu.VMEM((4, m.r, width), F32), pltpu.VMEM((gt_rows, 256), F32), pltpu.VMEM((sh, LANES * m.tiles), F32),
                        pltpu.VMEM((sh, m.k), BF16), pltpu.VMEM((SUB, LANES * m.tiles), F32), pltpu.VMEM((m.kr + SUB, LANES), F32),
                        pltpu.VMEM((16, m.kr + SUB, LANES), F32), pltpu.VMEM((sh, LANES), F32), pltpu.VMEM((sh, LANES), F32),
                        pltpu.VMEM((SUB, LANES), F32), pltpu.VMEM((16, SUB, LANES), F32),
                        pltpu.VMEM((SUB, sh), F32), pltpu.VMEM((SUB, m.k), F32), pltpu.VMEM((sh, LANES), F32), pltpu.VMEM((sh, LANES), F32),
                        pltpu.VMEM((m.kr, LANES), F32), pltpu.VMEM((m.kr, LANES), F32)]
            scratch += [dma((2, NCH)), dma((2, NCH)), dma((2, NCH)), dma((2, NCH)), dma((2,)), dma((2, 16)), dma((2,)), dma((2, 16)),
                        dma((2, NCH)), dma((2, NCH)), dma((2, NCH)), dma((2, 4, NCH)), dma((5,))]
        outs = pl.pallas_call(
            lambda *refs: main_kernel(mats, sh, *refs),
            in_specs=in_specs,
            out_specs=out_specs,
            out_shape=out_shape,
            scratch_shapes=scratch,
            compiler_params=pltpu.CompilerParams(has_side_effects=True, vmem_limit_bytes=67043328),
            name='step',
        )(*args)
        first, second = outs[0:4], outs[8:12]
        done = unpack((first[0], second[0]), (*first[1:], *second[1:]), sh)
        new_in = done[0].reshape(a.k, width).T[None]
        new_out = done[1].reshape(o.k, width)[None]
        mom_in, row_in, col_in, mom_out, row_out, col_out = done[2:]
        return (new_in, new_out, mom_in[None], mom_out.T[None], row_in, col_in, col_out, row_out)

    free = None
    rows_tp, cols_tp = P(free, 'tp', free), P(free, free, 'tp')
    on_dp, on_tp, whole = P(free, 'dp'), P(free, 'tp'), P()
    state_in, state_out = P(free, 'dp', 'tp'), P(free, 'tp', 'dp')
    in_specs = (cols_tp, rows_tp, P('dp', free, free, 'tp'), P('dp', free, 'tp', free), state_in, state_out, on_dp, on_tp, on_tp, on_dp, whole, whole, whole)
    out_specs = (cols_tp, rows_tp, state_in, state_out, on_dp, on_tp, on_tp, on_dp)
    return jax.shard_map(body, mesh=mesh, in_specs=in_specs, out_specs=out_specs, check_vma=False)
```

```python
import jax
import jax.numpy as jnp
from jax import lax
from jax.experimental import pallas as pl
from jax.experimental.pallas import tpu as pltpu
from jax.sharding import PartitionSpec as P

F32 = jnp.float32
LANES = 128
SUB = 8
DP = 8
BF16 = jnp.bfloat16
MESH = pl.DeviceIdType.MESH
NCH = 8
ORDER = (0, 4, 1, 5, 2, 6, 3, 7)


def chunk_rows(rows):
    tiles = rows // SUB
    out, start = [], 0
    for part in ((tiles + 1) // 2, tiles // 2):
        sizes = [part // 9, part * 3 // 10, part * 7 // 20]
        for n in sizes + [part - sum(sizes)]:
            out.append((SUB * start, SUB * n))
            start += n
    return out


def lane_chunks(total, width=1024):
    out, s = [], 0
    while s < total:
        n = total - s if total - s < 2 * width else width
        if n > width + 256:
            n = width
        out.append((s, n))
        s += n
    return out


class Mat:
    def __init__(self, kloc, width, tp, row_is_r):
        self.k, self.width, self.sh = kloc, width, width // 8
        self.r = kloc // 8
        self.ktot = kloc * tp
        self.row_is_r = row_is_r
        self.ch = chunk_rows(self.r)
        self.tiles = (kloc + 127) // LANES
        self.kr = (self.tiles + 7) // 8 * 8
        self.nmax = max(n for _, n in self.ch)
        self.ra = self.ch[4][0]
        self.keep = not row_is_r


def rcopy(src, dst, sems, dev):
    if sems[0].shape:
        ref, *at = sems
        sems = ref.at[(0, *at)], ref.at[(1, *at)]
    return pltpu.make_async_remote_copy(src_ref=src, dst_ref=dst, send_sem=sems[0], recv_sem=sems[1], device_id=dev, device_id_type=MESH)


def main_kernel(mats, sh, *refs):
    it = iter(refs)
    lr_ref, wd_ref, b2_ref = next(it), next(it), next(it)
    for m in mats:
        m.g, m.w, m.mom, m.row_arg, m.col_arg = (next(it) for _ in range(5))
    for m in mats:
        (m.ag, m.mom_new, m.row_out, m.col_out, m.d2d, m.xy1, m.x2, m.y2, m.fa, m.fb) = (next(it) for _ in range(10))
    stage, wst, usq, ucol = next(it), next(it), next(it), next(it)
    ld_sem, w_sem = next(it), next(it)
    for m in mats:
        (m.p, m.gt, m.gn, m.mv, m.colacc, m.msg, m.slots, m.rp, m.rz, m.sc, m.slots2, m.row_raw, m.col_raw, m.row_old, m.row_new, m.col_old, m.col_new) = (next(it) for _ in range(17))
        (m.d2d_s, m.rs1_s, m.x2_s, m.y2_s, m.ex_s, m.msg_s, m.z_s, m.sc_s, m.agx_s, m.agy_s, m.agd_s, m.ags_s, m.loc_s) = (next(it) for _ in range(13))
    tp = lax.axis_index('tp')
    dp = lax.axis_index('dp')
    c = lax.rem(dp, 2)
    chip = lax.div(dp, 2)
    x = lax.rem(chip, 2)
    y = lax.div(chip, 2)
    jx, jy, jd = chip + 1 - 2 * x, chip + 2 - 4 * y, 3 - chip
    qx, qy, qd, qs = 2 * jx + c, 2 * jy + c, 2 * jd + c, dp + 1 - 2 * c
    sib, xn, yn = {'tp': tp, 'dp': qs}, {'tp': tp, 'dp': qx}, {'tp': tp, 'dp': qy}
    zn = {'tp': 1 - tp, 'dp': dp}
    me16 = tp * 8 + dp

    sends = []

    def start(cp):
        cp.start()
        sends.append(cp)

    def d2d_copy(m, i):
        r0, n = m.ch[i]
        return rcopy(m.g.at[pl.ds(4 * (1 - c), 4), pl.ds(r0, n), :], m.d2d.at[:, pl.ds(r0, n), :], (m.d2d_s, i), sib)

    def load_pair(m, i, b):
        r0, n = m.ch[i]
        own = pltpu.make_async_copy(m.g.at[pl.ds(4 * c, 4), pl.ds(r0, n), :], stage.at[b, 0, :, pl.ds(0, n), :], ld_sem.at[b, 0])
        got = pltpu.make_async_copy(m.d2d.at[:, pl.ds(r0, n), :], stage.at[b, 1, :, pl.ds(0, n), :], ld_sem.at[b, 1])
        return own, got

    def start_loads(m, i, b):
        own, got = load_pair(m, i, b)
        own.start()
        d2d_copy(m, i).wait_recv()
        got.start()

    def pack_chunk(m, i, b):
        r0, n = m.ch[i]
        own, got = load_pair(m, i, b)
        own.wait()
        got.wait()

        def body(t, carry):
            rs = pl.multiple_of(t * SUB, SUB)
            rd = pl.multiple_of(r0 + t * SUB, SUB)
            xs = [stage[b, 0, k, pl.ds(rs, SUB), :] + stage[b, 1, k, pl.ds(rs, SUB), :] for k in range(4)]
            for j in range(4):
                parts = [xs[k][:, sh * (2 * j + cc):sh * (2 * j + cc + 1)] for cc in range(2) for k in range(4)]
                m.p[j, pl.ds(rd, SUB), :] = jnp.concatenate(parts, axis=1)
            return carry

        lax.fori_loop(0, n // SUB, body, 0)

    def pview(m, j, i):
        r0, n = m.ch[i]
        return m.p.at[j, pl.ds(r0, n), :]

    def hview(ref, m, i):
        r0, n = m.ch[i]
        return ref.at[pl.ds(r0, n), :]

    def rs1_copy(m, i):
        dev = xn if i < 4 else yn
        return rcopy(pview(m, jd, i), hview(m.xy1, m, i), (m.rs1_s, i), dev)

    def x2_copy(m, i):
        return rcopy(pview(m, jx, i), hview(m.x2, m, i), (m.x2_s, i), xn)

    def y2_copy(m, i):
        return rcopy(pview(m, jy, i), hview(m.y2, m, i), (m.y2_s, i), yn)

    def rs_free(m, i):
        start(x2_copy(m, i) if i < 4 else y2_copy(m, i))

    def rs_pack(m, send):
        for s, i in enumerate(ORDER):
            if s == 0:
                start_loads(m, i, 0)
            if s > 0 and s + 1 < NCH:
                start_loads(m, ORDER[s + 1], (s + 1) % 2)
            pack_chunk(m, i, s % 2)
            if s == 0:
                start_loads(m, ORDER[1], 1)
            if send:
                start(rs1_copy(m, i))
                if s < 4:
                    rs_free(m, i)

    def rs_dep(m, ids):
        def load(s):
            i = ids[s]
            r0, n = m.ch[i]
            return pltpu.make_async_copy(hview(m.xy1, m, i), stage.at[s % 2, 0, 0, pl.ds(0, n), :], ld_sem.at[s % 2, 0])

        for s, i in enumerate(ids):
            r0, n = m.ch[i]
            rs1_copy(m, i).wait_recv()
            load(s).start()
            load(s).wait()
            j = jy if i < 4 else jx

            def body(t, carry):
                rs = pl.multiple_of(t * SUB, SUB)
                rd = pl.multiple_of(r0 + t * SUB, SUB)
                m.p[j, pl.ds(rd, SUB), :] = m.p[j, pl.ds(rd, SUB), :] + stage[s % 2, 0, 0, pl.ds(rs, SUB), :]
                return carry

            lax.fori_loop(0, n // SUB, body, 0)
            start(y2_copy(m, i) if i < 4 else x2_copy(m, i))

    def acc_own(m, ids):
        base = (2 * c * (4 * m.r), (2 - c) * (4 * m.r))

        def loads(s):
            i = ids[s]
            r0, n = m.ch[i]
            b = s % 2
            return (pltpu.make_async_copy(hview(m.x2, m, i), stage.at[b, 0, 0, pl.ds(0, n), :], ld_sem.at[b, 0]),
                    pltpu.make_async_copy(hview(m.y2, m, i), stage.at[b, 0, 1, pl.ds(0, n), :], ld_sem.at[b, 1]))

        for s, i in enumerate(ids):
            r0, n = m.ch[i]
            b = s % 2
            x2_copy(m, i).wait_recv()
            y2_copy(m, i).wait_recv()
            la, lb = loads(s)
            la.start()
            lb.start()
            la.wait()
            lb.wait()

            def body(t, carry):
                rs = pl.multiple_of(t * SUB, SUB)
                rd = pl.multiple_of(r0 + t * SUB, SUB)
                v = m.p[chip, pl.ds(rd, SUB), :] + stage[b, 0, 0, pl.ds(rs, SUB), :] + stage[b, 0, 1, pl.ds(rs, SUB), :]
                for cc in range(2):
                    for k in range(4):
                        row = pl.multiple_of(base[cc] + k * m.r + r0 + t * SUB, SUB)
                        m.gt[pl.ds(row, SUB), 0:sh] = v[:, sh * (4 * cc + k):sh * (4 * cc + k + 1)]
                return carry

            lax.fori_loop(0, n // SUB, body, 0)

    def ex_copy(m):
        h = 4 * m.r
        return rcopy(m.gt.at[pl.ds(2 * h, h), :], m.gt.at[pl.ds(c * h, h), :], (m.ex_s,), sib)

    def ex_wait(m):
        h = 4 * m.r
        rcopy(m.gt.at[pl.ds(2 * h, h), :], m.gt.at[pl.ds((1 - c) * h, h), :], (m.ex_s,), sib).wait_recv()

    def to_gn(m):
        full = m.k // LANES

        def body(t, carry):
            o = pl.multiple_of(t * LANES, LANES)
            m.gn[:, pl.ds(o, LANES)] = m.gt[pl.ds(o, LANES), :].T[0:sh, :]
            return carry

        lax.fori_loop(0, full, body, 0)
        rest = m.k - full * LANES
        if rest:
            m.gn[:, full * LANES:m.k] = m.gt[full * LANES:full * LANES + LANES, :].T[0:sh, 0:rest]

    def from_gn(m):
        full = m.k // LANES
        pad = m.gt.shape[1] - sh

        def turn(v):
            return jnp.concatenate([v, jnp.zeros((pad, LANES), F32)], axis=0).T

        def body(t, carry):
            o = pl.multiple_of(t * LANES, LANES)
            m.gt[pl.ds(o, LANES), :] = turn(m.gn[:, pl.ds(o, LANES)])
            return carry

        lax.fori_loop(0, full, body, 0)
        rest = m.k - full * LANES
        if rest:
            v = jnp.concatenate([m.gn[:, full * LANES:m.k], jnp.zeros((sh, LANES - rest), F32)], axis=1)
            m.gt[full * LANES:m.k, :] = turn(v)[0:rest, :]

    def vec_loads(m):
        return (pltpu.make_async_copy(m.row_arg, m.row_raw.at[pl.ds(0, 1), :], m.loc_s.at[3]),
                pltpu.make_async_copy(m.col_arg, m.col_raw.at[pl.ds(0, 1), :], m.loc_s.at[4]))

    def vec_stores(m):
        return (pltpu.make_async_copy(m.row_raw.at[pl.ds(0, 1), :], m.row_out, m.loc_s.at[3]),
                pltpu.make_async_copy(m.col_raw.at[pl.ds(0, 1), :], m.col_out, m.loc_s.at[4]))

    def vec_prepare(m):
        for cp in vec_loads(m):
            cp.wait()
        pad = m.gt.shape[1] - sh
        row = jnp.concatenate([m.row_raw[0:1, :], jnp.zeros((1, pad), F32)], axis=1)
        m.row_old[...] = jnp.broadcast_to(row, (LANES, sh + pad)).T[0:sh, :]
        m.col_old[...] = jnp.zeros_like(m.col_old)
        for t in range(m.tiles):
            w = min(LANES, m.k - LANES * t)
            m.col_old[t:t + 1, 0:w] = m.col_raw[0:1, LANES * t:LANES * t + w]

    def vec_finish(m):
        pad = m.gt.shape[1] - sh
        m.row_raw[...] = jnp.concatenate([m.row_new[...], jnp.zeros((pad, LANES), F32)], axis=0).T[0:SUB, 0:sh]
        for t in range(m.tiles):
            w = min(LANES, m.k - LANES * t)
            m.col_raw[0:1, LANES * t:LANES * t + w] = m.col_new[t:t + 1, 0:w]
        for cp in vec_stores(m):
            cp.start()

    def peers():
        out = []
        for d in range(1, 8):
            q = lax.rem(dp + d, 8)
            out.append((True, tp, q))
        for d in range(8):
            q = lax.rem(dp + d, 8)
            out.append((False, 1 - tp, q))
        return out

    def msg_copies(m, sending):
        out = []
        for n, (same, t, q) in enumerate(peers()):
            slot = me16 if sending else t * SUB + q
            dev = {'tp': t, 'dp': q}
            sems = m.msg_s.at[0, n], m.msg_s.at[1, slot]
            if same:
                out.append(rcopy(m.msg, m.slots.at[slot], sems, dev))
            else:
                out.append(rcopy(m.msg.at[pl.ds(m.kr, SUB), :], m.slots.at[slot, pl.ds(m.kr, SUB), :], sems, dev))
        return out

    def z_copy(m):
        return rcopy(m.rp, m.rz, (m.z_s,), zn)

    def sc_copies(m, sending):
        out = []
        for n, (same, t, q) in enumerate(peers()):
            slot = me16 if sending else t * SUB + q
            out.append(rcopy(m.sc, m.slots2.at[slot], (m.sc_s.at[0, n], m.sc_s.at[1, slot]), {'tp': t, 'dp': q}))
        return out

    def stats1(m):
        b2 = b2_ref[0, 0]
        m.colacc[...] = jnp.zeros_like(m.colacc)

        def body(t, carry):
            rr = pl.multiple_of(t * SUB, SUB)
            rsum = jnp.zeros((8, 1), F32)
            for s0, w in lane_chunks(m.k):
                g = m.gn[pl.ds(rr, SUB), s0:s0 + w]
                sq = g * g + 1e-30
                m.colacc[:, s0:s0 + w] = m.colacc[:, s0:s0 + w] + sq
                rsum = rsum + jnp.sum(sq, axis=1, keepdims=True)
            m.rp[pl.ds(rr, SUB), :] = jnp.broadcast_to(rsum, (SUB, LANES))
            return carry

        lax.fori_loop(0, sh // SUB, body, 0)
        for i in range(m.tiles):
            w = min(LANES, m.k - LANES * i)
            m.msg[i:i + 1, 0:w] = jnp.sum(m.colacc[:, LANES * i:LANES * i + w], axis=0, keepdims=True)
        mean_s = jnp.sum(m.rp[...] * (1.0 / m.ktot), axis=0, keepdims=True) * (1.0 / m.width)
        if m.row_is_r:
            old = jnp.sum(m.row_old[...], axis=0, keepdims=True) * (0.5 / m.width)
        else:
            old = jnp.sum(jnp.sum(m.col_old[...], axis=0, keepdims=True), axis=1, keepdims=True) * (0.125 / m.ktot)
        m.msg[m.kr:m.kr + SUB, :] = jnp.broadcast_to(b2 * old + (1.0 - b2) * mean_s, (SUB, LANES))
        m.slots[me16, :, :] = m.msg[...]
        for cp in msg_copies(m, True):
            start(cp)
        start(z_copy(m))

    def stats2(m):
        b2 = b2_ref[0, 0]
        for cp in msg_copies(m, False):
            cp.wait_recv()
        z_copy(m).wait_recv()
        tot = m.slots[tp * 8, 0:m.kr, :]
        for q in range(1, 8):
            tot = tot + m.slots[tp * 8 + q, 0:m.kr, :]
        m.col_new[...] = b2 * m.col_old[...] + (1.0 - b2) * (tot / float(m.width))
        m.row_new[...] = b2 * m.row_old[...] + (1.0 - b2) * ((m.rp[...] + m.rz[...]) / float(m.ktot))
        mean_r = m.slots[0, m.kr:m.kr + SUB, :]
        for q in range(1, 16):
            mean_r = mean_r + m.slots[q, m.kr:m.kr + SUB, :]
        mean_r = mean_r[:, 0:1]
        usq[...] = jnp.zeros_like(usq)
        ucol[...] = jnp.zeros_like(ucol)

        def body(t, carry):
            rr = pl.multiple_of(t * SUB, SUB)
            rv = m.row_new[pl.ds(rr, SUB), 0:1]
            acc = jnp.zeros((8, 1), F32)
            for i in range(m.tiles):
                s0, w = LANES * i, min(LANES, m.k - LANES * i)
                second = rv * m.col_new[i:i + 1, 0:w] / mean_r
                u = m.gn[pl.ds(rr, SUB), s0:s0 + w] / jnp.sqrt(second)
                m.gn[pl.ds(rr, SUB), s0:s0 + w] = u
                if w == LANES:
                    usq[...] = usq[...] + u * u
                else:
                    acc = acc + jnp.sum(u * u, axis=1, keepdims=True)
            ucol[...] = ucol[...] + jnp.broadcast_to(acc, (SUB, LANES))
            return carry

        lax.fori_loop(0, sh // SUB, body, 0)
        usum = jnp.sum(jnp.sum(usq[...], axis=1, keepdims=True), axis=0, keepdims=True)
        usum = usum + jnp.sum(ucol[:, 0:1], axis=0, keepdims=True)
        m.sc[...] = jnp.broadcast_to(usum, (SUB, LANES))
        m.slots2[me16, :, :] = m.sc[...]
        for cp in sc_copies(m, True):
            start(cp)

    def stats3(m):
        for cp in sc_copies(m, False):
            cp.wait_recv()
        tot = m.slots2[0, :, :]
        for q in range(1, 16):
            tot = tot + m.slots2[q, :, :]
        den = jnp.maximum(1.0, jnp.sqrt(tot / (float(m.width) * float(m.ktot))))[0:1, 0:1]
        mom_load(m).wait()

        def body(t, carry):
            rr = pl.multiple_of(t * 16, 16)
            for s0, w in lane_chunks(m.k):
                u = m.gn[pl.ds(rr, 16), s0:s0 + w] / den
                mn = (0.9 * m.mv[pl.ds(rr, 16), s0:s0 + w].astype(F32) + 0.1 * u).astype(BF16)
                m.mv[pl.ds(rr, 16), s0:s0 + w] = mn
                m.gn[pl.ds(rr, 16), s0:s0 + w] = mn.astype(F32)
            return carry

        lax.fori_loop(0, sh // 16, body, 0)
        mom_store(m).start()
        from_gn(m)

    def mom_load(m):
        return pltpu.make_async_copy(m.mom, m.mv, m.loc_s.at[0])

    def mom_store(m):
        return pltpu.make_async_copy(m.mv, m.mom_new, m.loc_s.at[1])

    def own_copy(m):
        return pltpu.make_async_copy(m.p.at[chip], m.ag.at[dp], m.loc_s.at[2])

    lane0 = jnp.minimum(lax.div(sh * dp, LANES), 8)
    off = sh * dp - lane0 * LANES

    def w_load(m, i, b):
        r0, n = m.ch[i]
        return pltpu.make_async_copy(m.w.at[:, pl.ds(r0, n), pl.ds(pl.multiple_of(lane0 * LANES, LANES), 384)], wst.at[b, :, pl.ds(0, n), :], w_sem.at[b])

    def new_weights(m):
        lr, wd = lr_ref[0, 0], wd_ref[0, 0]
        w_load(m, 0, 0).start()
        for i in range(NCH):
            r0, n = m.ch[i]
            b = i % 2
            if i + 1 < NCH:
                w_load(m, i + 1, 1 - b).start()
            w_load(m, i, b).wait()

            def body(t, carry):
                rs = pl.multiple_of(t * SUB, SUB)
                rd = pl.multiple_of(r0 + t * SUB, SUB)
                parts = []
                for k in range(8):
                    w = pltpu.roll(wst[b, k, pl.ds(rs, SUB), :], lax.rem(384 - off, 384), 1)[:, 0:sh]
                    mt = m.gt[pl.ds(pl.multiple_of(k * m.r + r0 + t * SUB, SUB), 8), 0:sh]
                    parts.append(w - lr * mt - lr * wd * w)
                m.p[chip, pl.ds(rd, SUB), :] = jnp.concatenate(parts, axis=1)
                return carry

            lax.fori_loop(0, n // SUB, body, 0)

    def agrow(m, q, i):
        r0, n = m.ch[i]
        return m.ag.at[q, pl.ds(r0, n), :]

    def xrow(m, q, i):
        r0, n = m.ch[i]
        return m.fa.at[pl.ds(r0, n), :] if m.keep and i < 4 else agrow(m, q, i)

    def yrow(m, q, i):
        r0, n = m.ch[i]
        return m.fb.at[pl.ds(r0 - m.ra, n), :] if m.keep and i >= 4 else agrow(m, q, i)

    def ag_own(m, i):
        start(rcopy(pview(m, chip, i), xrow(m, dp, i), (m.agx_s, i), xn))
        start(rcopy(pview(m, chip, i), yrow(m, dp, i), (m.agy_s, i), yn))

    def ag_sib_own(m, i):
        start(rcopy(pview(m, chip, i), agrow(m, dp, i), (m.ags_s, 0, i), sib))

    def ag_sib(m, which, src, q, i):
        start(rcopy(src, agrow(m, q, i), (m.ags_s, which, i), sib))

    def ag_xy(m, i):
        fx, fy = xrow(m, qx, i), yrow(m, qy, i)
        rcopy(fx, fx, (m.agx_s, i), xn).wait_recv()
        rcopy(fy, fy, (m.agy_s, i), yn).wait_recv()
        if not m.keep:
            if i < 4:
                start(rcopy(fx, fx, (m.agd_s, i), yn))
            else:
                start(rcopy(fy, fy, (m.agd_s, i), xn))
        ag_sib(m, 1, fx, qx, i)
        ag_sib(m, 2, fy, qy, i)

    def ag_d(m, i):
        rcopy(agrow(m, qd, i), agrow(m, qd, i), (m.agd_s, i), xn).wait_recv()
        ag_sib(m, 3, agrow(m, qd, i), qd, i)

    def ag_end(m):
        blocks = (qs, qx + 1 - 2 * c, qy + 1 - 2 * c, qd + 1 - 2 * c)
        for which, q in enumerate(blocks[0:3] if m.keep else blocks):
            for i in range(NCH):
                rcopy(agrow(m, q, i), agrow(m, q, i), (m.ags_s, which, i), sib).wait_recv()

    a, o = mats
    for i in ORDER:
        start(d2d_copy(a, i))
    rs_pack(a, True)
    for i in ORDER[4:]:
        rs_free(a, i)
    for i in ORDER:
        start(d2d_copy(o, i))
    for m in mats:
        mom_load(m).start()
        for cp in vec_loads(m):
            cp.start()
    rs_dep(a, ORDER)
    rs_pack(o, False)
    for m in mats:
        vec_prepare(m)
    for i in ORDER[0:6]:
        start(rs1_copy(o, i))
    acc_own(a, ORDER)
    start(ex_copy(a))
    ex_wait(a)
    to_gn(a)
    stats1(a)
    for i in ORDER[6:]:
        start(rs1_copy(o, i))
    stats2(a)
    for i in ORDER[0:4]:
        rs_free(o, i)
    stats3(a)
    for i in ORDER[4:]:
        rs_free(o, i)
    new_weights(a)
    vec_finish(a)
    own_copy(a).start()
    rs_dep(o, ORDER)
    for i in range(2):
        ag_own(a, i)
    for i in range(NCH):
        ag_sib_own(a, i)
    acc_own(o, ORDER)
    start(ex_copy(o))
    ex_wait(o)
    to_gn(o)
    stats1(o)
    for i in range(2, 4):
        ag_own(a, i)
    stats2(o)
    for i in range(4, 6):
        ag_own(a, i)
    stats3(o)
    for i in range(6, 8):
        ag_own(a, i)
    new_weights(o)
    vec_finish(o)
    own_copy(o).start()
    for i in range(NCH):
        ag_sib_own(o, i)
    for i in range(NCH):
        ag_xy(a, i)
    for i in range(NCH):
        ag_own(o, i)
    for i in range(NCH):
        ag_d(a, i)
    for i in range(NCH):
        ag_xy(o, i)
    for m in mats:
        ag_end(m)
        own_copy(m).wait()
        mom_store(m).wait()
        for cp in vec_stores(m):
            cp.wait()
    for cp in sends:
        cp.wait_send()


def split_rows(rows, parts):
    tiles = rows // 8
    out, start = [], 0
    for i in range(parts):
        n = tiles // parts + (1 if i < tiles % parts else 0)
        out.append((8 * start, 8 * n))
        start += n
    return out


def unpack_kernel(sh, work, counts, *refs):
    it = iter(refs)

    def take(n):
        return [next(it) for _ in range(n)]

    n_src, n_small = counts
    srcs, small = take(n_src), take(n_small)
    dst, small_out = next(it), take(n_small)
    src_v, dst_v, in_sem, out_sem, small_sem = take(5)
    small_v = take(n_small)
    ins, outs = src_v.shape[0], dst_v.shape[0]

    def loads(s):
        r0, n = work[s]
        b = s % ins
        if n_src == 1:
            return [pltpu.make_async_copy(srcs[0].at[:, pl.ds(r0, n), :], src_v.at[b, :, pl.ds(0, n), :], in_sem.at[b, 0])]
        ag, fa, fb, da, db, sa, sb = srcs
        dp = lax.axis_index('dp')
        c = lax.rem(dp, 2)
        chip = lax.div(dp, 2)
        x, y = lax.rem(chip, 2), lax.div(chip, 2)
        qx, qy = dp + 2 - 4 * x, dp + 4 - DP * y
        qd, other = qx + qy - dp, 1 - 2 * c
        first = r0 < fa.shape[0]
        rr = r0 if first else r0 - fa.shape[0]

        def block(q):
            return ag.at[q, pl.ds(r0, n), :]

        def part(ref):
            return ref.at[pl.ds(rr, n), :]

        pairs = [(dp, block(dp)), (dp + other, block(dp + other)), (qx + other, block(qx + other)), (qy + other, block(qy + other))]
        pairs += [(qx, part(fa) if first else block(qx)), (qy, block(qy) if first else part(fb))]
        pairs += [(qd, part(da if first else db)), (qd + other, part(sa if first else sb))]
        return [pltpu.make_async_copy(v, src_v.at[b, q, pl.ds(0, n), :], in_sem.at[b, e]) for e, (q, v) in enumerate(pairs)]

    def store(s):
        r0, n = work[s]
        return pltpu.make_async_copy(dst_v.at[s % outs, :, pl.ds(0, n), :], dst.at[:, pl.ds(r0, n), :], out_sem.at[s % outs])

    def small_in(k):
        return pltpu.make_async_copy(small[k], small_v[k], small_sem.at[0, k])

    def small_back(k):
        return pltpu.make_async_copy(small_v[k], small_out[k], small_sem.at[1, k])

    def start_loads(s):
        for cp in loads(s):
            cp.start()

    for s in range(ins - 1):
        start_loads(s)
    for k in range(n_small):
        small_in(k).start()
    for s, (r0, n) in enumerate(work):
        bi, bo = s % ins, s % outs
        if s + ins - 1 < len(work):
            start_loads(s + ins - 1)
        for cp in loads(s):
            cp.wait()
        if s >= outs:
            store(s - outs).wait()

        def body(t, carry):
            r = pl.multiple_of(t * SUB, SUB)
            xs = [src_v[bi, q, pl.ds(r, SUB), :] for q in range(DP)]
            for k in range(DP):
                dst_v[bo, k, pl.ds(r, SUB), :] = jnp.concatenate([v[:, sh * k:sh * (k + 1)] for v in xs], axis=1)
            return carry

        lax.fori_loop(0, n // SUB, body, 0)
        store(s).start()
        if s == ins:
            for k in range(n_small):
                small_in(k).wait()
                small_back(k).start()
    for s in range(len(work) - outs, len(work)):
        store(s).wait()
    for k in range(n_small):
        small_back(k).wait()


def unpack(packed, small, sh, work, name):
    nmax = max(n for _, n in work)
    shape = packed[0].shape
    anyspec = pl.BlockSpec(memory_space=pl.ANY)
    counts = (len(packed), len(small))
    dma = pltpu.SemaphoreType.DMA
    size = shape[0] * shape[1] * shape[2]
    return pl.pallas_call(
        lambda *refs: unpack_kernel(sh, work, counts, *refs),
        in_specs=[anyspec] * sum(counts),
        out_specs=[anyspec] * (1 + len(small)),
        out_shape=[jax.ShapeDtypeStruct(v.shape, v.dtype) for v in (packed[0], *small)],
        scratch_shapes=[pltpu.VMEM((4, DP, nmax, shape[2]), F32), pltpu.VMEM((3, DP, nmax, shape[2]), F32), dma((4, DP)), dma((3,)), dma((2, max(1, len(small))))]
        + [pltpu.VMEM(v.shape, v.dtype) for v in small],
        compiler_params=pltpu.CompilerParams(vmem_limit_bytes=67043328),
        cost_estimate=pl.CostEstimate(flops=1000 * size, bytes_accessed=DP * size, transcendentals=0),
        name=name,
    )(*packed, *small)


def solution(mesh):
    tp_devs = mesh.shape['tp']

    def body(w_in, w_out, g_in, g_out, m_in, m_out, r_in, c_in, r_out, c_out, learn_rate, weight_decay, beta_two):
        width = w_in.shape[1]
        sh = width // 8
        mats = (Mat(w_in.shape[2], width, tp_devs, True), Mat(w_out.shape[1], width, tp_devs, False))
        a, o = mats

        def grouped(v, m):
            return v.reshape(8, m.r, width)

        scal = [v.reshape(1, 1) for v in (learn_rate, weight_decay, beta_two)]
        args = list(scal)
        args += [grouped(g_in[0, 0].T, a), grouped(w_in[0].T, a), m_in[0], r_in, c_in]
        args += [grouped(g_out[0, 0], o), grouped(w_out[0], o), m_out[0].T, c_out, r_out]
        anyspec = pl.BlockSpec(memory_space=pl.ANY)
        sspec = pl.BlockSpec(memory_space=pltpu.SMEM)
        in_specs = [sspec] * 3 + [anyspec] * 10
        out_shape, out_specs = [], []
        for m in mats:
            big = jax.ShapeDtypeStruct((m.r, width), F32)
            out_shape += [jax.ShapeDtypeStruct((8, m.r, width), F32), jax.ShapeDtypeStruct((sh, m.k), BF16),
                          jax.ShapeDtypeStruct((1, sh), F32), jax.ShapeDtypeStruct((1, m.k), F32),
                          jax.ShapeDtypeStruct((4, m.r, width), F32), big, big, big,
                          jax.ShapeDtypeStruct((m.ra, width), F32), jax.ShapeDtypeStruct((m.r - m.ra, width), F32)]
            out_specs += [anyspec] * 10
        nmax = max(m.nmax for m in mats)
        dma = pltpu.SemaphoreType.DMA
        scratch = [pltpu.VMEM((2, 2, 4, nmax, width), F32), pltpu.VMEM((2, 8, nmax, 384), F32), pltpu.VMEM((SUB, LANES), F32), pltpu.VMEM((SUB, LANES), F32), dma((2, 2)), dma((2,))]
        for m in mats:
            gt_rows = 12 * m.r
            scratch += [pltpu.VMEM((4, m.r, width), F32), pltpu.VMEM((gt_rows, 256), F32), pltpu.VMEM((sh, LANES * m.tiles), F32),
                        pltpu.VMEM((sh, m.k), BF16), pltpu.VMEM((SUB, LANES * m.tiles), F32), pltpu.VMEM((m.kr + SUB, LANES), F32),
                        pltpu.VMEM((16, m.kr + SUB, LANES), F32), pltpu.VMEM((sh, LANES), F32), pltpu.VMEM((sh, LANES), F32),
                        pltpu.VMEM((SUB, LANES), F32), pltpu.VMEM((16, SUB, LANES), F32),
                        pltpu.VMEM((SUB, sh), F32), pltpu.VMEM((SUB, m.k), F32), pltpu.VMEM((sh, LANES), F32), pltpu.VMEM((sh, LANES), F32),
                        pltpu.VMEM((m.kr, LANES), F32), pltpu.VMEM((m.kr, LANES), F32)]
            scratch += [dma((2, NCH)), dma((2, NCH)), dma((2, NCH)), dma((2, NCH)), dma((2,)), dma((2, 16)), dma((2,)), dma((2, 16)),
                        dma((2, NCH)), dma((2, NCH)), dma((2, NCH)), dma((2, 4, NCH)), dma((5,))]
        outs = pl.pallas_call(
            lambda *refs: main_kernel(mats, sh, *refs),
            in_specs=in_specs,
            out_specs=out_specs,
            out_shape=out_shape,
            scratch_shapes=scratch,
            compiler_params=pltpu.CompilerParams(has_side_effects=True, vmem_limit_bytes=67043328),
            name='step',
        )(*args)
        first, second = outs[0:4], outs[10:14]
        fa, fb = outs[18:]
        chips = mesh.shape['dp'] // 2

        def swap(v, bit):
            return lax.ppermute(v, 'dp', [(q, q ^ bit) for q in range(2 * chips)])

        da, db = swap(fa, 4), swap(fb, 2)
        done = unpack((first[0],), (*first[1:], *second[1:]), sh, split_rows(a.r, 14), 'unpack_in')
        da, db, small = lax.optimization_barrier((da, db, done[2]))
        sa, sb = swap(da, 1), swap(db, 1)
        work = split_rows(o.ra, 5) + [(o.ra + r0, n) for r0, n in split_rows(o.r - o.ra, 5)]
        last = unpack((second[0], fa, fb, da, db, sa, sb), (), sh, work, 'unpack_out')
        new_in = done[0].reshape(a.k, width).T[None]
        new_out = last[0].reshape(o.k, width)[None]
        mom_in, _, col_in, mom_out, row_out, col_out = done[1:]
        return (new_in, new_out, mom_in[None], mom_out.T[None], small, col_in, col_out, row_out)

    free = None
    rows_tp, cols_tp = P(free, 'tp', free), P(free, free, 'tp')
    on_dp, on_tp, whole = P(free, 'dp'), P(free, 'tp'), P()
    state_in, state_out = P(free, 'dp', 'tp'), P(free, 'tp', 'dp')
    in_specs = (cols_tp, rows_tp, P('dp', free, free, 'tp'), P('dp', free, 'tp', free), state_in, state_out, on_dp, on_tp, on_tp, on_dp, whole, whole, whole)
    out_specs = (cols_tp, rows_tp, state_in, state_out, on_dp, on_tp, on_tp, on_dp)
    return jax.shard_map(body, mesh=mesh, in_specs=in_specs, out_specs=out_specs, check_vma=False)
```

```python
import jax
import jax.numpy as jnp
from jax import lax
from jax.experimental import pallas as pl
from jax.experimental.pallas import tpu as pltpu
from jax.sharding import PartitionSpec as P

F32 = jnp.float32
LANES = 128
SUB = 8
DP = 8
EVERY = 16
ALL_VMEM = 67043328
BESIDE_HOLD = 45000000
BF16 = jnp.bfloat16
MESH = pl.DeviceIdType.MESH
NCH = 8
ORDER = (0, 4, 1, 5, 2, 6, 3, 7)


def chunk_rows(rows, small_last):
    tiles = rows // SUB
    out, start = [], 0
    for part in ((tiles + 1) // 2, tiles // 2):
        sizes = [part // 9, part * 3 // 10, part * 7 // 20]
        sizes.append(part - sum(sizes))
        for n in sizes[::-1] if small_last and out else sizes:
            out.append((SUB * start, SUB * n))
            start += n
    return out


def lane_chunks(total):
    width = SUB * LANES
    out = [(s, width) for s in range(0, total - width, width)]
    last = len(out) * width
    if total - last < width // 4:
        s, n = out.pop()
        return out + [(s, n + total - last)]
    return out + [(last, total - last)]


class Mat:
    def __init__(self, kloc, width, tp, row_is_r):
        self.k, self.width, self.sh = kloc, width, width // 8
        self.r = kloc // 8
        self.ktot = kloc * tp
        self.row_is_r = row_is_r
        self.ch = chunk_rows(self.r, not row_is_r)
        self.tiles = (kloc + 127) // LANES
        self.kr = (self.tiles + SUB) // SUB * SUB
        self.nmax = max(n for _, n in self.ch)
        self.ra = self.ch[4][0]
        self.keep = not row_is_r


def rcopy(src, dst, sems, dev):
    if sems[0].shape:
        ref, *at = sems
        sems = ref.at[(0, *at)], ref.at[(1, *at)]
    return pltpu.make_async_remote_copy(src_ref=src, dst_ref=dst, send_sem=sems[0], recv_sem=sems[1], device_id=dev, device_id_type=MESH)


def places():
    dp = lax.axis_index('dp')
    c, chip = lax.rem(dp, 2), lax.div(dp, 2)
    x, y = lax.rem(chip, 2), lax.div(chip, 2)
    return dp, c, chip, chip + 1 - 2 * x, chip + 2 - 4 * y, 3 - chip


def main_kernel(mats, sh, *refs):
    it = iter(refs)
    lr_ref, wd_ref, b2_ref = next(it), next(it), next(it)
    for m in mats:
        m.g, m.w, m.mom, m.row_arg, m.col_arg = (next(it) for _ in range(5))
    for m in mats:
        (m.ag, m.mom_new, m.row_out, m.col_out, m.d2d, m.xy1, m.x2, m.y2, m.fa, m.fb) = (next(it) for _ in range(10))
    stage, wst, usq, ucol = next(it), next(it), next(it), next(it)
    ld_sem, w_sem = next(it), next(it)
    for m in mats:
        (m.p, m.gt, m.gn, m.mv, m.colacc, m.msg, m.slots, m.rp, m.rz, m.sc, m.slots2, m.row_raw, m.col_raw, m.row_old, m.row_new, m.col_old, m.col_new) = (next(it) for _ in range(17))
        (m.d2d_s, m.rs1_s, m.x2_s, m.y2_s, m.ex_s, m.msg_s, m.z_s, m.sc_s, m.agx_s, m.agy_s, m.agd_s, m.ags_s, m.loc_s) = (next(it) for _ in range(13))
    tp = lax.axis_index('tp')
    dp, c, chip, jx, jy, jd = places()
    qx, qy, qd, qs = 2 * jx + c, 2 * jy + c, 2 * jd + c, dp + 1 - 2 * c
    sib, xn, yn = {'tp': tp, 'dp': qs}, {'tp': tp, 'dp': qx}, {'tp': tp, 'dp': qy}
    zn = {'tp': 1 - tp, 'dp': dp}
    me16 = tp * DP + dp

    sends = []

    def start(cp):
        cp.start()
        sends.append(cp)

    def d2d_copy(m, i):
        r0, n = m.ch[i]
        return rcopy(m.g.at[pl.ds(4 * (1 - c), 4), pl.ds(r0, n), :], m.d2d.at[:, pl.ds(r0, n), :], (m.d2d_s, i), sib)

    def load_pair(m, i, b):
        r0, n = m.ch[i]
        own = pltpu.make_async_copy(m.g.at[pl.ds(4 * c, 4), pl.ds(r0, n), :], stage.at[b, 0, :, pl.ds(0, n), :], ld_sem.at[b, 0])
        got = pltpu.make_async_copy(m.d2d.at[:, pl.ds(r0, n), :], stage.at[b, 1, :, pl.ds(0, n), :], ld_sem.at[b, 1])
        return own, got

    def start_loads(m, i, b):
        own, got = load_pair(m, i, b)
        own.start()
        d2d_copy(m, i).wait_recv()
        got.start()

    def pack_chunk(m, i, b):
        r0, n = m.ch[i]
        own, got = load_pair(m, i, b)
        own.wait()
        got.wait()

        def body(t, carry):
            rs = pl.multiple_of(t * SUB, SUB)
            rd = pl.multiple_of(r0 + t * SUB, SUB)
            xs = [stage[b, 0, k, pl.ds(rs, SUB), :] + stage[b, 1, k, pl.ds(rs, SUB), :] for k in range(4)]
            for j in range(4):
                parts = [xs[k][:, sh * (2 * j + cc):sh * (2 * j + cc + 1)] for cc in range(2) for k in range(4)]
                m.p[j, pl.ds(rd, SUB), :] = jnp.concatenate(parts, axis=1)
            return carry

        lax.fori_loop(0, n // SUB, body, 0)

    def pview(m, j, i):
        r0, n = m.ch[i]
        return m.p.at[j, pl.ds(r0, n), :]

    def hview(ref, m, i):
        r0, n = m.ch[i]
        return ref.at[pl.ds(r0, n), :]

    def rs1_copy(m, i):
        dev = xn if i < 4 else yn
        return rcopy(pview(m, jd, i), hview(m.xy1, m, i), (m.rs1_s, i), dev)

    def x2_copy(m, i):
        return rcopy(pview(m, jx, i), hview(m.x2, m, i), (m.x2_s, i), xn)

    def y2_copy(m, i):
        return rcopy(pview(m, jy, i), hview(m.y2, m, i), (m.y2_s, i), yn)

    def rs_free(m, i):
        start(x2_copy(m, i) if i < 4 else y2_copy(m, i))

    def rs_pack(m, send):
        for s, i in enumerate(ORDER):
            if s == 0:
                start_loads(m, i, 0)
            if s > 0 and s + 1 < NCH:
                start_loads(m, ORDER[s + 1], (s + 1) % 2)
            pack_chunk(m, i, s % 2)
            if s == 0:
                start_loads(m, ORDER[1], 1)
            if send:
                start(rs1_copy(m, i))
                if s < 4:
                    rs_free(m, i)

    def rs_dep(m, ids):
        def load(s):
            i = ids[s]
            r0, n = m.ch[i]
            return pltpu.make_async_copy(hview(m.xy1, m, i), stage.at[s % 2, 0, 0, pl.ds(0, n), :], ld_sem.at[s % 2, 0])

        for s, i in enumerate(ids):
            r0, n = m.ch[i]
            rs1_copy(m, i).wait_recv()
            load(s).start()
            load(s).wait()
            j = jy if i < 4 else jx

            def body(t, carry):
                rs = pl.multiple_of(t * SUB, SUB)
                rd = pl.multiple_of(r0 + t * SUB, SUB)
                m.p[j, pl.ds(rd, SUB), :] = m.p[j, pl.ds(rd, SUB), :] + stage[s % 2, 0, 0, pl.ds(rs, SUB), :]
                return carry

            lax.fori_loop(0, n // SUB, body, 0)
            start(y2_copy(m, i) if i < 4 else x2_copy(m, i))

    def acc_own(m, ids):
        base = (2 * c * (4 * m.r), (2 - c) * (4 * m.r))

        def loads(s):
            i = ids[s]
            r0, n = m.ch[i]
            b = s % 2
            return (pltpu.make_async_copy(hview(m.x2, m, i), stage.at[b, 0, 0, pl.ds(0, n), :], ld_sem.at[b, 0]),
                    pltpu.make_async_copy(hview(m.y2, m, i), stage.at[b, 0, 1, pl.ds(0, n), :], ld_sem.at[b, 1]))

        for s, i in enumerate(ids):
            r0, n = m.ch[i]
            b = s % 2
            x2_copy(m, i).wait_recv()
            y2_copy(m, i).wait_recv()
            la, lb = loads(s)
            la.start()
            lb.start()
            la.wait()
            lb.wait()

            def body(t, carry):
                rs = pl.multiple_of(t * SUB, SUB)
                rd = pl.multiple_of(r0 + t * SUB, SUB)
                v = m.p[chip, pl.ds(rd, SUB), :] + stage[b, 0, 0, pl.ds(rs, SUB), :] + stage[b, 0, 1, pl.ds(rs, SUB), :]
                for cc in range(2):
                    for k in range(4):
                        row = pl.multiple_of(base[cc] + k * m.r + r0 + t * SUB, SUB)
                        m.gt[pl.ds(row, SUB), 0:sh] = v[:, sh * (4 * cc + k):sh * (4 * cc + k + 1)]
                return carry

            lax.fori_loop(0, n // SUB, body, 0)

    def ex_copy(m):
        h = 4 * m.r
        return rcopy(m.gt.at[pl.ds(2 * h, h), :], m.gt.at[pl.ds(c * h, h), :], (m.ex_s,), sib)

    def ex_wait(m):
        h = 4 * m.r
        rcopy(m.gt.at[pl.ds(2 * h, h), :], m.gt.at[pl.ds((1 - c) * h, h), :], (m.ex_s,), sib).wait_recv()

    def to_gn(m):
        full = m.k // LANES

        def body(t, carry):
            o = pl.multiple_of(t * LANES, LANES)
            m.gn[:, pl.ds(o, LANES)] = m.gt[pl.ds(o, LANES), :].T[0:sh, :]
            return carry

        lax.fori_loop(0, full, body, 0)
        rest = m.k - full * LANES
        if rest:
            m.gn[:, full * LANES:m.k] = m.gt[full * LANES:full * LANES + LANES, :].T[0:sh, 0:rest]

    def from_gn(m):
        full = m.k // LANES
        pad = m.gt.shape[1] - sh

        def turn(v):
            return jnp.concatenate([v, jnp.zeros((pad, LANES), F32)], axis=0).T

        def body(t, carry):
            o = pl.multiple_of(t * LANES, LANES)
            m.gt[pl.ds(o, LANES), :] = turn(m.gn[:, pl.ds(o, LANES)])
            return carry

        lax.fori_loop(0, full, body, 0)
        rest = m.k - full * LANES
        if rest:
            v = jnp.concatenate([m.gn[:, full * LANES:m.k], jnp.zeros((sh, LANES - rest), F32)], axis=1)
            m.gt[full * LANES:m.k, :] = turn(v)[0:rest, :]

    def vec_loads(m):
        return (pltpu.make_async_copy(m.row_arg, m.row_raw.at[pl.ds(0, 1), :], m.loc_s.at[3]),
                pltpu.make_async_copy(m.col_arg, m.col_raw.at[pl.ds(0, 1), :], m.loc_s.at[4]))

    def vec_stores(m):
        return (pltpu.make_async_copy(m.row_raw.at[pl.ds(0, 1), :], m.row_out, m.loc_s.at[3]),
                pltpu.make_async_copy(m.col_raw.at[pl.ds(0, 1), :], m.col_out, m.loc_s.at[4]))

    def vec_prepare(m):
        for cp in vec_loads(m):
            cp.wait()
        pad = m.gt.shape[1] - sh
        row = jnp.concatenate([m.row_raw[0:1, :], jnp.zeros((1, pad), F32)], axis=1)
        m.row_old[...] = jnp.broadcast_to(row, (LANES, sh + pad)).T[0:sh, :]
        m.col_old[...] = jnp.zeros_like(m.col_old)
        for t in range(m.tiles):
            w = min(LANES, m.k - LANES * t)
            m.col_old[t:t + 1, 0:w] = m.col_raw[0:1, LANES * t:LANES * t + w]

    def vec_finish(m):
        pad = m.gt.shape[1] - sh
        m.row_raw[...] = jnp.concatenate([m.row_new[...], jnp.zeros((pad, LANES), F32)], axis=0).T[0:SUB, 0:sh]
        for t in range(m.tiles):
            w = min(LANES, m.k - LANES * t)
            m.col_raw[0:1, LANES * t:LANES * t + w] = m.col_new[t:t + 1, 0:w]
        for cp in vec_stores(m):
            cp.start()

    def peers():
        out = []
        for d in range(1, 8):
            q = lax.rem(dp + d, 8)
            out.append((True, tp, q))
        for d in range(8):
            q = lax.rem(dp + d, 8)
            out.append((False, 1 - tp, q))
        return out

    def msg_copies(m, sending):
        out = []
        for n, (same, t, q) in enumerate(peers()):
            slot = me16 if sending else t * SUB + q
            dev = {'tp': t, 'dp': q}
            sems = m.msg_s.at[0, n], m.msg_s.at[1, slot]
            rows = pl.ds(0, m.tiles + 1) if same else pl.ds(m.tiles, 1)
            out.append(rcopy(m.msg.at[rows, :], m.slots.at[slot, rows, :], sems, dev))
        return out

    def z_copy(m):
        return rcopy(m.rp, m.rz, (m.z_s,), zn)

    def sc_copies(m, sending):
        out = []
        for n, (same, t, q) in enumerate(peers()):
            slot = me16 if sending else t * SUB + q
            out.append(rcopy(m.sc.at[pl.ds(0, 1), :], m.slots2.at[slot, pl.ds(0, 1), :], (m.sc_s.at[0, n], m.sc_s.at[1, slot]), {'tp': t, 'dp': q}))
        return out

    def stats1(m):
        b2 = b2_ref[0, 0]
        m.colacc[...] = jnp.zeros_like(m.colacc)

        def body(t, carry):
            rr = pl.multiple_of(t * SUB, SUB)
            rsum = jnp.zeros((8, 1), F32)
            for s0, w in lane_chunks(m.k):
                g = m.gn[pl.ds(rr, SUB), s0:s0 + w]
                sq = g * g + 1e-30
                m.colacc[:, s0:s0 + w] = m.colacc[:, s0:s0 + w] + sq
                rsum = rsum + jnp.sum(sq, axis=1, keepdims=True)
            m.rp[pl.ds(rr, SUB), :] = jnp.broadcast_to(rsum, (SUB, LANES))
            return carry

        lax.fori_loop(0, sh // SUB, body, 0)
        for i in range(m.tiles):
            w = min(LANES, m.k - LANES * i)
            m.msg[i:i + 1, 0:w] = jnp.sum(m.colacc[:, LANES * i:LANES * i + w], axis=0, keepdims=True)
        mean_s = jnp.sum(m.rp[...] * (1.0 / m.ktot), axis=0, keepdims=True) * (1.0 / m.width)
        if m.row_is_r:
            old = jnp.sum(m.row_old[...], axis=0, keepdims=True) * (0.5 / m.width)
        else:
            old = jnp.sum(jnp.sum(m.col_old[...], axis=0, keepdims=True), axis=1, keepdims=True) * (0.125 / m.ktot)
        m.msg[m.tiles:m.tiles + 1, :] = jnp.broadcast_to(b2 * old + (1.0 - b2) * mean_s, (1, LANES))
        m.slots[me16, :, :] = m.msg[...]
        for cp in msg_copies(m, True):
            start(cp)
        start(z_copy(m))

    def stats2(m):
        b2 = b2_ref[0, 0]
        for cp in msg_copies(m, False):
            cp.wait_recv()
        z_copy(m).wait_recv()
        tot = m.slots[tp * 8, 0:m.kr, :]
        for q in range(1, 8):
            tot = tot + m.slots[tp * 8 + q, 0:m.kr, :]
        m.col_new[...] = b2 * m.col_old[...] + (1.0 - b2) * (tot / float(m.width))
        m.row_new[...] = b2 * m.row_old[...] + (1.0 - b2) * ((m.rp[...] + m.rz[...]) / float(m.ktot))
        mean_r = m.slots[0, m.tiles:m.tiles + 1, :]
        for q in range(1, EVERY):
            mean_r = mean_r + m.slots[q, m.tiles:m.tiles + 1, :]
        mean_r = mean_r[:, 0:1]
        usq[...] = jnp.zeros_like(usq)
        ucol[...] = jnp.zeros_like(ucol)

        def body(t, carry):
            rr = pl.multiple_of(t * SUB, SUB)
            rv = m.row_new[pl.ds(rr, SUB), 0:1]
            acc = jnp.zeros((8, 1), F32)
            for i in range(m.tiles):
                s0, w = LANES * i, min(LANES, m.k - LANES * i)
                second = rv * m.col_new[i:i + 1, 0:w] / mean_r
                u = m.gn[pl.ds(rr, SUB), s0:s0 + w] / jnp.sqrt(second)
                m.gn[pl.ds(rr, SUB), s0:s0 + w] = u
                if w == LANES:
                    usq[...] = usq[...] + u * u
                else:
                    acc = acc + jnp.sum(u * u, axis=1, keepdims=True)
            ucol[...] = ucol[...] + jnp.broadcast_to(acc, (SUB, LANES))
            return carry

        lax.fori_loop(0, sh // SUB, body, 0)
        usum = jnp.sum(jnp.sum(usq[...], axis=1, keepdims=True), axis=0, keepdims=True)
        usum = usum + jnp.sum(ucol[:, 0:1], axis=0, keepdims=True)
        m.sc[...] = jnp.broadcast_to(usum, (SUB, LANES))
        m.slots2[me16, :, :] = m.sc[...]
        for cp in sc_copies(m, True):
            start(cp)

    def stats3(m):
        for cp in sc_copies(m, False):
            cp.wait_recv()
        tot = m.slots2[0, 0:1, :]
        for q in range(1, EVERY):
            tot = tot + m.slots2[q, 0:1, :]
        den = jnp.maximum(1.0, jnp.sqrt(tot / (float(m.width) * float(m.ktot))))[0:1, 0:1]
        mom_load(m).wait()

        def body(t, carry):
            rr = pl.multiple_of(t * 16, 16)
            for s0, w in lane_chunks(m.k):
                u = m.gn[pl.ds(rr, 16), s0:s0 + w] / den
                mn = (0.9 * m.mv[pl.ds(rr, 16), s0:s0 + w].astype(F32) + 0.1 * u).astype(BF16)
                m.mv[pl.ds(rr, 16), s0:s0 + w] = mn
                m.gn[pl.ds(rr, 16), s0:s0 + w] = mn.astype(F32)
            return carry

        lax.fori_loop(0, sh // 16, body, 0)
        mom_store(m).start()
        from_gn(m)

    def mom_load(m):
        return pltpu.make_async_copy(m.mom, m.mv, m.loc_s.at[0])

    def mom_store(m):
        return pltpu.make_async_copy(m.mv, m.mom_new, m.loc_s.at[1])

    def own_copy(m):
        return pltpu.make_async_copy(m.p.at[chip], m.ag.at[dp], m.loc_s.at[2])

    lane0 = jnp.minimum(lax.div(sh * dp, LANES), 8)
    off = sh * dp - lane0 * LANES

    def w_load(m, i, b):
        r0, n = m.ch[i]
        return pltpu.make_async_copy(m.w.at[:, pl.ds(r0, n), pl.ds(pl.multiple_of(lane0 * LANES, LANES), 384)], wst.at[b, :, pl.ds(0, n), :], w_sem.at[b])

    def new_weights(m):
        lr, wd = lr_ref[0, 0], wd_ref[0, 0]
        w_load(m, 0, 0).start()
        for i in range(NCH):
            r0, n = m.ch[i]
            b = i % 2
            if i + 1 < NCH:
                w_load(m, i + 1, 1 - b).start()
            w_load(m, i, b).wait()

            def body(t, carry):
                rs = pl.multiple_of(t * SUB, SUB)
                rd = pl.multiple_of(r0 + t * SUB, SUB)
                parts = []
                for k in range(8):
                    w = pltpu.roll(wst[b, k, pl.ds(rs, SUB), :], lax.rem(384 - off, 384), 1)[:, 0:sh]
                    mt = m.gt[pl.ds(pl.multiple_of(k * m.r + r0 + t * SUB, SUB), 8), 0:sh]
                    parts.append(w - lr * mt - lr * wd * w)
                m.p[chip, pl.ds(rd, SUB), :] = jnp.concatenate(parts, axis=1)
                return carry

            lax.fori_loop(0, n // SUB, body, 0)

    def agrow(m, q, i):
        r0, n = m.ch[i]
        return m.ag.at[q, pl.ds(r0, n), :]

    def xrow(m, q, i):
        r0, n = m.ch[i]
        return m.fa.at[pl.ds(r0, n), :] if m.keep and i < 4 else agrow(m, q, i)

    def yrow(m, q, i):
        r0, n = m.ch[i]
        return m.fb.at[pl.ds(r0 - m.ra, n), :] if m.keep and i >= 4 else agrow(m, q, i)

    def ag_own(m, i):
        start(rcopy(pview(m, chip, i), xrow(m, dp, i), (m.agx_s, i), xn))
        start(rcopy(pview(m, chip, i), yrow(m, dp, i), (m.agy_s, i), yn))

    def ag_sib_own(m, i):
        start(rcopy(pview(m, chip, i), agrow(m, dp, i), (m.ags_s, 0, i), sib))

    def ag_sib(m, which, src, q, i):
        start(rcopy(src, agrow(m, q, i), (m.ags_s, which, i), sib))

    def ag_xy(m, i):
        fx, fy = xrow(m, qx, i), yrow(m, qy, i)
        rcopy(fx, fx, (m.agx_s, i), xn).wait_recv()
        rcopy(fy, fy, (m.agy_s, i), yn).wait_recv()
        if not m.keep:
            if i < 4:
                start(rcopy(fx, fx, (m.agd_s, i), yn))
            else:
                start(rcopy(fy, fy, (m.agd_s, i), xn))
        ag_sib(m, 1, fx, qx, i)
        ag_sib(m, 2, fy, qy, i)

    def ag_d(m, i):
        rcopy(agrow(m, qd, i), agrow(m, qd, i), (m.agd_s, i), xn).wait_recv()
        ag_sib(m, 3, agrow(m, qd, i), qd, i)

    def ag_end(m):
        blocks = (qs, qx + 1 - 2 * c, qy + 1 - 2 * c, qd + 1 - 2 * c)
        for which, q in enumerate(blocks[0:3] if m.keep else blocks):
            for i in range(NCH):
                rcopy(agrow(m, q, i), agrow(m, q, i), (m.ags_s, which, i), sib).wait_recv()

    a, o = mats
    for i in ORDER:
        start(d2d_copy(a, i))
    rs_pack(a, True)
    for i in ORDER[4:]:
        rs_free(a, i)
    for i in ORDER:
        start(d2d_copy(o, i))
    for m in mats:
        mom_load(m).start()
        for cp in vec_loads(m):
            cp.start()
    rs_dep(a, ORDER)
    rs_pack(o, False)
    for m in mats:
        vec_prepare(m)
    for i in ORDER[0:6]:
        start(rs1_copy(o, i))
    acc_own(a, ORDER)
    start(ex_copy(a))
    ex_wait(a)
    to_gn(a)
    stats1(a)
    for i in ORDER[6:]:
        start(rs1_copy(o, i))
    stats2(a)
    for i in ORDER[0:4]:
        rs_free(o, i)
    stats3(a)
    for i in ORDER[4:]:
        rs_free(o, i)
    new_weights(a)
    vec_finish(a)
    own_copy(a).start()
    rs_dep(o, ORDER)
    for i in range(2):
        ag_own(a, i)
    for i in range(NCH):
        ag_sib_own(a, i)
    acc_own(o, ORDER)
    start(ex_copy(o))
    ex_wait(o)
    to_gn(o)
    stats1(o)
    for i in range(2, 4):
        ag_own(a, i)
    stats2(o)
    for i in range(4, 6):
        ag_own(a, i)
    stats3(o)
    for i in range(6, 8):
        ag_own(a, i)
    new_weights(o)
    vec_finish(o)
    own_copy(o).start()
    for i in range(NCH):
        ag_sib_own(o, i)
    for i in range(NCH):
        ag_xy(a, i)
    for i in range(NCH):
        ag_own(o, i)
    for i in range(NCH):
        ag_d(a, i)
    for i in range(NCH):
        ag_xy(o, i)
    for m in mats:
        ag_end(m)
        own_copy(m).wait()
        mom_store(m).wait()
        for cp in vec_stores(m):
            cp.wait()
    for cp in sends:
        cp.wait_send()


def split_rows(rows, parts):
    tiles = rows // SUB
    inner = tiles - 4
    out, start = [], 0
    for n in [2] + [inner // parts + (1 if i < inner % parts else 0) for i in range(parts)] + [2]:
        out.append((SUB * start, SUB * n))
        start += n
    return out


def turn_rows(sh, src, dst, row, rows):
    def body(t, carry):
        rs = pl.multiple_of(row + t * SUB, SUB)
        rd = pl.multiple_of(t * SUB, SUB)
        xs = [src[q, pl.ds(rs, SUB), :] for q in range(DP)]
        for k in range(DP):
            dst[k, pl.ds(rd, SUB), :] = jnp.concatenate([v[:, sh * k:sh * (k + 1)] for v in xs], axis=1)
        return carry

    lax.fori_loop(0, rows // SUB, body, 0)


def unpack_in_kernel(sh, work, count, src, *refs):
    small, dst, small_out = refs[0:count], refs[count], refs[count + 1:2 * count + 1]
    src_v, dst_v, in_sem, out_sem, small_sem, *small_v = refs[2 * count + 1:]
    ins, outs = src_v.shape[0], dst_v.shape[0]

    def load(s):
        r0, n = work[s]
        return pltpu.make_async_copy(src.at[:, pl.ds(r0, n), :], src_v.at[s % ins, :, pl.ds(0, n), :], in_sem.at[s % ins])

    def store(s):
        r0, n = work[s]
        return pltpu.make_async_copy(dst_v.at[s % outs, :, pl.ds(0, n), :], dst.at[:, pl.ds(r0, n), :], out_sem.at[s % outs])

    def small_in(k):
        return pltpu.make_async_copy(small[k], small_v[k], small_sem.at[0, k])

    def small_back(k):
        return pltpu.make_async_copy(small_v[k], small_out[k], small_sem.at[1, k])

    for s in range(ins - 1):
        load(s).start()
    for k in range(count):
        small_in(k).start()
    for s, (r0, n) in enumerate(work):
        if s + ins - 1 < len(work):
            load(s + ins - 1).start()
        load(s).wait()
        if s >= outs:
            store(s - outs).wait()
        turn_rows(sh, src_v.at[s % ins], dst_v.at[s % outs], 0, n)
        store(s).start()
        if s == ins:
            for k in range(count):
                small_in(k).wait()
                small_back(k).start()
    for s in range(len(work) - outs, len(work)):
        store(s).wait()
    for k in range(count):
        small_back(k).wait()


def early_kernel(ag, fa, fb, hold, sem):
    dp, c, chip, *chips = places()
    qx, qy, _ = (2 * j + c for j in chips)
    other = 1 - 2 * c
    half = fa.shape[0]
    lo, hi = pl.ds(0, half), pl.ds(half, fb.shape[0])
    copies = [(ag.at[q], hold.at[q]) for q in (dp, dp + other, qx + other, qy + other)]
    copies += [(fa, hold.at[qx, lo, :]), (ag.at[qx, hi, :], hold.at[qx, hi, :])]
    copies += [(ag.at[qy, lo, :], hold.at[qy, lo, :]), (fb, hold.at[qy, hi, :])]
    copies = [pltpu.make_async_copy(v, w, sem.at[e]) for e, (v, w) in enumerate(copies)]
    for cp in copies:
        cp.start()
    for cp in copies:
        cp.wait()


def late_kernel(sh, work, _, da, db, sa, sb, dst, hold, dst_v, in_sem, out_sem):
    *_, c, _, _, _, jd = places()
    half = da.shape[0]
    outs = dst_v.shape[0]

    def loads(s):
        r0, n = work[s]
        pair, first = ((da, sa), 0) if r0 < half else ((db, sb), half)
        blocks = 2 * jd + c, 2 * jd + 1 - c
        return [pltpu.make_async_copy(v.at[pl.ds(r0 - first, n), :], hold.at[q, pl.ds(r0, n), :], in_sem.at[s, e]) for e, (v, q) in enumerate(zip(pair, blocks))]

    def store(s):
        r0, n = work[s]
        return pltpu.make_async_copy(dst_v.at[s % outs, :, pl.ds(0, n), :], dst.at[:, pl.ds(r0, n), :], out_sem.at[s % outs])

    for s in range(len(work)):
        for cp in loads(s):
            cp.start()
    for s, (r0, n) in enumerate(work):
        for cp in loads(s):
            cp.wait()
        if s >= outs:
            store(s - outs).wait()
        turn_rows(sh, hold, dst_v.at[s % outs], r0, n)
        store(s).start()
    for s in range(len(work) - outs, len(work)):
        store(s).wait()


IN_HBM = pl.BlockSpec(memory_space=pl.ANY)
IN_VMEM = pl.BlockSpec(memory_space=pltpu.VMEM)


def costing(size):
    return pl.CostEstimate(flops=1000 * size, bytes_accessed=DP * size, transcendentals=0)


def unpack_in(packed, small, sh):
    work = split_rows(packed.shape[1], 13)
    nmax = max(n for _, n in work)
    count = len(small)
    dma = pltpu.SemaphoreType.DMA
    buf = (DP, nmax, packed.shape[2])
    return pl.pallas_call(
        lambda *refs: unpack_in_kernel(sh, work, count, *refs),
        in_specs=[IN_HBM] * (1 + count),
        out_specs=[IN_HBM] * (1 + count),
        out_shape=[jax.ShapeDtypeStruct(v.shape, v.dtype) for v in (packed, *small)],
        scratch_shapes=[pltpu.VMEM((4, *buf), F32), pltpu.VMEM((3, *buf), F32), dma((4,)), dma((3,)), dma((2, count))]
        + [pltpu.VMEM(v.shape, v.dtype) for v in small],
        compiler_params=pltpu.CompilerParams(vmem_limit_bytes=ALL_VMEM),
        cost_estimate=costing(packed.size),
        name='unpack_in',
    )(packed, *small)


def early_out(ag, fa, fb):
    return pl.pallas_call(
        early_kernel,
        in_specs=[IN_HBM] * 3,
        out_specs=IN_VMEM,
        out_shape=pltpu.VMEM(ag.shape, F32),
        scratch_shapes=[pltpu.SemaphoreType.DMA((DP,))],
        compiler_params=pltpu.CompilerParams(vmem_limit_bytes=BESIDE_HOLD),
        cost_estimate=costing(ag.size),
        name='early_out',
    )(ag, fa, fb)


def late_out(hold, da, db, sa, sb, sh):
    ra, shape = da.shape[0], hold.shape
    work = split_rows(ra, 4) + [(ra + r0, n) for r0, n in split_rows(shape[1] - ra, 4)]
    nmax = max(n for _, n in work)
    dma = pltpu.SemaphoreType.DMA
    return pl.pallas_call(
        lambda *refs: late_kernel(sh, work, *refs),
        in_specs=[IN_VMEM] + [IN_HBM] * 4,
        out_specs=[IN_HBM, IN_VMEM],
        out_shape=[jax.ShapeDtypeStruct(shape, F32), pltpu.VMEM(shape, F32)],
        input_output_aliases={0: 1},
        scratch_shapes=[pltpu.VMEM((4, DP, nmax, shape[2]), F32), dma((len(work), 2)), dma((4,))],
        compiler_params=pltpu.CompilerParams(vmem_limit_bytes=BESIDE_HOLD),
        name='late_out',
    )(hold, da, db, sa, sb)[0]


def solution(mesh):
    tp_devs = mesh.shape['tp']

    def body(w_in, w_out, g_in, g_out, m_in, m_out, r_in, c_in, r_out, c_out, learn_rate, weight_decay, beta_two):
        width = w_in.shape[1]
        sh = width // 8
        mats = (Mat(w_in.shape[2], width, tp_devs, True), Mat(w_out.shape[1], width, tp_devs, False))
        a, o = mats

        def grouped(v, m):
            return v.reshape(8, m.r, width)

        scal = [v.reshape(1, 1) for v in (learn_rate, weight_decay, beta_two)]
        args = list(scal)
        args += [grouped(g_in[0, 0].T, a), grouped(w_in[0].T, a), m_in[0], r_in, c_in]
        args += [grouped(g_out[0, 0], o), grouped(w_out[0], o), m_out[0].T, c_out, r_out]
        sspec = pl.BlockSpec(memory_space=pltpu.SMEM)
        in_specs = [sspec] * 3 + [IN_HBM] * 10
        out_shape, out_specs = [], []
        for m in mats:
            big = jax.ShapeDtypeStruct((m.r, width), F32)
            out_shape += [jax.ShapeDtypeStruct((8, m.r, width), F32), jax.ShapeDtypeStruct((sh, m.k), BF16),
                          jax.ShapeDtypeStruct((1, sh), F32), jax.ShapeDtypeStruct((1, m.k), F32),
                          jax.ShapeDtypeStruct((4, m.r, width), F32), big, big, big,
                          jax.ShapeDtypeStruct((m.ra, width), F32), jax.ShapeDtypeStruct((m.r - m.ra, width), F32)]
            out_specs += [IN_HBM] * 10
        nmax = max(m.nmax for m in mats)
        dma = pltpu.SemaphoreType.DMA
        scratch = [pltpu.VMEM((2, 2, 4, nmax, width), F32), pltpu.VMEM((2, 8, nmax, 384), F32), pltpu.VMEM((SUB, LANES), F32), pltpu.VMEM((SUB, LANES), F32), dma((2, 2)), dma((2,))]
        for m in mats:
            gt_rows = 12 * m.r
            scratch += [pltpu.VMEM((4, m.r, width), F32), pltpu.VMEM((gt_rows, 256), F32), pltpu.VMEM((sh, LANES * m.tiles), F32),
                        pltpu.VMEM((sh, m.k), BF16), pltpu.VMEM((SUB, LANES * m.tiles), F32), pltpu.VMEM((m.kr, LANES), F32),
                        pltpu.VMEM((EVERY, m.kr, LANES), F32), pltpu.VMEM((sh, LANES), F32), pltpu.VMEM((sh, LANES), F32),
                        pltpu.VMEM((SUB, LANES), F32), pltpu.VMEM((EVERY, SUB, LANES), F32),
                        pltpu.VMEM((SUB, sh), F32), pltpu.VMEM((SUB, m.k), F32), pltpu.VMEM((sh, LANES), F32), pltpu.VMEM((sh, LANES), F32),
                        pltpu.VMEM((m.kr, LANES), F32), pltpu.VMEM((m.kr, LANES), F32)]
            scratch += [dma((2, NCH)), dma((2, NCH)), dma((2, NCH)), dma((2, NCH)), dma((2,)), dma((2, EVERY)), dma((2,)), dma((2, EVERY)),
                        dma((2, NCH)), dma((2, NCH)), dma((2, NCH)), dma((2, 4, NCH)), dma((5,))]
        outs = pl.pallas_call(
            lambda *refs: main_kernel(mats, sh, *refs),
            in_specs=in_specs,
            out_specs=out_specs,
            out_shape=out_shape,
            scratch_shapes=scratch,
            compiler_params=pltpu.CompilerParams(has_side_effects=True, vmem_limit_bytes=ALL_VMEM),
            name='step',
        )(*args)
        first, second = outs[0:4], outs[10:14]
        fa, fb = outs[18:]
        chips = mesh.shape['dp'] // 2

        def swap(v, bit):
            return lax.ppermute(v, 'dp', [(q, q ^ bit) for q in range(2 * chips)])

        da, db = swap(fa, 4), swap(fb, 2)
        done = unpack_in(first[0], (*first[1:], *second[1:]), sh)
        fa, fb, small = lax.optimization_barrier((fa, fb, done[2]))
        hold = early_out(second[0], fa, fb)
        da, db, hold = lax.optimization_barrier((da, db, hold))
        sa, sb = swap(da, 1), swap(db, 1)
        new_in = done[0].reshape(a.k, width).T[None]
        new_out = late_out(hold, da, db, sa, sb, sh).reshape(o.k, width)[None]
        mom_in, _, col_in, mom_out, row_out, col_out = done[1:]
        return (new_in, new_out, mom_in[None], mom_out.T[None], small, col_in, col_out, row_out)

    free = None
    rows_tp, cols_tp = P(free, 'tp', free), P(free, free, 'tp')
    on_dp, on_tp, whole = P(free, 'dp'), P(free, 'tp'), P()
    state_in, state_out = P(free, 'dp', 'tp'), P(free, 'tp', 'dp')
    in_specs = (cols_tp, rows_tp, P('dp', free, free, 'tp'), P('dp', free, 'tp', free), state_in, state_out, on_dp, on_tp, on_tp, on_dp, whole, whole, whole)
    out_specs = (cols_tp, rows_tp, state_in, state_out, on_dp, on_tp, on_tp, on_dp)
    return jax.shard_map(body, mesh=mesh, in_specs=in_specs, out_specs=out_specs, check_vma=False)
```

```python
import jax
import jax.numpy as jnp
from jax import lax
from jax.experimental import pallas as pl
from jax.experimental.pallas import tpu as pltpu
from jax.sharding import PartitionSpec as P

F32 = jnp.float32
LANES = 128
SUB = 8
DP = 8
EVERY = 16
ALL_VMEM = 67043328
BESIDE_HOLD = 45000000
BF16 = jnp.bfloat16
MESH = pl.DeviceIdType.MESH
NCH = 8
WINDOW = 384
ORDER = (0, 4, 1, 5, 2, 6, 3, 7)


def chunk_rows(rows, small_last):
    tiles = rows // SUB
    out, start = [], 0
    for part in ((tiles + 1) // 2, tiles // 2):
        sizes = [part // 9, part * 3 // 10, part * 7 // 20]
        sizes.append(part - sum(sizes))
        for n in sizes[::-1] if small_last and out else sizes:
            out.append((SUB * start, SUB * n))
            start += n
    return out


def lane_chunks(total):
    width = SUB * LANES
    out = [(s, width) for s in range(0, total - width, width)]
    last = len(out) * width
    if total - last < width // 4:
        s, n = out.pop()
        return out + [(s, n + total - last)]
    return out + [(last, total - last)]


class Mat:
    def __init__(self, kloc, width, tp, row_is_r):
        self.k, self.width, self.sh = kloc, width, width // DP
        self.r = kloc // DP
        self.ktot = kloc * tp
        self.row_is_r = row_is_r
        self.ch = chunk_rows(self.r, not row_is_r)
        self.tiles = (kloc + 127) // LANES
        self.kr = (self.tiles + SUB) // SUB * SUB
        self.nmax = max(n for _, n in self.ch)
        self.ra = self.ch[4][0]
        self.keep = not row_is_r


def rcopy(src, dst, sems, dev):
    if sems[0].shape:
        ref, *at = sems
        sems = ref.at[(0, *at)], ref.at[(1, *at)]
    return pltpu.make_async_remote_copy(src_ref=src, dst_ref=dst, send_sem=sems[0], recv_sem=sems[1], device_id=dev, device_id_type=MESH)


def places():
    dp = lax.axis_index('dp')
    c, chip = lax.rem(dp, 2), lax.div(dp, 2)
    x, y = lax.rem(chip, 2), lax.div(chip, 2)
    return dp, c, chip, chip + 1 - 2 * x, chip + 2 - 4 * y, 3 - chip


def main_kernel(mats, sh, *refs):
    it = iter(refs)
    lr_ref, wd_ref, b2_ref = next(it), next(it), next(it)
    for m in mats:
        m.g, m.w, m.mom, m.row_arg, m.col_arg = (next(it) for _ in range(5))
    for m in mats:
        (m.ag, m.mom_new, m.row_out, m.col_out, m.d2d, m.xy1, m.x2, m.y2, m.fa, m.fb) = (next(it) for _ in range(10))
    stage, wst, usq, ucol = next(it), next(it), next(it), next(it)
    ld_sem, w_sem = next(it), next(it)
    for m in mats:
        (m.p, m.gt, m.gn, m.mv, m.colacc, m.msg, m.slots, m.rp, m.rz, m.sc, m.slots2, m.row_raw, m.col_raw, m.row_old, m.row_new, m.col_old, m.col_new) = (next(it) for _ in range(17))
        (m.d2d_s, m.rs1_s, m.x2_s, m.y2_s, m.ex_s, m.msg_s, m.z_s, m.sc_s, m.agx_s, m.agy_s, m.agd_s, m.ags_s, m.loc_s) = (next(it) for _ in range(13))
    tp = lax.axis_index('tp')
    dp, c, chip, jx, jy, jd = places()
    qx, qy, qd, qs = 2 * jx + c, 2 * jy + c, 2 * jd + c, dp + 1 - 2 * c
    sib, xn, yn = {'tp': tp, 'dp': qs}, {'tp': tp, 'dp': qx}, {'tp': tp, 'dp': qy}
    zn = {'tp': 1 - tp, 'dp': dp}
    me16 = tp * DP + dp

    sends = []

    def start(cp):
        cp.start()
        sends.append(cp)

    def d2d_copy(m, i):
        r0, n = m.ch[i]
        return rcopy(m.g.at[pl.ds(4 * (1 - c), 4), pl.ds(r0, n), :], m.d2d.at[:, pl.ds(r0, n), :], (m.d2d_s, i), sib)

    def own_load(m, i, b):
        r0, n = m.ch[i]
        return pltpu.make_async_copy(m.g.at[pl.ds(4 * c, 4), pl.ds(r0, n), :], stage.at[b, 0, :, pl.ds(0, n), :], ld_sem.at[b, 0])

    def got_load(m, i, b):
        r0, n = m.ch[i]
        return pltpu.make_async_copy(m.d2d.at[:, pl.ds(r0, n), :], stage.at[b, 1, :, pl.ds(0, n), :], ld_sem.at[b, 1])

    def pack_chunk(m, i, b):
        r0, n = m.ch[i]
        own_load(m, i, b).wait()
        got_load(m, i, b).wait()

        def body(t, carry):
            rs = pl.multiple_of(t * SUB, SUB)
            rd = pl.multiple_of(r0 + t * SUB, SUB)
            xs = [stage[b, 0, k, pl.ds(rs, SUB), :] + stage[b, 1, k, pl.ds(rs, SUB), :] for k in range(4)]
            for j in range(4):
                parts = [xs[k][:, sh * (2 * j + cc):sh * (2 * j + cc + 1)] for cc in range(2) for k in range(4)]
                m.p[j, pl.ds(rd, SUB), :] = jnp.concatenate(parts, axis=1)
            return carry

        lax.fori_loop(0, n // SUB, body, 0)

    def pview(m, j, i):
        r0, n = m.ch[i]
        return m.p.at[j, pl.ds(r0, n), :]

    def hview(ref, m, i):
        r0, n = m.ch[i]
        return ref.at[pl.ds(r0, n), :]

    def rs1_copy(m, i):
        dev = xn if i < 4 else yn
        return rcopy(pview(m, jd, i), hview(m.xy1, m, i), (m.rs1_s, i), dev)

    def x2_copy(m, i):
        return rcopy(pview(m, jx, i), hview(m.x2, m, i), (m.x2_s, i), xn)

    def y2_copy(m, i):
        return rcopy(pview(m, jy, i), hview(m.y2, m, i), (m.y2_s, i), yn)

    def rs_free(m, i):
        start(x2_copy(m, i) if i < 4 else y2_copy(m, i))

    def rs_pack(m, send):
        own_load(m, ORDER[0], 0).start()
        for s, i in enumerate(ORDER):
            d2d_copy(m, i).wait_recv()
            got_load(m, i, s % 2).start()
            if s + 1 < NCH:
                own_load(m, ORDER[s + 1], (s + 1) % 2).start()
            pack_chunk(m, i, s % 2)
            if send:
                start(rs1_copy(m, i))
                if s < 4:
                    rs_free(m, i)

    def rs_dep(m, ids):
        def load(s):
            i = ids[s]
            r0, n = m.ch[i]
            return pltpu.make_async_copy(hview(m.xy1, m, i), stage.at[s % 2, 0, 0, pl.ds(0, n), :], ld_sem.at[s % 2, 0])

        for s, i in enumerate(ids):
            r0, n = m.ch[i]
            rs1_copy(m, i).wait_recv()
            load(s).start()
            load(s).wait()
            j = jy if i < 4 else jx

            def body(t, carry):
                rs = pl.multiple_of(t * SUB, SUB)
                rd = pl.multiple_of(r0 + t * SUB, SUB)
                m.p[j, pl.ds(rd, SUB), :] = m.p[j, pl.ds(rd, SUB), :] + stage[s % 2, 0, 0, pl.ds(rs, SUB), :]
                return carry

            lax.fori_loop(0, n // SUB, body, 0)
            start(y2_copy(m, i) if i < 4 else x2_copy(m, i))

    def acc_own(m, ids):
        base = (2 * c * (4 * m.r), (2 - c) * (4 * m.r))

        def loads(s):
            i = ids[s]
            r0, n = m.ch[i]
            b = s % 2
            return (pltpu.make_async_copy(hview(m.x2, m, i), stage.at[b, 0, 0, pl.ds(0, n), :], ld_sem.at[b, 0]),
                    pltpu.make_async_copy(hview(m.y2, m, i), stage.at[b, 0, 1, pl.ds(0, n), :], ld_sem.at[b, 1]))

        for s, i in enumerate(ids):
            r0, n = m.ch[i]
            b = s % 2
            x2_copy(m, i).wait_recv()
            y2_copy(m, i).wait_recv()
            la, lb = loads(s)
            la.start()
            lb.start()
            la.wait()
            lb.wait()

            def body(t, carry):
                rs = pl.multiple_of(t * SUB, SUB)
                rd = pl.multiple_of(r0 + t * SUB, SUB)
                v = m.p[chip, pl.ds(rd, SUB), :] + stage[b, 0, 0, pl.ds(rs, SUB), :] + stage[b, 0, 1, pl.ds(rs, SUB), :]
                for cc in range(2):
                    for k in range(4):
                        row = pl.multiple_of(base[cc] + k * m.r + r0 + t * SUB, SUB)
                        m.gt[pl.ds(row, SUB), 0:sh] = v[:, sh * (4 * cc + k):sh * (4 * cc + k + 1)]
                return carry

            lax.fori_loop(0, n // SUB, body, 0)

    def ex_copy(m):
        h = 4 * m.r
        return rcopy(m.gt.at[pl.ds(2 * h, h), :], m.gt.at[pl.ds(c * h, h), :], (m.ex_s,), sib)

    def ex_wait(m):
        h = 4 * m.r
        rcopy(m.gt.at[pl.ds(2 * h, h), :], m.gt.at[pl.ds((1 - c) * h, h), :], (m.ex_s,), sib).wait_recv()

    def to_gn(m):
        full = m.k // LANES

        def body(t, carry):
            o = pl.multiple_of(t * LANES, LANES)
            m.gn[:, pl.ds(o, LANES)] = m.gt[pl.ds(o, LANES), :].T[0:sh, :]
            return carry

        lax.fori_loop(0, full, body, 0)
        rest = m.k - full * LANES
        if rest:
            m.gn[:, full * LANES:m.k] = m.gt[full * LANES:full * LANES + LANES, :].T[0:sh, 0:rest]

    def from_gn(m):
        full = m.k // LANES
        pad = m.gt.shape[1] - sh

        def turn(v):
            return jnp.concatenate([v, jnp.zeros((pad, LANES), F32)], axis=0).T

        def body(t, carry):
            o = pl.multiple_of(t * LANES, LANES)
            m.gt[pl.ds(o, LANES), :] = turn(m.gn[:, pl.ds(o, LANES)])
            return carry

        lax.fori_loop(0, full, body, 0)
        rest = m.k - full * LANES
        if rest:
            v = jnp.concatenate([m.gn[:, full * LANES:m.k], jnp.zeros((sh, LANES - rest), F32)], axis=1)
            m.gt[full * LANES:m.k, :] = turn(v)[0:rest, :]

    def vec_loads(m):
        return (pltpu.make_async_copy(m.row_arg, m.row_raw.at[pl.ds(0, 1), :], m.loc_s.at[3]),
                pltpu.make_async_copy(m.col_arg, m.col_raw.at[pl.ds(0, 1), :], m.loc_s.at[4]))

    def vec_stores(m):
        return (pltpu.make_async_copy(m.row_raw.at[pl.ds(0, 1), :], m.row_out, m.loc_s.at[3]),
                pltpu.make_async_copy(m.col_raw.at[pl.ds(0, 1), :], m.col_out, m.loc_s.at[4]))

    def vec_prepare(m):
        for cp in vec_loads(m):
            cp.wait()
        pad = m.gt.shape[1] - sh
        row = jnp.concatenate([m.row_raw[0:1, :], jnp.zeros((1, pad), F32)], axis=1)
        m.row_old[...] = jnp.broadcast_to(row, (LANES, sh + pad)).T[0:sh, :]
        m.col_old[...] = jnp.zeros_like(m.col_old)
        for t in range(m.tiles):
            w = min(LANES, m.k - LANES * t)
            m.col_old[t:t + 1, 0:w] = m.col_raw[0:1, LANES * t:LANES * t + w]

    def vec_finish(m):
        pad = m.gt.shape[1] - sh
        m.row_raw[...] = jnp.concatenate([m.row_new[...], jnp.zeros((pad, LANES), F32)], axis=0).T[0:SUB, 0:sh]
        for t in range(m.tiles):
            w = min(LANES, m.k - LANES * t)
            m.col_raw[0:1, LANES * t:LANES * t + w] = m.col_new[t:t + 1, 0:w]
        for cp in vec_stores(m):
            cp.start()

    def peers():
        out = []
        for d in range(1, DP):
            q = lax.rem(dp + d, DP)
            out.append((True, tp, q))
        for d in range(DP):
            q = lax.rem(dp + d, DP)
            out.append((False, 1 - tp, q))
        return out

    def msg_copies(m, sending):
        out = []
        for n, (same, t, q) in enumerate(peers()):
            slot = me16 if sending else t * SUB + q
            dev = {'tp': t, 'dp': q}
            sems = m.msg_s.at[0, n], m.msg_s.at[1, slot]
            rows = pl.ds(0, m.tiles + 1) if same else pl.ds(m.tiles, 1)
            out.append(rcopy(m.msg.at[rows, :], m.slots.at[slot, rows, :], sems, dev))
        return out

    def z_copy(m):
        return rcopy(m.rp, m.rz, (m.z_s,), zn)

    def sc_copies(m, sending):
        out = []
        for n, (same, t, q) in enumerate(peers()):
            slot = me16 if sending else t * SUB + q
            out.append(rcopy(m.sc.at[pl.ds(0, 1), :], m.slots2.at[slot, pl.ds(0, 1), :], (m.sc_s.at[0, n], m.sc_s.at[1, slot]), {'tp': t, 'dp': q}))
        return out

    def stats1(m):
        b2 = b2_ref[0, 0]
        m.colacc[...] = jnp.zeros_like(m.colacc)

        def body(t, carry):
            rr = pl.multiple_of(t * SUB, SUB)
            rsum = jnp.zeros((DP, 1), F32)
            for s0, w in lane_chunks(m.k):
                g = m.gn[pl.ds(rr, SUB), s0:s0 + w]
                sq = g * g + 1e-30
                m.colacc[:, s0:s0 + w] = m.colacc[:, s0:s0 + w] + sq
                rsum = rsum + jnp.sum(sq, axis=1, keepdims=True)
            m.rp[pl.ds(rr, SUB), :] = jnp.broadcast_to(rsum, (SUB, LANES))
            return carry

        lax.fori_loop(0, sh // SUB, body, 0)
        for i in range(m.tiles):
            w = min(LANES, m.k - LANES * i)
            m.msg[i:i + 1, 0:w] = jnp.sum(m.colacc[:, LANES * i:LANES * i + w], axis=0, keepdims=True)
        mean_s = jnp.sum(m.rp[...] * (1.0 / m.ktot), axis=0, keepdims=True) * (1.0 / m.width)
        if m.row_is_r:
            old = jnp.sum(m.row_old[...], axis=0, keepdims=True) * (0.5 / m.width)
        else:
            old = jnp.sum(jnp.sum(m.col_old[...], axis=0, keepdims=True), axis=1, keepdims=True) * (0.125 / m.ktot)
        m.msg[m.tiles:m.tiles + 1, :] = jnp.broadcast_to(b2 * old + (1.0 - b2) * mean_s, (1, LANES))
        m.slots[me16, :, :] = m.msg[...]
        for cp in msg_copies(m, True):
            start(cp)
        start(z_copy(m))

    def stats2(m):
        b2 = b2_ref[0, 0]
        for cp in msg_copies(m, False):
            cp.wait_recv()
        z_copy(m).wait_recv()
        tot = m.slots[tp * DP, 0:m.kr, :]
        for q in range(1, DP):
            tot = tot + m.slots[tp * DP + q, 0:m.kr, :]
        m.col_new[...] = b2 * m.col_old[...] + (1.0 - b2) * (tot / float(m.width))
        m.row_new[...] = b2 * m.row_old[...] + (1.0 - b2) * ((m.rp[...] + m.rz[...]) / float(m.ktot))
        mean_r = m.slots[0, m.tiles:m.tiles + 1, :]
        for q in range(1, EVERY):
            mean_r = mean_r + m.slots[q, m.tiles:m.tiles + 1, :]
        mean_r = mean_r[:, 0:1]
        usq[...] = jnp.zeros_like(usq)
        ucol[...] = jnp.zeros_like(ucol)

        def body(t, carry):
            rr = pl.multiple_of(t * SUB, SUB)
            rv = m.row_new[pl.ds(rr, SUB), 0:1]
            acc = jnp.zeros((DP, 1), F32)
            for i in range(m.tiles):
                s0, w = LANES * i, min(LANES, m.k - LANES * i)
                second = rv * m.col_new[i:i + 1, 0:w] / mean_r
                u = m.gn[pl.ds(rr, SUB), s0:s0 + w] / jnp.sqrt(second)
                m.gn[pl.ds(rr, SUB), s0:s0 + w] = u
                if w == LANES:
                    usq[...] = usq[...] + u * u
                else:
                    acc = acc + jnp.sum(u * u, axis=1, keepdims=True)
            ucol[...] = ucol[...] + jnp.broadcast_to(acc, (SUB, LANES))
            return carry

        lax.fori_loop(0, sh // SUB, body, 0)
        usum = jnp.sum(jnp.sum(usq[...], axis=1, keepdims=True), axis=0, keepdims=True)
        usum = usum + jnp.sum(ucol[:, 0:1], axis=0, keepdims=True)
        m.sc[...] = jnp.broadcast_to(usum, (SUB, LANES))
        m.slots2[me16, :, :] = m.sc[...]
        for cp in sc_copies(m, True):
            start(cp)

    def stats3(m):
        for cp in sc_copies(m, False):
            cp.wait_recv()
        tot = m.slots2[0, 0:1, :]
        for q in range(1, EVERY):
            tot = tot + m.slots2[q, 0:1, :]
        den = jnp.maximum(1.0, jnp.sqrt(tot / (float(m.width) * float(m.ktot))))[0:1, 0:1]
        mom_load(m).wait()

        def body(t, carry):
            rr = pl.multiple_of(t * 16, 16)
            for s0, w in lane_chunks(m.k):
                u = m.gn[pl.ds(rr, 16), s0:s0 + w] / den
                mn = (0.9 * m.mv[pl.ds(rr, 16), s0:s0 + w].astype(F32) + 0.1 * u).astype(BF16)
                m.mv[pl.ds(rr, 16), s0:s0 + w] = mn
                m.gn[pl.ds(rr, 16), s0:s0 + w] = mn.astype(F32)
            return carry

        lax.fori_loop(0, sh // 16, body, 0)
        mom_store(m).start()
        from_gn(m)

    def mom_load(m):
        return pltpu.make_async_copy(m.mom, m.mv, m.loc_s.at[0])

    def mom_store(m):
        return pltpu.make_async_copy(m.mv, m.mom_new, m.loc_s.at[1])

    def own_copy(m):
        return pltpu.make_async_copy(m.p.at[chip], m.ag.at[dp], m.loc_s.at[2])

    lane0 = jnp.minimum(lax.div(sh * dp, LANES), DP)
    off = sh * dp - lane0 * LANES

    def w_load(m, i, b):
        r0, n = m.ch[i]
        return pltpu.make_async_copy(m.w.at[:, pl.ds(r0, n), pl.ds(pl.multiple_of(lane0 * LANES, LANES), WINDOW)], wst.at[b, :, pl.ds(0, n), :], w_sem.at[b])

    def new_weights(m):
        lr, wd = lr_ref[0, 0], wd_ref[0, 0]
        w_load(m, 0, 0).start()
        for i in range(NCH):
            r0, n = m.ch[i]
            b = i % 2
            if i + 1 < NCH:
                w_load(m, i + 1, 1 - b).start()
            w_load(m, i, b).wait()

            def body(t, carry):
                rs = pl.multiple_of(t * SUB, SUB)
                rd = pl.multiple_of(r0 + t * SUB, SUB)
                heads, tails = [], []
                for k in range(DP):
                    w = pltpu.roll(wst[b, k, pl.ds(rs, SUB), :], lax.rem(WINDOW - off, WINDOW), 1)[:, 0:sh]
                    mt = m.gt[pl.ds(pl.multiple_of(k * m.r + r0 + t * SUB, SUB), DP), 0:sh]
                    new = w - lr * mt - lr * wd * w
                    heads.append(pltpu.roll(new[:, 0:LANES], lax.rem(sh * dp, LANES), 1))
                    tails.append(new[:, LANES:sh])
                m.p[chip, pl.ds(rd, SUB), :] = jnp.concatenate(heads + tails, axis=1)
                return carry

            lax.fori_loop(0, n // SUB, body, 0)

    def agrow(m, q, i):
        r0, n = m.ch[i]
        return m.ag.at[q, pl.ds(r0, n), :]

    def xrow(m, q, i):
        r0, n = m.ch[i]
        return m.fa.at[pl.ds(r0, n), :] if m.keep and i < 4 else agrow(m, q, i)

    def yrow(m, q, i):
        r0, n = m.ch[i]
        return m.fb.at[pl.ds(r0 - m.ra, n), :] if m.keep and i >= 4 else agrow(m, q, i)

    def ag_own(m, i):
        start(rcopy(pview(m, chip, i), xrow(m, dp, i), (m.agx_s, i), xn))
        start(rcopy(pview(m, chip, i), yrow(m, dp, i), (m.agy_s, i), yn))

    def ag_sib_own(m, i):
        start(rcopy(pview(m, chip, i), agrow(m, dp, i), (m.ags_s, 0, i), sib))

    def ag_sib(m, which, src, q, i):
        start(rcopy(src, agrow(m, q, i), (m.ags_s, which, i), sib))

    def ag_xy(m, i):
        fx, fy = xrow(m, qx, i), yrow(m, qy, i)
        rcopy(fx, fx, (m.agx_s, i), xn).wait_recv()
        rcopy(fy, fy, (m.agy_s, i), yn).wait_recv()
        if not m.keep:
            if i < 4:
                start(rcopy(fx, fx, (m.agd_s, i), yn))
            else:
                start(rcopy(fy, fy, (m.agd_s, i), xn))
        ag_sib(m, 1, fx, qx, i)
        ag_sib(m, 2, fy, qy, i)

    def ag_d(m, i):
        rcopy(agrow(m, qd, i), agrow(m, qd, i), (m.agd_s, i), xn).wait_recv()
        ag_sib(m, 3, agrow(m, qd, i), qd, i)

    def ag_end(m):
        blocks = (qs, qx + 1 - 2 * c, qy + 1 - 2 * c, qd + 1 - 2 * c)
        for which, q in enumerate(blocks[0:3] if m.keep else blocks):
            for i in range(NCH):
                rcopy(agrow(m, q, i), agrow(m, q, i), (m.ags_s, which, i), sib).wait_recv()

    a, o = mats
    for i in ORDER:
        start(d2d_copy(a, i))
    rs_pack(a, True)
    for i in ORDER[4:]:
        rs_free(a, i)
    for i in ORDER:
        start(d2d_copy(o, i))
    for m in mats:
        mom_load(m).start()
        for cp in vec_loads(m):
            cp.start()
    rs_dep(a, ORDER)
    rs_pack(o, False)
    for m in mats:
        vec_prepare(m)
    for i in ORDER[0:6]:
        start(rs1_copy(o, i))
    acc_own(a, ORDER)
    start(ex_copy(a))
    ex_wait(a)
    to_gn(a)
    stats1(a)
    for i in ORDER[6:]:
        start(rs1_copy(o, i))
    for i in ORDER[0:2]:
        rs_free(o, i)
    stats2(a)
    for i in ORDER[2:4]:
        rs_free(o, i)
    stats3(a)
    for i in ORDER[4:]:
        rs_free(o, i)
    new_weights(a)
    vec_finish(a)
    own_copy(a).start()
    rs_dep(o, ORDER)
    for i in range(2):
        ag_own(a, i)
    for i in range(NCH):
        ag_sib_own(a, i)
    acc_own(o, ORDER)
    start(ex_copy(o))
    ex_wait(o)
    to_gn(o)
    stats1(o)
    for i in range(2, 4):
        ag_own(a, i)
    stats2(o)
    for i in range(4, 6):
        ag_own(a, i)
    stats3(o)
    for i in range(6, DP):
        ag_own(a, i)
    new_weights(o)
    vec_finish(o)
    own_copy(o).start()
    for i in range(NCH):
        ag_sib_own(o, i)
    for i in range(NCH):
        ag_xy(a, i)
    for i in range(NCH):
        ag_own(o, i)
    for i in range(NCH):
        ag_d(a, i)
    for i in range(NCH):
        ag_xy(o, i)
    for m in mats:
        ag_end(m)
        own_copy(m).wait()
        mom_store(m).wait()
        for cp in vec_stores(m):
            cp.wait()
    for cp in sends:
        cp.wait_send()


def split_rows(rows, parts):
    tiles = rows // SUB
    inner = tiles - 4
    out, start = [], 0
    for n in [2] + [inner // parts + (1 if i < inner % parts else 0) for i in range(parts)] + [2]:
        out.append((SUB * start, SUB * n))
        start += n
    return out


def turn_rows(sh, src, dst, row, rows):
    extra = sh - LANES
    tiles = DP * sh // LANES

    def tile(t):
        return pl.ds(LANES * t, LANES)

    def body(t, carry):
        lane = lax.broadcasted_iota(jnp.int32, (SUB, LANES), 1)
        rs = pl.ds(pl.multiple_of(row + t * SUB, SUB), SUB)
        rd = pl.ds(pl.multiple_of(t * SUB, SUB), SUB)
        ends = [[src[q, rs, tile(e)] for e in range(DP, tiles)] for q in range(DP)]
        for k in range(DP):
            out = [None] * tiles

            def place(v, lo, hi):
                for e in range(lo // LANES, (hi - 1) // LANES + 1):
                    at = max(lo - LANES * e, 0)
                    out[e] = v if out[e] is None else jnp.where(lane >= at, v, out[e])

            first, last = extra * k // LANES, (extra * (k + 1) - 1) // LANES
            for q in range(DP):
                place(src[q, rs, tile(k)], sh * q, sh * q + LANES)
                v = ends[q][first]
                if last > first:
                    v = jnp.where(lane >= extra * k % LANES, v, ends[q][last])
                turn = extra * (q - k) % LANES
                if turn:
                    v = pltpu.roll(v, turn, 1)
                place(v, sh * q + LANES, sh * (q + 1))
            for e in range(tiles):
                dst[k, rd, tile(e)] = out[e]
        return carry

    lax.fori_loop(0, rows // SUB, body, 0)


def unpack_in_kernel(sh, work, count, src, *refs):
    small, dst, small_out = refs[0:count], refs[count], refs[count + 1:2 * count + 1]
    src_v, dst_v, in_sem, out_sem, small_sem, *small_v = refs[2 * count + 1:]
    ins, outs = src_v.shape[0], dst_v.shape[0]

    def load(s):
        r0, n = work[s]
        return pltpu.make_async_copy(src.at[:, pl.ds(r0, n), :], src_v.at[s % ins, :, pl.ds(0, n), :], in_sem.at[s % ins])

    def store(s):
        r0, n = work[s]
        return pltpu.make_async_copy(dst_v.at[s % outs, :, pl.ds(0, n), :], dst.at[:, pl.ds(r0, n), :], out_sem.at[s % outs])

    def small_in(k):
        return pltpu.make_async_copy(small[k], small_v[k], small_sem.at[0, k])

    def small_back(k):
        return pltpu.make_async_copy(small_v[k], small_out[k], small_sem.at[1, k])

    for s in range(ins - 1):
        load(s).start()
    for k in range(count):
        small_in(k).start()
    for s, (r0, n) in enumerate(work):
        if s + ins - 1 < len(work):
            load(s + ins - 1).start()
        load(s).wait()
        if s >= outs:
            store(s - outs).wait()
        turn_rows(sh, src_v.at[s % ins], dst_v.at[s % outs], 0, n)
        store(s).start()
        if s == ins:
            for k in range(count):
                small_in(k).wait()
                small_back(k).start()
    for s in range(len(work) - outs, len(work)):
        store(s).wait()
    for k in range(count):
        small_back(k).wait()


def early_kernel(ag, fa, fb, hold, sem):
    dp, c, chip, *chips = places()
    qx, qy, _ = (2 * j + c for j in chips)
    other = 1 - 2 * c
    half = fa.shape[0]
    lo, hi = pl.ds(0, half), pl.ds(half, fb.shape[0])
    copies = [(ag.at[q], hold.at[q]) for q in (dp, dp + other, qx + other, qy + other)]
    copies += [(fa, hold.at[qx, lo, :]), (ag.at[qx, hi, :], hold.at[qx, hi, :])]
    copies += [(ag.at[qy, lo, :], hold.at[qy, lo, :]), (fb, hold.at[qy, hi, :])]
    copies = [pltpu.make_async_copy(v, w, sem.at[e]) for e, (v, w) in enumerate(copies)]
    for cp in copies:
        cp.start()
    for cp in copies:
        cp.wait()


def late_kernel(sh, work, _, da, db, sa, sb, dst, hold, dst_v, in_sem, out_sem):
    *_, c, _, _, _, jd = places()
    half = da.shape[0]
    outs = dst_v.shape[0]

    def loads(s):
        r0, n = work[s]
        pair, first = ((da, sa), 0) if r0 < half else ((db, sb), half)
        blocks = 2 * jd + c, 2 * jd + 1 - c
        return [pltpu.make_async_copy(v.at[pl.ds(r0 - first, n), :], hold.at[q, pl.ds(r0, n), :], in_sem.at[s, e]) for e, (v, q) in enumerate(zip(pair, blocks))]

    def store(s):
        r0, n = work[s]
        return pltpu.make_async_copy(dst_v.at[s % outs, :, pl.ds(0, n), :], dst.at[:, pl.ds(r0, n), :], out_sem.at[s % outs])

    for s in range(len(work)):
        for cp in loads(s):
            cp.start()
    for s, (r0, n) in enumerate(work):
        for cp in loads(s):
            cp.wait()
        if s >= outs:
            store(s - outs).wait()
        turn_rows(sh, hold, dst_v.at[s % outs], r0, n)
        store(s).start()
    for s in range(len(work) - outs, len(work)):
        store(s).wait()


IN_HBM = pl.BlockSpec(memory_space=pl.ANY)
IN_VMEM = pl.BlockSpec(memory_space=pltpu.VMEM)


def costing(size):
    return pl.CostEstimate(flops=1000 * size, bytes_accessed=DP * size, transcendentals=0)


def unpack_in(packed, small, sh):
    work = split_rows(packed.shape[1], 13)
    nmax = max(n for _, n in work)
    count = len(small)
    dma = pltpu.SemaphoreType.DMA
    buf = (DP, nmax, packed.shape[2])
    return pl.pallas_call(
        lambda *refs: unpack_in_kernel(sh, work, count, *refs),
        in_specs=[IN_HBM] * (1 + count),
        out_specs=[IN_HBM] * (1 + count),
        out_shape=[jax.ShapeDtypeStruct(v.shape, v.dtype) for v in (packed, *small)],
        scratch_shapes=[pltpu.VMEM((4, *buf), F32), pltpu.VMEM((3, *buf), F32), dma((4,)), dma((3,)), dma((2, count))]
        + [pltpu.VMEM(v.shape, v.dtype) for v in small],
        compiler_params=pltpu.CompilerParams(vmem_limit_bytes=ALL_VMEM),
        cost_estimate=costing(packed.size),
        name='unpack_in',
    )(packed, *small)


def early_out(ag, fa, fb):
    return pl.pallas_call(
        early_kernel,
        in_specs=[IN_HBM] * 3,
        out_specs=IN_VMEM,
        out_shape=pltpu.VMEM(ag.shape, F32),
        scratch_shapes=[pltpu.SemaphoreType.DMA((DP,))],
        compiler_params=pltpu.CompilerParams(vmem_limit_bytes=BESIDE_HOLD),
        cost_estimate=costing(ag.size),
        name='early_out',
    )(ag, fa, fb)


def late_out(hold, da, db, sa, sb, sh):
    ra, shape = da.shape[0], hold.shape
    work = split_rows(ra, 4) + [(ra + r0, n) for r0, n in split_rows(shape[1] - ra, 4)]
    nmax = max(n for _, n in work)
    dma = pltpu.SemaphoreType.DMA
    return pl.pallas_call(
        lambda *refs: late_kernel(sh, work, *refs),
        in_specs=[IN_VMEM] + [IN_HBM] * 4,
        out_specs=[IN_HBM, IN_VMEM],
        out_shape=[jax.ShapeDtypeStruct(shape, F32), pltpu.VMEM(shape, F32)],
        input_output_aliases={0: 1},
        scratch_shapes=[pltpu.VMEM((4, DP, nmax, shape[2]), F32), dma((len(work), 2)), dma((4,))],
        compiler_params=pltpu.CompilerParams(vmem_limit_bytes=BESIDE_HOLD),
        name='late_out',
    )(hold, da, db, sa, sb)[0]


def solution(mesh):
    tp_devs = mesh.shape['tp']

    def body(w_in, w_out, g_in, g_out, m_in, m_out, r_in, c_in, r_out, c_out, learn_rate, weight_decay, beta_two):
        width = w_in.shape[1]
        sh = width // DP
        mats = (Mat(w_in.shape[2], width, tp_devs, True), Mat(w_out.shape[1], width, tp_devs, False))
        a, o = mats

        def grouped(v, m):
            return v.reshape(DP, m.r, width)

        scal = [v.reshape(1, 1) for v in (learn_rate, weight_decay, beta_two)]
        args = list(scal)
        args += [grouped(g_in[0, 0].T, a), grouped(w_in[0].T, a), m_in[0], r_in, c_in]
        args += [grouped(g_out[0, 0], o), grouped(w_out[0], o), m_out[0].T, c_out, r_out]
        sspec = pl.BlockSpec(memory_space=pltpu.SMEM)
        in_specs = [sspec] * 3 + [IN_HBM] * 10
        out_shape, out_specs = [], []
        for m in mats:
            big = jax.ShapeDtypeStruct((m.r, width), F32)
            out_shape += [jax.ShapeDtypeStruct((DP, m.r, width), F32), jax.ShapeDtypeStruct((sh, m.k), BF16),
                          jax.ShapeDtypeStruct((1, sh), F32), jax.ShapeDtypeStruct((1, m.k), F32),
                          jax.ShapeDtypeStruct((4, m.r, width), F32), big, big, big,
                          jax.ShapeDtypeStruct((m.ra, width), F32), jax.ShapeDtypeStruct((m.r - m.ra, width), F32)]
            out_specs += [IN_HBM] * 10
        nmax = max(m.nmax for m in mats)
        dma = pltpu.SemaphoreType.DMA
        scratch = [pltpu.VMEM((2, 2, 4, nmax, width), F32), pltpu.VMEM((2, DP, nmax, WINDOW), F32), pltpu.VMEM((SUB, LANES), F32), pltpu.VMEM((SUB, LANES), F32), dma((2, 2)), dma((2,))]
        for m in mats:
            gt_rows = 12 * m.r
            scratch += [pltpu.VMEM((4, m.r, width), F32), pltpu.VMEM((gt_rows, 256), F32), pltpu.VMEM((sh, LANES * m.tiles), F32),
                        pltpu.VMEM((sh, m.k), BF16), pltpu.VMEM((SUB, LANES * m.tiles), F32), pltpu.VMEM((m.kr, LANES), F32),
                        pltpu.VMEM((EVERY, m.kr, LANES), F32), pltpu.VMEM((sh, LANES), F32), pltpu.VMEM((sh, LANES), F32),
                        pltpu.VMEM((SUB, LANES), F32), pltpu.VMEM((EVERY, SUB, LANES), F32),
                        pltpu.VMEM((SUB, sh), F32), pltpu.VMEM((SUB, m.k), F32), pltpu.VMEM((sh, LANES), F32), pltpu.VMEM((sh, LANES), F32),
                        pltpu.VMEM((m.kr, LANES), F32), pltpu.VMEM((m.kr, LANES), F32)]
            scratch += [dma((2, NCH)), dma((2, NCH)), dma((2, NCH)), dma((2, NCH)), dma((2,)), dma((2, EVERY)), dma((2,)), dma((2, EVERY)),
                        dma((2, NCH)), dma((2, NCH)), dma((2, NCH)), dma((2, 4, NCH)), dma((5,))]
        outs = pl.pallas_call(
            lambda *refs: main_kernel(mats, sh, *refs),
            in_specs=in_specs,
            out_specs=out_specs,
            out_shape=out_shape,
            scratch_shapes=scratch,
            compiler_params=pltpu.CompilerParams(has_side_effects=True, vmem_limit_bytes=ALL_VMEM),
            name='step',
        )(*args)
        first, second = outs[0:4], outs[10:14]
        fa, fb = outs[18:]
        chips = mesh.shape['dp'] // 2

        def swap(v, bit):
            return lax.ppermute(v, 'dp', [(q, q ^ bit) for q in range(2 * chips)])

        da, db = swap(fa, 4), swap(fb, 2)
        done = unpack_in(first[0], (*first[1:], *second[1:]), sh)
        fa, fb, small = lax.optimization_barrier((fa, fb, done[2]))
        hold = early_out(second[0], fa, fb)
        da, db, hold = lax.optimization_barrier((da, db, hold))
        sa, sb = swap(da, 1), swap(db, 1)
        new_in = done[0].reshape(a.k, width).T[None]
        new_out = late_out(hold, da, db, sa, sb, sh).reshape(o.k, width)[None]
        mom_in, _, col_in, mom_out, row_out, col_out = done[1:]
        return (new_in, new_out, mom_in[None], mom_out.T[None], small, col_in, col_out, row_out)

    free = None
    rows_tp, cols_tp = P(free, 'tp', free), P(free, free, 'tp')
    on_dp, on_tp, whole = P(free, 'dp'), P(free, 'tp'), P()
    state_in, state_out = P(free, 'dp', 'tp'), P(free, 'tp', 'dp')
    in_specs = (cols_tp, rows_tp, P('dp', free, free, 'tp'), P('dp', free, 'tp', free), state_in, state_out, on_dp, on_tp, on_tp, on_dp, whole, whole, whole)
    out_specs = (cols_tp, rows_tp, state_in, state_out, on_dp, on_tp, on_tp, on_dp)
    return jax.shard_map(body, mesh=mesh, in_specs=in_specs, out_specs=out_specs, check_vma=False)
```

```python
import jax
import jax.numpy as jnp
from jax import lax
from jax.experimental import pallas as pl
from jax.experimental.pallas import tpu as pltpu
from jax.sharding import PartitionSpec as P

F32 = jnp.float32
LANES = 128
SUB = 8
DP = 8
EVERY = 16
ALL_VMEM = 67043328
BESIDE_HOLD = 45000000
BF16 = jnp.bfloat16
MESH = pl.DeviceIdType.MESH
NCH = 8
WINDOW = 384
ORDER = (0, 4, 1, 5, 2, 6, 3, 7)


def chunk_rows(rows, small_last):
    tiles = rows // SUB
    out, start = [], 0
    for part in ((tiles + 1) // 2, tiles // 2):
        sizes = [part // 9, part * 3 // 10, part * 7 // 20]
        sizes.append(part - sum(sizes))
        for n in sizes[::-1] if small_last and out else sizes:
            out.append((SUB * start, SUB * n))
            start += n
    return out


def lane_chunks(total):
    width = SUB * LANES
    out = [(s, width) for s in range(0, total - width, width)]
    last = len(out) * width
    if total - last < width // 4:
        s, n = out.pop()
        return out + [(s, n + total - last)]
    return out + [(last, total - last)]


class Mat:
    def __init__(self, kloc, width, tp, row_is_r):
        self.k, self.width, self.sh = kloc, width, width // DP
        self.r = kloc // DP
        self.ktot = kloc * tp
        self.row_is_r = row_is_r
        self.ch = chunk_rows(self.r, not row_is_r)
        self.tiles = (kloc + 127) // LANES
        self.kr = (self.tiles + SUB) // SUB * SUB
        self.nmax = max(n for _, n in self.ch)
        self.ra = self.ch[4][0]
        self.keep = not row_is_r


def rcopy(src, dst, sems, dev):
    if sems[0].shape:
        ref, *at = sems
        sems = ref.at[(0, *at)], ref.at[(1, *at)]
    return pltpu.make_async_remote_copy(src_ref=src, dst_ref=dst, send_sem=sems[0], recv_sem=sems[1], device_id=dev, device_id_type=MESH)


def places():
    dp = lax.axis_index('dp')
    c, chip = lax.rem(dp, 2), lax.div(dp, 2)
    x, y = lax.rem(chip, 2), lax.div(chip, 2)
    return dp, c, chip, chip + 1 - 2 * x, chip + 2 - 4 * y, 3 - chip


def main_kernel(mats, sh, *refs):
    it = iter(refs)
    lr_ref, wd_ref, b2_ref = next(it), next(it), next(it)
    for m in mats:
        m.g, m.w, m.mom, m.row_arg, m.col_arg = (next(it) for _ in range(5))
    for m in mats:
        (m.ag, m.mom_new, m.row_out, m.col_out, m.d2d, m.xy1, m.x2, m.y2, m.fa, m.fb) = (next(it) for _ in range(10))
    stage, wst, usq, ucol = next(it), next(it), next(it), next(it)
    ld_sem, w_sem = next(it), next(it)
    for m in mats:
        (m.p, m.gt, m.gn, m.mv, m.colacc, m.msg, m.slots, m.rp, m.rz, m.sc, m.slots2, m.row_raw, m.col_raw, m.row_old, m.row_new, m.col_old, m.col_new) = (next(it) for _ in range(17))
        (m.d2d_s, m.rs1_s, m.x2_s, m.y2_s, m.ex_s, m.msg_s, m.z_s, m.sc_s, m.agx_s, m.agy_s, m.agd_s, m.ags_s, m.loc_s) = (next(it) for _ in range(13))
    tp = lax.axis_index('tp')
    dp, c, chip, jx, jy, jd = places()
    qx, qy, qd, qs = 2 * jx + c, 2 * jy + c, 2 * jd + c, dp + 1 - 2 * c
    sib, xn, yn = {'tp': tp, 'dp': qs}, {'tp': tp, 'dp': qx}, {'tp': tp, 'dp': qy}
    zn = {'tp': 1 - tp, 'dp': dp}
    me16 = tp * DP + dp

    sends = []

    def start(cp):
        cp.start()
        sends.append(cp)

    def d2d_copy(m, i):
        r0, n = m.ch[i]
        return rcopy(m.g.at[pl.ds(4 * (1 - c), 4), pl.ds(r0, n), :], m.d2d.at[:, pl.ds(r0, n), :], (m.d2d_s, i), sib)

    def own_load(m, i, b):
        r0, n = m.ch[i]
        return pltpu.make_async_copy(m.g.at[pl.ds(4 * c, 4), pl.ds(r0, n), :], stage.at[b, 0, :, pl.ds(0, n), :], ld_sem.at[b, 0])

    def got_load(m, i, b):
        r0, n = m.ch[i]
        return pltpu.make_async_copy(m.d2d.at[:, pl.ds(r0, n), :], stage.at[b, 1, :, pl.ds(0, n), :], ld_sem.at[b, 1])

    def pack_chunk(m, i, b):
        r0, n = m.ch[i]
        own_load(m, i, b).wait()
        got_load(m, i, b).wait()

        def body(t, carry):
            rs = pl.multiple_of(t * SUB, SUB)
            rd = pl.multiple_of(r0 + t * SUB, SUB)
            xs = [stage[b, 0, k, pl.ds(rs, SUB), :] + stage[b, 1, k, pl.ds(rs, SUB), :] for k in range(4)]
            for j in range(4):
                parts = [xs[k][:, sh * (2 * j + cc):sh * (2 * j + cc + 1)] for cc in range(2) for k in range(4)]
                m.p[j, pl.ds(rd, SUB), :] = jnp.concatenate(parts, axis=1)
            return carry

        lax.fori_loop(0, n // SUB, body, 0)

    def pview(m, j, i):
        r0, n = m.ch[i]
        return m.p.at[j, pl.ds(r0, n), :]

    def hview(ref, m, i):
        r0, n = m.ch[i]
        return ref.at[pl.ds(r0, n), :]

    def rs1_copy(m, i):
        dev = xn if i < 4 else yn
        return rcopy(pview(m, jd, i), hview(m.xy1, m, i), (m.rs1_s, i), dev)

    def x2_copy(m, i):
        return rcopy(pview(m, jx, i), hview(m.x2, m, i), (m.x2_s, i), xn)

    def y2_copy(m, i):
        return rcopy(pview(m, jy, i), hview(m.y2, m, i), (m.y2_s, i), yn)

    def rs_free(m, i):
        start(x2_copy(m, i) if i < 4 else y2_copy(m, i))

    def rs_pack(m, send):
        own_load(m, ORDER[0], 0).start()
        for s, i in enumerate(ORDER):
            d2d_copy(m, i).wait_recv()
            got_load(m, i, s % 2).start()
            if s + 1 < NCH:
                own_load(m, ORDER[s + 1], (s + 1) % 2).start()
            pack_chunk(m, i, s % 2)
            if send:
                start(rs1_copy(m, i))
                if s < 4:
                    rs_free(m, i)

    def rs_dep(m, ids):
        def load(s):
            i = ids[s]
            r0, n = m.ch[i]
            return pltpu.make_async_copy(hview(m.xy1, m, i), stage.at[s % 2, 0, 0, pl.ds(0, n), :], ld_sem.at[s % 2, 0])

        for s, i in enumerate(ids):
            r0, n = m.ch[i]
            rs1_copy(m, i).wait_recv()
            load(s).start()
            load(s).wait()
            j = jy if i < 4 else jx

            def body(t, carry):
                rs = pl.multiple_of(t * SUB, SUB)
                rd = pl.multiple_of(r0 + t * SUB, SUB)
                m.p[j, pl.ds(rd, SUB), :] = m.p[j, pl.ds(rd, SUB), :] + stage[s % 2, 0, 0, pl.ds(rs, SUB), :]
                return carry

            lax.fori_loop(0, n // SUB, body, 0)
            start(y2_copy(m, i) if i < 4 else x2_copy(m, i))

    def acc_own(m, ids):
        base = (2 * c * (4 * m.r), (2 - c) * (4 * m.r))

        def loads(s):
            i = ids[s]
            r0, n = m.ch[i]
            b = s % 2
            return (pltpu.make_async_copy(hview(m.x2, m, i), stage.at[b, 0, 0, pl.ds(0, n), :], ld_sem.at[b, 0]),
                    pltpu.make_async_copy(hview(m.y2, m, i), stage.at[b, 0, 1, pl.ds(0, n), :], ld_sem.at[b, 1]))

        for s, i in enumerate(ids):
            r0, n = m.ch[i]
            b = s % 2
            x2_copy(m, i).wait_recv()
            y2_copy(m, i).wait_recv()
            la, lb = loads(s)
            la.start()
            lb.start()
            la.wait()
            lb.wait()

            def body(t, carry):
                rs = pl.multiple_of(t * SUB, SUB)
                rd = pl.multiple_of(r0 + t * SUB, SUB)
                v = m.p[chip, pl.ds(rd, SUB), :] + stage[b, 0, 0, pl.ds(rs, SUB), :] + stage[b, 0, 1, pl.ds(rs, SUB), :]
                for cc in range(2):
                    for k in range(4):
                        row = pl.multiple_of(base[cc] + k * m.r + r0 + t * SUB, SUB)
                        m.gt[pl.ds(row, SUB), 0:sh] = v[:, sh * (4 * cc + k):sh * (4 * cc + k + 1)]
                return carry

            lax.fori_loop(0, n // SUB, body, 0)

    def ex_copy(m):
        h = 4 * m.r
        return rcopy(m.gt.at[pl.ds(2 * h, h), :], m.gt.at[pl.ds(c * h, h), :], (m.ex_s,), sib)

    def ex_wait(m):
        h = 4 * m.r
        rcopy(m.gt.at[pl.ds(2 * h, h), :], m.gt.at[pl.ds((1 - c) * h, h), :], (m.ex_s,), sib).wait_recv()

    def to_gn(m):
        full = m.k // LANES

        def body(t, carry):
            o = pl.multiple_of(t * LANES, LANES)
            m.gn[:, pl.ds(o, LANES)] = m.gt[pl.ds(o, LANES), :].T[0:sh, :]
            return carry

        lax.fori_loop(0, full, body, 0)
        rest = m.k - full * LANES
        if rest:
            m.gn[:, full * LANES:m.k] = m.gt[full * LANES:full * LANES + LANES, :].T[0:sh, 0:rest]

    def from_gn(m):
        full = m.k // LANES
        pad = m.gt.shape[1] - sh

        def turn(v):
            return jnp.concatenate([v, jnp.zeros((pad, LANES), F32)], axis=0).T

        def body(t, carry):
            o = pl.multiple_of(t * LANES, LANES)
            m.gt[pl.ds(o, LANES), :] = turn(m.gn[:, pl.ds(o, LANES)])
            return carry

        lax.fori_loop(0, full, body, 0)
        rest = m.k - full * LANES
        if rest:
            v = jnp.concatenate([m.gn[:, full * LANES:m.k], jnp.zeros((sh, LANES - rest), F32)], axis=1)
            m.gt[full * LANES:m.k, :] = turn(v)[0:rest, :]

    def vec_loads(m):
        return (pltpu.make_async_copy(m.row_arg, m.row_raw.at[pl.ds(0, 1), :], m.loc_s.at[3]),
                pltpu.make_async_copy(m.col_arg, m.col_raw.at[pl.ds(0, 1), :], m.loc_s.at[4]))

    def vec_stores(m):
        return (pltpu.make_async_copy(m.row_raw.at[pl.ds(0, 1), :], m.row_out, m.loc_s.at[3]),
                pltpu.make_async_copy(m.col_raw.at[pl.ds(0, 1), :], m.col_out, m.loc_s.at[4]))

    def vec_prepare(m):
        for cp in vec_loads(m):
            cp.wait()
        pad = m.gt.shape[1] - sh
        row = jnp.concatenate([m.row_raw[0:1, :], jnp.zeros((1, pad), F32)], axis=1)
        m.row_old[...] = jnp.broadcast_to(row, (LANES, sh + pad)).T[0:sh, :]
        m.col_old[...] = jnp.zeros_like(m.col_old)
        for t in range(m.tiles):
            w = min(LANES, m.k - LANES * t)
            m.col_old[t:t + 1, 0:w] = m.col_raw[0:1, LANES * t:LANES * t + w]

    def vec_finish(m):
        pad = m.gt.shape[1] - sh
        m.row_raw[...] = jnp.concatenate([m.row_new[...], jnp.zeros((pad, LANES), F32)], axis=0).T[0:SUB, 0:sh]
        for t in range(m.tiles):
            w = min(LANES, m.k - LANES * t)
            m.col_raw[0:1, LANES * t:LANES * t + w] = m.col_new[t:t + 1, 0:w]
        for cp in vec_stores(m):
            cp.start()

    def peers():
        out = []
        for d in range(1, DP):
            q = lax.rem(dp + d, DP)
            out.append((True, tp, q))
        for d in range(DP):
            q = lax.rem(dp + d, DP)
            out.append((False, 1 - tp, q))
        return out

    def msg_copies(m, sending):
        out = []
        for n, (same, t, q) in enumerate(peers()):
            slot = me16 if sending else t * SUB + q
            dev = {'tp': t, 'dp': q}
            sems = m.msg_s.at[0, n], m.msg_s.at[1, slot]
            rows = pl.ds(0, m.tiles + 1) if same else pl.ds(m.tiles, 1)
            out.append(rcopy(m.msg.at[rows, :], m.slots.at[slot, rows, :], sems, dev))
        return out

    def z_copy(m):
        return rcopy(m.rp, m.rz, (m.z_s,), zn)

    def sc_copies(m, sending):
        out = []
        for n, (same, t, q) in enumerate(peers()):
            slot = me16 if sending else t * SUB + q
            out.append(rcopy(m.sc.at[pl.ds(0, 1), :], m.slots2.at[slot, pl.ds(0, 1), :], (m.sc_s.at[0, n], m.sc_s.at[1, slot]), {'tp': t, 'dp': q}))
        return out

    def stats1(m):
        b2 = b2_ref[0, 0]
        m.colacc[...] = jnp.zeros_like(m.colacc)

        def body(t, carry):
            rr = pl.multiple_of(t * SUB, SUB)
            rsum = jnp.zeros((DP, 1), F32)
            for s0, w in lane_chunks(m.k):
                g = m.gn[pl.ds(rr, SUB), s0:s0 + w]
                sq = g * g + 1e-30
                m.colacc[:, s0:s0 + w] = m.colacc[:, s0:s0 + w] + sq
                rsum = rsum + jnp.sum(sq, axis=1, keepdims=True)
            m.rp[pl.ds(rr, SUB), :] = jnp.broadcast_to(rsum, (SUB, LANES))
            return carry

        lax.fori_loop(0, sh // SUB, body, 0)
        for i in range(m.tiles):
            w = min(LANES, m.k - LANES * i)
            m.msg[i:i + 1, 0:w] = jnp.sum(m.colacc[:, LANES * i:LANES * i + w], axis=0, keepdims=True)
        mean_s = jnp.sum(m.rp[...] * (1.0 / m.ktot), axis=0, keepdims=True) * (1.0 / m.width)
        if m.row_is_r:
            old = jnp.sum(m.row_old[...], axis=0, keepdims=True) * (0.5 / m.width)
        else:
            old = jnp.sum(jnp.sum(m.col_old[...], axis=0, keepdims=True), axis=1, keepdims=True) * (0.125 / m.ktot)
        m.msg[m.tiles:m.tiles + 1, :] = jnp.broadcast_to(b2 * old + (1.0 - b2) * mean_s, (1, LANES))
        m.slots[me16, :, :] = m.msg[...]
        for cp in msg_copies(m, True):
            start(cp)
        start(z_copy(m))

    def stats2(m):
        b2 = b2_ref[0, 0]
        for cp in msg_copies(m, False):
            cp.wait_recv()
        z_copy(m).wait_recv()
        tot = m.slots[tp * DP, 0:m.kr, :]
        for q in range(1, DP):
            tot = tot + m.slots[tp * DP + q, 0:m.kr, :]
        m.col_new[...] = b2 * m.col_old[...] + (1.0 - b2) * (tot / float(m.width))
        m.row_new[...] = b2 * m.row_old[...] + (1.0 - b2) * ((m.rp[...] + m.rz[...]) / float(m.ktot))
        mean_r = m.slots[0, m.tiles:m.tiles + 1, :]
        for q in range(1, EVERY):
            mean_r = mean_r + m.slots[q, m.tiles:m.tiles + 1, :]
        mean_r = mean_r[:, 0:1]
        usq[...] = jnp.zeros_like(usq)
        ucol[...] = jnp.zeros_like(ucol)

        def body(t, carry):
            rr = pl.multiple_of(t * SUB, SUB)
            rv = m.row_new[pl.ds(rr, SUB), 0:1]
            acc = jnp.zeros((DP, 1), F32)
            for i in range(m.tiles):
                s0, w = LANES * i, min(LANES, m.k - LANES * i)
                second = rv * m.col_new[i:i + 1, 0:w] / mean_r
                u = m.gn[pl.ds(rr, SUB), s0:s0 + w] / jnp.sqrt(second)
                m.gn[pl.ds(rr, SUB), s0:s0 + w] = u
                if w == LANES:
                    usq[...] = usq[...] + u * u
                else:
                    acc = acc + jnp.sum(u * u, axis=1, keepdims=True)
            ucol[...] = ucol[...] + jnp.broadcast_to(acc, (SUB, LANES))
            return carry

        lax.fori_loop(0, sh // SUB, body, 0)
        usum = jnp.sum(jnp.sum(usq[...], axis=1, keepdims=True), axis=0, keepdims=True)
        usum = usum + jnp.sum(ucol[:, 0:1], axis=0, keepdims=True)
        m.sc[...] = jnp.broadcast_to(usum, (SUB, LANES))
        m.slots2[me16, :, :] = m.sc[...]
        for cp in sc_copies(m, True):
            start(cp)

    def stats2_end(m):
        for cp in sc_copies(m, False):
            cp.wait_recv()

    def stats3(m):
        tot = m.slots2[0, 0:1, :]
        for q in range(1, EVERY):
            tot = tot + m.slots2[q, 0:1, :]
        den = jnp.maximum(1.0, jnp.sqrt(tot / (float(m.width) * float(m.ktot))))[0:1, 0:1]
        mom_load(m).wait()

        def body(t, carry):
            rr = pl.multiple_of(t * 16, 16)
            for s0, w in lane_chunks(m.k):
                u = m.gn[pl.ds(rr, 16), s0:s0 + w] / den
                mn = (0.9 * m.mv[pl.ds(rr, 16), s0:s0 + w].astype(F32) + 0.1 * u).astype(BF16)
                m.mv[pl.ds(rr, 16), s0:s0 + w] = mn
                m.gn[pl.ds(rr, 16), s0:s0 + w] = mn.astype(F32)
            return carry

        lax.fori_loop(0, sh // 16, body, 0)
        mom_store(m).start()
        from_gn(m)

    def mom_load(m):
        return pltpu.make_async_copy(m.mom, m.mv, m.loc_s.at[0])

    def mom_store(m):
        return pltpu.make_async_copy(m.mv, m.mom_new, m.loc_s.at[1])

    def own_copy(m):
        return pltpu.make_async_copy(m.p.at[chip], m.ag.at[dp], m.loc_s.at[2])

    lane0 = jnp.minimum(lax.div(sh * dp, LANES), DP)
    off = sh * dp - lane0 * LANES

    def w_load(m, i, b):
        r0, n = m.ch[i]
        return pltpu.make_async_copy(m.w.at[:, pl.ds(r0, n), pl.ds(pl.multiple_of(lane0 * LANES, LANES), WINDOW)], wst.at[b, :, pl.ds(0, n), :], w_sem.at[b])

    def new_weights(m, sent):
        lr, wd = lr_ref[0, 0], wd_ref[0, 0]
        w_load(m, 0, 0).start()
        for i in range(NCH):
            r0, n = m.ch[i]
            b = i % 2
            if i + 1 < NCH:
                w_load(m, i + 1, 1 - b).start()
            w_load(m, i, b).wait()

            def body(t, carry):
                rs = pl.multiple_of(t * SUB, SUB)
                rd = pl.multiple_of(r0 + t * SUB, SUB)
                heads, tails = [], []
                for k in range(DP):
                    w = pltpu.roll(wst[b, k, pl.ds(rs, SUB), :], lax.rem(WINDOW - off, WINDOW), 1)[:, 0:sh]
                    mt = m.gt[pl.ds(pl.multiple_of(k * m.r + r0 + t * SUB, SUB), DP), 0:sh]
                    new = w - lr * mt - lr * wd * w
                    heads.append(pltpu.roll(new[:, 0:LANES], lax.rem(sh * dp, LANES), 1))
                    tails.append(new[:, LANES:sh])
                m.p[chip, pl.ds(rd, SUB), :] = jnp.concatenate(heads + tails, axis=1)
                return carry

            lax.fori_loop(0, n // SUB, body, 0)
            if i < sent:
                ag_own(m, i)

    def agrow(m, q, i):
        r0, n = m.ch[i]
        return m.ag.at[q, pl.ds(r0, n), :]

    def xrow(m, q, i):
        r0, n = m.ch[i]
        return m.fa.at[pl.ds(r0, n), :] if m.keep and i < 4 else agrow(m, q, i)

    def yrow(m, q, i):
        r0, n = m.ch[i]
        return m.fb.at[pl.ds(r0 - m.ra, n), :] if m.keep and i >= 4 else agrow(m, q, i)

    def ag_own(m, i):
        start(rcopy(pview(m, chip, i), xrow(m, dp, i), (m.agx_s, i), xn))
        start(rcopy(pview(m, chip, i), yrow(m, dp, i), (m.agy_s, i), yn))

    def ag_sib_own(m, i):
        start(rcopy(pview(m, chip, i), agrow(m, dp, i), (m.ags_s, 0, i), sib))

    def ag_sib(m, which, src, q, i):
        start(rcopy(src, agrow(m, q, i), (m.ags_s, which, i), sib))

    def ag_xy(m, i):
        fx, fy = xrow(m, qx, i), yrow(m, qy, i)
        rcopy(fx, fx, (m.agx_s, i), xn).wait_recv()
        rcopy(fy, fy, (m.agy_s, i), yn).wait_recv()
        if not m.keep:
            if i < 4:
                start(rcopy(fx, fx, (m.agd_s, i), yn))
            else:
                start(rcopy(fy, fy, (m.agd_s, i), xn))
        ag_sib(m, 1, fx, qx, i)
        ag_sib(m, 2, fy, qy, i)

    def ag_d(m, i):
        rcopy(agrow(m, qd, i), agrow(m, qd, i), (m.agd_s, i), xn).wait_recv()
        ag_sib(m, 3, agrow(m, qd, i), qd, i)

    def ag_end(m):
        blocks = (qs, qx + 1 - 2 * c, qy + 1 - 2 * c, qd + 1 - 2 * c)
        for which, q in enumerate(blocks[0:3] if m.keep else blocks):
            for i in range(NCH):
                rcopy(agrow(m, q, i), agrow(m, q, i), (m.ags_s, which, i), sib).wait_recv()

    a, o = mats
    for i in ORDER:
        start(d2d_copy(a, i))
    rs_pack(a, True)
    for i in ORDER[4:]:
        rs_free(a, i)
    for i in ORDER:
        start(d2d_copy(o, i))
    for m in mats:
        mom_load(m).start()
        for cp in vec_loads(m):
            cp.start()
    rs_dep(a, ORDER)
    rs_pack(o, False)
    for m in mats:
        vec_prepare(m)
    for i in ORDER[0:6]:
        start(rs1_copy(o, i))
    acc_own(a, ORDER)
    start(ex_copy(a))
    for i in ORDER[6:]:
        start(rs1_copy(o, i))
    for i in ORDER[0:2]:
        rs_free(o, i)
    ex_wait(a)
    to_gn(a)
    stats1(a)
    for i in ORDER[2:4]:
        rs_free(o, i)
    stats2(a)
    for i in ORDER[4:6]:
        rs_free(o, i)
    stats2_end(a)
    for i in ORDER[6:]:
        rs_free(o, i)
    rs_dep(o, ORDER)
    stats3(a)
    new_weights(a, 3)
    vec_finish(a)
    own_copy(a).start()
    for i in range(NCH):
        ag_sib_own(a, i)
    acc_own(o, ORDER)
    start(ex_copy(o))
    ex_wait(o)
    to_gn(o)
    stats1(o)
    for i in range(3, 5):
        ag_own(a, i)
    stats2(o)
    ag_own(a, 5)
    stats2_end(o)
    for i in range(6, NCH):
        ag_own(a, i)
    stats3(o)
    new_weights(o, 0)
    vec_finish(o)
    own_copy(o).start()
    for i in range(NCH):
        ag_sib_own(o, i)
    for i in range(NCH):
        ag_xy(a, i)
    for i in range(NCH):
        ag_own(o, i)
    for i in range(NCH):
        ag_d(a, i)
    for i in range(NCH):
        ag_xy(o, i)
    for m in mats:
        ag_end(m)
        own_copy(m).wait()
        mom_store(m).wait()
        for cp in vec_stores(m):
            cp.wait()
    for cp in sends:
        cp.wait_send()


def split_rows(rows, parts):
    tiles = rows // SUB
    inner = tiles - 4
    out, start = [], 0
    for n in [2] + [inner // parts + (1 if i < inner % parts else 0) for i in range(parts)] + [2]:
        out.append((SUB * start, SUB * n))
        start += n
    return out


def turn_rows(sh, src, dst, row, rows):
    extra = sh - LANES
    tiles = DP * sh // LANES

    def tile(t):
        return pl.ds(LANES * t, LANES)

    def body(t, carry):
        lane = lax.broadcasted_iota(jnp.int32, (SUB, LANES), 1)
        rs = pl.ds(pl.multiple_of(row + t * SUB, SUB), SUB)
        rd = pl.ds(pl.multiple_of(t * SUB, SUB), SUB)
        ends = [[src[q, rs, tile(e)] for e in range(DP, tiles)] for q in range(DP)]
        for k in range(DP):
            out = [None] * tiles

            def place(v, lo, hi):
                for e in range(lo // LANES, (hi - 1) // LANES + 1):
                    at = max(lo - LANES * e, 0)
                    out[e] = v if out[e] is None else jnp.where(lane >= at, v, out[e])

            first, last = extra * k // LANES, (extra * (k + 1) - 1) // LANES
            for q in range(DP):
                place(src[q, rs, tile(k)], sh * q, sh * q + LANES)
                v = ends[q][first]
                if last > first:
                    v = jnp.where(lane >= extra * k % LANES, v, ends[q][last])
                turn = extra * (q - k) % LANES
                if turn:
                    v = pltpu.roll(v, turn, 1)
                place(v, sh * q + LANES, sh * (q + 1))
            for e in range(tiles):
                dst[k, rd, tile(e)] = out[e]
        return carry

    lax.fori_loop(0, rows // SUB, body, 0)


def unpack_in_kernel(sh, work, count, src, *refs):
    small, dst, small_out = refs[0:count], refs[count], refs[count + 1:2 * count + 1]
    src_v, dst_v, in_sem, out_sem, small_sem, *small_v = refs[2 * count + 1:]
    ins, outs = src_v.shape[0], dst_v.shape[0]

    def load(s):
        r0, n = work[s]
        return pltpu.make_async_copy(src.at[:, pl.ds(r0, n), :], src_v.at[s % ins, :, pl.ds(0, n), :], in_sem.at[s % ins])

    def store(s):
        r0, n = work[s]
        return pltpu.make_async_copy(dst_v.at[s % outs, :, pl.ds(0, n), :], dst.at[:, pl.ds(r0, n), :], out_sem.at[s % outs])

    def small_in(k):
        return pltpu.make_async_copy(small[k], small_v[k], small_sem.at[0, k])

    def small_back(k):
        return pltpu.make_async_copy(small_v[k], small_out[k], small_sem.at[1, k])

    for s in range(ins - 1):
        load(s).start()
    for k in range(count):
        small_in(k).start()
    for s, (r0, n) in enumerate(work):
        if s + ins - 1 < len(work):
            load(s + ins - 1).start()
        load(s).wait()
        if s >= outs:
            store(s - outs).wait()
        turn_rows(sh, src_v.at[s % ins], dst_v.at[s % outs], 0, n)
        store(s).start()
        if s == ins:
            for k in range(count):
                small_in(k).wait()
                small_back(k).start()
    for s in range(len(work) - outs, len(work)):
        store(s).wait()
    for k in range(count):
        small_back(k).wait()


def early_kernel(ag, fa, fb, hold, sem):
    dp, c, chip, *chips = places()
    qx, qy, _ = (2 * j + c for j in chips)
    other = 1 - 2 * c
    half = fa.shape[0]
    lo, hi = pl.ds(0, half), pl.ds(half, fb.shape[0])
    copies = [(ag.at[q], hold.at[q]) for q in (dp, dp + other, qx + other, qy + other)]
    copies += [(fa, hold.at[qx, lo, :]), (ag.at[qx, hi, :], hold.at[qx, hi, :])]
    copies += [(ag.at[qy, lo, :], hold.at[qy, lo, :]), (fb, hold.at[qy, hi, :])]
    copies = [pltpu.make_async_copy(v, w, sem.at[e]) for e, (v, w) in enumerate(copies)]
    for cp in copies:
        cp.start()
    for cp in copies:
        cp.wait()


def late_kernel(sh, work, _, da, db, sa, sb, dst, hold, dst_v, in_sem, out_sem):
    *_, c, _, _, _, jd = places()
    half = da.shape[0]
    outs = dst_v.shape[0]

    def loads(s):
        r0, n = work[s]
        pair, first = ((da, sa), 0) if r0 < half else ((db, sb), half)
        blocks = 2 * jd + c, 2 * jd + 1 - c
        return [pltpu.make_async_copy(v.at[pl.ds(r0 - first, n), :], hold.at[q, pl.ds(r0, n), :], in_sem.at[s, e]) for e, (v, q) in enumerate(zip(pair, blocks))]

    def store(s):
        r0, n = work[s]
        return pltpu.make_async_copy(dst_v.at[s % outs, :, pl.ds(0, n), :], dst.at[:, pl.ds(r0, n), :], out_sem.at[s % outs])

    for s in range(len(work)):
        for cp in loads(s):
            cp.start()
    for s, (r0, n) in enumerate(work):
        for cp in loads(s):
            cp.wait()
        if s >= outs:
            store(s - outs).wait()
        turn_rows(sh, hold, dst_v.at[s % outs], r0, n)
        store(s).start()
    for s in range(len(work) - outs, len(work)):
        store(s).wait()


IN_HBM = pl.BlockSpec(memory_space=pl.ANY)
IN_VMEM = pl.BlockSpec(memory_space=pltpu.VMEM)


def costing(size):
    return pl.CostEstimate(flops=1000 * size, bytes_accessed=DP * size, transcendentals=0)


def unpack_in(packed, small, sh):
    work = split_rows(packed.shape[1], 13)
    nmax = max(n for _, n in work)
    count = len(small)
    dma = pltpu.SemaphoreType.DMA
    buf = (DP, nmax, packed.shape[2])
    return pl.pallas_call(
        lambda *refs: unpack_in_kernel(sh, work, count, *refs),
        in_specs=[IN_HBM] * (1 + count),
        out_specs=[IN_HBM] * (1 + count),
        out_shape=[jax.ShapeDtypeStruct(v.shape, v.dtype) for v in (packed, *small)],
        scratch_shapes=[pltpu.VMEM((4, *buf), F32), pltpu.VMEM((3, *buf), F32), dma((4,)), dma((3,)), dma((2, count))]
        + [pltpu.VMEM(v.shape, v.dtype) for v in small],
        compiler_params=pltpu.CompilerParams(vmem_limit_bytes=ALL_VMEM),
        cost_estimate=costing(packed.size),
        name='unpack_in',
    )(packed, *small)


def early_out(ag, fa, fb):
    return pl.pallas_call(
        early_kernel,
        in_specs=[IN_HBM] * 3,
        out_specs=IN_VMEM,
        out_shape=pltpu.VMEM(ag.shape, F32),
        scratch_shapes=[pltpu.SemaphoreType.DMA((DP,))],
        compiler_params=pltpu.CompilerParams(vmem_limit_bytes=BESIDE_HOLD),
        cost_estimate=costing(ag.size),
        name='early_out',
    )(ag, fa, fb)


def late_out(hold, da, db, sa, sb, sh):
    ra, shape = da.shape[0], hold.shape
    work = split_rows(ra, 4) + [(ra + r0, n) for r0, n in split_rows(shape[1] - ra, 4)]
    nmax = max(n for _, n in work)
    dma = pltpu.SemaphoreType.DMA
    return pl.pallas_call(
        lambda *refs: late_kernel(sh, work, *refs),
        in_specs=[IN_VMEM] + [IN_HBM] * 4,
        out_specs=[IN_HBM, IN_VMEM],
        out_shape=[jax.ShapeDtypeStruct(shape, F32), pltpu.VMEM(shape, F32)],
        input_output_aliases={0: 1},
        scratch_shapes=[pltpu.VMEM((4, DP, nmax, shape[2]), F32), dma((len(work), 2)), dma((4,))],
        compiler_params=pltpu.CompilerParams(vmem_limit_bytes=BESIDE_HOLD),
        name='late_out',
    )(hold, da, db, sa, sb)[0]


def solution(mesh):
    tp_devs = mesh.shape['tp']

    def body(w_in, w_out, g_in, g_out, m_in, m_out, r_in, c_in, r_out, c_out, learn_rate, weight_decay, beta_two):
        width = w_in.shape[1]
        sh = width // DP
        mats = (Mat(w_in.shape[2], width, tp_devs, True), Mat(w_out.shape[1], width, tp_devs, False))
        a, o = mats

        def grouped(v, m):
            return v.reshape(DP, m.r, width)

        scal = [v.reshape(1, 1) for v in (learn_rate, weight_decay, beta_two)]
        args = list(scal)
        args += [grouped(g_in[0, 0].T, a), grouped(w_in[0].T, a), m_in[0], r_in, c_in]
        args += [grouped(g_out[0, 0], o), grouped(w_out[0], o), m_out[0].T, c_out, r_out]
        sspec = pl.BlockSpec(memory_space=pltpu.SMEM)
        in_specs = [sspec] * 3 + [IN_HBM] * 10
        out_shape, out_specs = [], []
        for m in mats:
            big = jax.ShapeDtypeStruct((m.r, width), F32)
            out_shape += [jax.ShapeDtypeStruct((DP, m.r, width), F32), jax.ShapeDtypeStruct((sh, m.k), BF16),
                          jax.ShapeDtypeStruct((1, sh), F32), jax.ShapeDtypeStruct((1, m.k), F32),
                          jax.ShapeDtypeStruct((4, m.r, width), F32), big, big, big,
                          jax.ShapeDtypeStruct((m.ra, width), F32), jax.ShapeDtypeStruct((m.r - m.ra, width), F32)]
            out_specs += [IN_HBM] * 10
        nmax = max(m.nmax for m in mats)
        dma = pltpu.SemaphoreType.DMA
        scratch = [pltpu.VMEM((2, 2, 4, nmax, width), F32), pltpu.VMEM((2, DP, nmax, WINDOW), F32), pltpu.VMEM((SUB, LANES), F32), pltpu.VMEM((SUB, LANES), F32), dma((2, 2)), dma((2,))]
        for m in mats:
            gt_rows = 12 * m.r
            scratch += [pltpu.VMEM((4, m.r, width), F32), pltpu.VMEM((gt_rows, 256), F32), pltpu.VMEM((sh, LANES * m.tiles), F32),
                        pltpu.VMEM((sh, m.k), BF16), pltpu.VMEM((SUB, LANES * m.tiles), F32), pltpu.VMEM((m.kr, LANES), F32),
                        pltpu.VMEM((EVERY, m.kr, LANES), F32), pltpu.VMEM((sh, LANES), F32), pltpu.VMEM((sh, LANES), F32),
                        pltpu.VMEM((SUB, LANES), F32), pltpu.VMEM((EVERY, SUB, LANES), F32),
                        pltpu.VMEM((SUB, sh), F32), pltpu.VMEM((SUB, m.k), F32), pltpu.VMEM((sh, LANES), F32), pltpu.VMEM((sh, LANES), F32),
                        pltpu.VMEM((m.kr, LANES), F32), pltpu.VMEM((m.kr, LANES), F32)]
            scratch += [dma((2, NCH)), dma((2, NCH)), dma((2, NCH)), dma((2, NCH)), dma((2,)), dma((2, EVERY)), dma((2,)), dma((2, EVERY)),
                        dma((2, NCH)), dma((2, NCH)), dma((2, NCH)), dma((2, 4, NCH)), dma((5,))]
        outs = pl.pallas_call(
            lambda *refs: main_kernel(mats, sh, *refs),
            in_specs=in_specs,
            out_specs=out_specs,
            out_shape=out_shape,
            scratch_shapes=scratch,
            compiler_params=pltpu.CompilerParams(has_side_effects=True, vmem_limit_bytes=ALL_VMEM),
            name='step',
        )(*args)
        first, second = outs[0:4], outs[10:14]
        fa, fb = outs[18:]
        chips = mesh.shape['dp'] // 2

        def swap(v, bit):
            return lax.ppermute(v, 'dp', [(q, q ^ bit) for q in range(2 * chips)])

        da, db = swap(fa, 4), swap(fb, 2)
        done = unpack_in(first[0], (*first[1:], *second[1:]), sh)
        fa, fb, small = lax.optimization_barrier((fa, fb, done[2]))
        hold = early_out(second[0], fa, fb)
        da, db, hold = lax.optimization_barrier((da, db, hold))
        sa, sb = swap(da, 1), swap(db, 1)
        new_in = done[0].reshape(a.k, width).T[None]
        new_out = late_out(hold, da, db, sa, sb, sh).reshape(o.k, width)[None]
        mom_in, _, col_in, mom_out, row_out, col_out = done[1:]
        return (new_in, new_out, mom_in[None], mom_out.T[None], small, col_in, col_out, row_out)

    free = None
    rows_tp, cols_tp = P(free, 'tp', free), P(free, free, 'tp')
    on_dp, on_tp, whole = P(free, 'dp'), P(free, 'tp'), P()
    state_in, state_out = P(free, 'dp', 'tp'), P(free, 'tp', 'dp')
    in_specs = (cols_tp, rows_tp, P('dp', free, free, 'tp'), P('dp', free, 'tp', free), state_in, state_out, on_dp, on_tp, on_tp, on_dp, whole, whole, whole)
    out_specs = (cols_tp, rows_tp, state_in, state_out, on_dp, on_tp, on_tp, on_dp)
    return jax.shard_map(body, mesh=mesh, in_specs=in_specs, out_specs=out_specs, check_vma=False)
```

```python
import jax
import jax.numpy as jnp
from jax import lax
from jax.experimental import pallas as pl
from jax.experimental.pallas import tpu as pltpu
from jax.sharding import PartitionSpec as P


F32 = jnp.float32
LANES = 128
SUB = 8
DP = 8
EVERY = 16
ALL_VMEM = 67043328
BESIDE_HOLD = 45500000
YES, NO = True, False
BF16 = jnp.bfloat16
MESH = pl.DeviceIdType.MESH
NCH = 8
WINDOW = 384
ORDER = (0, 4, 1, 5, 2, 6, 3, 7)


def chunk_rows(rows, small_last):
    tiles = rows // SUB
    out, start = [], 0
    for part in ((tiles + 1) // 2, tiles // 2):
        sizes = [part // 10, part // 2 - part // 10, part // 4 + 1] if small_last else [part // 20, part * 9 // 40, part * 3 // 8]
        sizes.append(part - sum(sizes))
        for n in sizes[::-1] if small_last and out else sizes:
            out.append((SUB * start, SUB * n))
            start += n
    return out


def lane_chunks(total):
    width = SUB * LANES
    out = [(s, width) for s in range(0, total - width, width)]
    last = len(out) * width
    if total - last < width // 4:
        s, n = out.pop()
        return out + [(s, n + total - last)]
    return out + [(last, total - last)]


class Mat:
    def __init__(self, kloc, width, tp, row_is_r):
        self.k, self.width, self.sh = kloc, width, width // DP
        self.r = kloc // DP
        self.ktot = kloc * tp
        self.row_is_r = row_is_r
        self.ch = chunk_rows(self.r, not row_is_r)
        self.tiles = (kloc + 127) // LANES
        self.kr = (self.tiles + SUB) // SUB * SUB
        self.nmax = max(n for _, n in self.ch)
        self.cut = [self.ch[i][0] for i in range(0, NCH, 2)] + [self.r]
        self.keep = not row_is_r


def rcopy(src, dst, sems, dev):
    if sems[0].shape:
        ref, *at = sems
        sems = ref.at[(0, *at)], ref.at[(1, *at)]
    return pltpu.make_async_remote_copy(src_ref=src, dst_ref=dst, send_sem=sems[0], recv_sem=sems[1], device_id=dev, device_id_type=MESH)


def places():
    dp = lax.axis_index('dp')
    c, chip = lax.rem(dp, 2), lax.div(dp, 2)
    x, y = lax.rem(chip, 2), lax.div(chip, 2)
    return dp, c, chip, chip + 1 - 2 * x, chip + 2 - 4 * y, 3 - chip


def main_kernel(mats, sh, *refs):
    it = iter(refs)
    lr_ref, wd_ref, b2_ref = next(it), next(it), next(it)
    for m in mats:
        m.g, m.w, m.mom, m.row_arg, m.col_arg = (next(it) for _ in range(5))
    for m in mats:
        (m.ag, m.mom_new, m.row_out, m.col_out, m.d2d, m.xy1, m.x2, m.y2, *m.far) = (next(it) for _ in range(12))
    stage, wst, usq, ucol = next(it), next(it), next(it), next(it)
    ld_sem, w_sem = next(it), next(it)
    for m in mats:
        (m.p, m.gt, m.gn, m.mv, m.colacc, m.msg, m.slots, m.rp, m.rz, m.sc, m.slots2, m.row_raw, m.col_raw, m.row_old, m.row_new, m.col_old, m.col_new) = (next(it) for _ in range(17))
        (m.d2d_s, m.rs1_s, m.x2_s, m.y2_s, m.ex_s, m.msg_s, m.z_s, m.sc_s, m.agx_s, m.agy_s, m.agd_s, m.ags_s, m.loc_s) = (next(it) for _ in range(13))
    tp = lax.axis_index('tp')
    dp, c, chip, jx, jy, jd = places()
    qx, qy, qd, qs = 2 * jx + c, 2 * jy + c, 2 * jd + c, dp + 1 - 2 * c
    sib, xn, yn = {'tp': tp, 'dp': qs}, {'tp': tp, 'dp': qx}, {'tp': tp, 'dp': qy}
    zn = {'tp': 1 - tp, 'dp': dp}
    me16 = tp * DP + dp

    sends = []

    def start(cp):
        cp.start()
        sends.append(cp)

    def d2d_copy(m, i):
        r0, n = m.ch[i]
        return rcopy(m.g.at[pl.ds(4 * (1 - c), 4), pl.ds(r0, n), :], m.d2d.at[:, pl.ds(r0, n), :], (m.d2d_s, i), sib)

    def own_load(m, i, b):
        r0, n = m.ch[i]
        return pltpu.make_async_copy(m.g.at[pl.ds(4 * c, 4), pl.ds(r0, n), :], stage.at[b, 0, :, pl.ds(0, n), :], ld_sem.at[b, 0])

    def got_load(m, i, b):
        r0, n = m.ch[i]
        return pltpu.make_async_copy(m.d2d.at[:, pl.ds(r0, n), :], stage.at[b, 1, :, pl.ds(0, n), :], ld_sem.at[b, 1])

    def pack_chunk(m, i, b):
        r0, n = m.ch[i]
        own_load(m, i, b).wait()
        got_load(m, i, b).wait()

        def body(t, carry):
            rs = pl.multiple_of(t * SUB, SUB)
            rd = pl.multiple_of(r0 + t * SUB, SUB)
            xs = [stage[b, 0, k, pl.ds(rs, SUB), :] + stage[b, 1, k, pl.ds(rs, SUB), :] for k in range(4)]
            for j in range(4):
                parts = [xs[k][:, sh * (2 * j + cc):sh * (2 * j + cc + 1)] for cc in range(2) for k in range(4)]
                m.p[j, pl.ds(rd, SUB), :] = jnp.concatenate(parts, axis=1)
            return carry

        lax.fori_loop(0, n // SUB, body, 0)

    def pview(m, j, i):
        r0, n = m.ch[i]
        return m.p.at[j, pl.ds(r0, n), :]

    def hview(ref, m, i):
        r0, n = m.ch[i]
        return ref.at[pl.ds(r0, n), :]

    def rs1_copy(m, i):
        dev = xn if i < 4 else yn
        return rcopy(pview(m, jd, i), hview(m.xy1, m, i), (m.rs1_s, i), dev)

    def x2_copy(m, i):
        return rcopy(pview(m, jx, i), hview(m.x2, m, i), (m.x2_s, i), xn)

    def y2_copy(m, i):
        return rcopy(pview(m, jy, i), hview(m.y2, m, i), (m.y2_s, i), yn)

    def rs_free(m, i):
        start(x2_copy(m, i) if i < 4 else y2_copy(m, i))

    def rs_pack(m, send):
        own_load(m, ORDER[0], 0).start()
        for s, i in enumerate(ORDER):
            d2d_copy(m, i).wait_recv()
            got_load(m, i, s % 2).start()
            if s + 1 < NCH:
                own_load(m, ORDER[s + 1], (s + 1) % 2).start()
            pack_chunk(m, i, s % 2)
            if send:
                start(rs1_copy(m, i))
                if s < 4:
                    rs_free(m, i)

    def rs_dep(m, ids):
        def load(s):
            i = ids[s]
            _, n = m.ch[i]
            return pltpu.make_async_copy(hview(m.xy1, m, i), stage.at[s % 2, 0, 0, pl.ds(0, n), :], ld_sem.at[s % 2, 0])

        for s, i in enumerate(ids):
            r0, n = m.ch[i]
            rs1_copy(m, i).wait_recv()
            load(s).start()
            load(s).wait()
            j = jy if i < 4 else jx

            def body(t, carry):
                rs = pl.multiple_of(t * SUB, SUB)
                rd = pl.multiple_of(r0 + t * SUB, SUB)
                m.p[j, pl.ds(rd, SUB), :] = m.p[j, pl.ds(rd, SUB), :] + stage[s % 2, 0, 0, pl.ds(rs, SUB), :]
                return carry

            lax.fori_loop(0, n // SUB, body, 0)
            start(y2_copy(m, i) if i < 4 else x2_copy(m, i))

    def acc_own(m, ids):
        base = (2 * c * (4 * m.r), (2 - c) * (4 * m.r))

        def loads(s):
            i = ids[s]
            _, n = m.ch[i]
            b = s % 2
            return (pltpu.make_async_copy(hview(m.x2, m, i), stage.at[b, 0, 0, pl.ds(0, n), :], ld_sem.at[b, 0]),
                    pltpu.make_async_copy(hview(m.y2, m, i), stage.at[b, 0, 1, pl.ds(0, n), :], ld_sem.at[b, 1]))

        for s, i in enumerate(ids):
            r0, n = m.ch[i]
            b = s % 2
            x2_copy(m, i).wait_recv()
            y2_copy(m, i).wait_recv()
            la, lb = loads(s)
            la.start()
            lb.start()
            la.wait()
            lb.wait()

            def body(t, carry):
                rs = pl.multiple_of(t * SUB, SUB)
                rd = pl.multiple_of(r0 + t * SUB, SUB)
                v = m.p[chip, pl.ds(rd, SUB), :] + stage[b, 0, 0, pl.ds(rs, SUB), :] + stage[b, 0, 1, pl.ds(rs, SUB), :]
                for cc in range(2):
                    for k in range(4):
                        row = pl.multiple_of(base[cc] + k * m.r + r0 + t * SUB, SUB)
                        m.gt[pl.ds(row, SUB), 0:sh] = v[:, sh * (4 * cc + k):sh * (4 * cc + k + 1)]
                return carry

            lax.fori_loop(0, n // SUB, body, 0)

    def ex_copy(m):
        h = 4 * m.r
        return rcopy(m.gt.at[pl.ds(2 * h, h), :], m.gt.at[pl.ds(c * h, h), :], (m.ex_s,), sib)

    def ex_wait(m):
        h = 4 * m.r
        rcopy(m.gt.at[pl.ds(2 * h, h), :], m.gt.at[pl.ds((1 - c) * h, h), :], (m.ex_s,), sib).wait_recv()

    def to_gn(m):
        full = m.k // LANES

        def body(t, carry):
            o = pl.multiple_of(t * LANES, LANES)
            m.gn[:, pl.ds(o, LANES)] = m.gt[pl.ds(o, LANES), :].T[0:sh, :]
            return carry

        lax.fori_loop(0, full, body, 0)
        rest = m.k - full * LANES
        if rest:
            m.gn[:, full * LANES:m.k] = m.gt[full * LANES:full * LANES + LANES, :].T[0:sh, 0:rest]

    def from_gn(m):
        full = m.k // LANES
        pad = m.gt.shape[1] - sh

        def turn(v):
            return jnp.concatenate([v, jnp.zeros((pad, LANES), F32)], axis=0).T

        def body(t, carry):
            o = pl.multiple_of(t * LANES, LANES)
            m.gt[pl.ds(o, LANES), :] = turn(m.gn[:, pl.ds(o, LANES)])
            return carry

        lax.fori_loop(0, full, body, 0)
        rest = m.k - full * LANES
        if rest:
            v = jnp.concatenate([m.gn[:, full * LANES:m.k], jnp.zeros((sh, LANES - rest), F32)], axis=1)
            m.gt[full * LANES:m.k, :] = turn(v)[0:rest, :]

    def vec_loads(m):
        return (pltpu.make_async_copy(m.row_arg, m.row_raw.at[pl.ds(0, 1), :], m.loc_s.at[3]),
                pltpu.make_async_copy(m.col_arg, m.col_raw.at[pl.ds(0, 1), :], m.loc_s.at[4]))

    def vec_stores(m):
        return (pltpu.make_async_copy(m.row_raw.at[pl.ds(0, 1), :], m.row_out, m.loc_s.at[3]),
                pltpu.make_async_copy(m.col_raw.at[pl.ds(0, 1), :], m.col_out, m.loc_s.at[4]))

    def vec_prepare(m):
        for cp in vec_loads(m):
            cp.wait()
        pad = m.gt.shape[1] - sh
        row = jnp.concatenate([m.row_raw[0:1, :], jnp.zeros((1, pad), F32)], axis=1)
        m.row_old[...] = jnp.broadcast_to(row, (LANES, sh + pad)).T[0:sh, :]
        m.col_old[...] = jnp.zeros_like(m.col_old)
        for t in range(m.tiles):
            w = min(LANES, m.k - LANES * t)
            m.col_old[t:t + 1, 0:w] = m.col_raw[0:1, LANES * t:LANES * t + w]

    def vec_finish(m):
        pad = m.gt.shape[1] - sh
        m.row_raw[...] = jnp.concatenate([m.row_new[...], jnp.zeros((pad, LANES), F32)], axis=0).T[0:SUB, 0:sh]
        for t in range(m.tiles):
            w = min(LANES, m.k - LANES * t)
            m.col_raw[0:1, LANES * t:LANES * t + w] = m.col_new[t:t + 1, 0:w]
        for cp in vec_stores(m):
            cp.start()

    def peers():
        out = []
        for d in range(1, DP):
            q = lax.rem(dp + d, DP)
            out.append((YES, tp, q))
        for d in range(DP):
            q = lax.rem(dp + d, DP)
            out.append((NO, 1 - tp, q))
        return out

    def msg_copies(m, sending):
        out = []
        for n, (same, t, q) in enumerate(peers()):
            slot = me16 if sending else t * SUB + q
            dev = {'tp': t, 'dp': q}
            sems = m.msg_s.at[0, n], m.msg_s.at[1, slot]
            rows = pl.ds(0, m.tiles + 1) if same else pl.ds(m.tiles, 1)
            out.append(rcopy(m.msg.at[rows, :], m.slots.at[slot, rows, :], sems, dev))
        return out

    def z_copy(m):
        return rcopy(m.rp, m.rz, (m.z_s,), zn)

    def sc_copies(m, sending):
        out = []
        for n, (same, t, q) in enumerate(peers()):
            slot = me16 if sending else t * SUB + q
            out.append(rcopy(m.sc.at[pl.ds(0, 1), :], m.slots2.at[slot, pl.ds(0, 1), :], (m.sc_s.at[0, n], m.sc_s.at[1, slot]), {'tp': t, 'dp': q}))
        return out

    def stats1(m):
        b2 = b2_ref[0]
        m.colacc[...] = jnp.zeros_like(m.colacc)

        def body(t, carry):
            rr = pl.multiple_of(t * SUB, SUB)
            rsum = jnp.zeros((DP, 1), F32)
            for s0, w in lane_chunks(m.k):
                g = m.gn[pl.ds(rr, SUB), s0:s0 + w]
                sq = g * g + 1e-30
                m.colacc[:, s0:s0 + w] = m.colacc[:, s0:s0 + w] + sq
                rsum = rsum + jnp.sum(sq, axis=1, keepdims=YES)
            m.rp[pl.ds(rr, SUB), :] = jnp.broadcast_to(rsum, (SUB, LANES))
            return carry

        lax.fori_loop(0, sh // SUB, body, 0)
        for i in range(m.tiles):
            w = min(LANES, m.k - LANES * i)
            m.msg[i:i + 1, 0:w] = jnp.sum(m.colacc[:, LANES * i:LANES * i + w], axis=0, keepdims=YES)
        mean_s = jnp.sum(m.rp[...] * (1.0 / m.ktot), axis=0, keepdims=YES) * (1.0 / m.width)
        if m.row_is_r:
            old = jnp.sum(m.row_old[...], axis=0, keepdims=YES) * (0.5 / m.width)
        else:
            old = jnp.sum(jnp.sum(m.col_old[...], axis=0, keepdims=YES), axis=1, keepdims=YES) * (0.125 / m.ktot)
        m.msg[m.tiles:m.tiles + 1, :] = jnp.broadcast_to(b2 * old + (1.0 - b2) * mean_s, (1, LANES))
        m.slots[me16, :, :] = m.msg[...]
        for cp in msg_copies(m, YES):
            start(cp)
        start(z_copy(m))

    def stats2(m):
        b2 = b2_ref[0]
        for cp in msg_copies(m, NO):
            cp.wait_recv()
        z_copy(m).wait_recv()
        tot = m.slots[tp * DP, 0:m.kr, :]
        for q in range(1, DP):
            tot = tot + m.slots[tp * DP + q, 0:m.kr, :]
        m.col_new[...] = b2 * m.col_old[...] + (1.0 - b2) * (tot / float(m.width))
        m.row_new[...] = b2 * m.row_old[...] + (1.0 - b2) * ((m.rp[...] + m.rz[...]) / float(m.ktot))
        mean_r = m.slots[0, m.tiles:m.tiles + 1, :]
        for q in range(1, EVERY):
            mean_r = mean_r + m.slots[q, m.tiles:m.tiles + 1, :]
        mean_r = mean_r[:, 0:1]
        usq[...] = jnp.zeros_like(usq)
        ucol[...] = jnp.zeros_like(ucol)

        def body(t, carry):
            rr = pl.multiple_of(t * SUB, SUB)
            rv = m.row_new[pl.ds(rr, SUB), 0:1]
            acc = jnp.zeros((DP, 1), F32)
            for i in range(m.tiles):
                s0, w = LANES * i, min(LANES, m.k - LANES * i)
                second = rv * m.col_new[i:i + 1, 0:w] / mean_r
                u = m.gn[pl.ds(rr, SUB), s0:s0 + w] / jnp.sqrt(second)
                m.gn[pl.ds(rr, SUB), s0:s0 + w] = u
                if w == LANES:
                    usq[...] = usq[...] + u * u
                else:
                    acc = acc + jnp.sum(u * u, axis=1, keepdims=YES)
            ucol[...] = ucol[...] + jnp.broadcast_to(acc, (SUB, LANES))
            return carry

        lax.fori_loop(0, sh // SUB, body, 0)
        usum = jnp.sum(jnp.sum(usq[...], axis=1, keepdims=YES), axis=0, keepdims=YES)
        usum = usum + jnp.sum(ucol[:, 0:1], axis=0, keepdims=YES)
        m.sc[...] = jnp.broadcast_to(usum, (SUB, LANES))
        m.slots2[me16, :, :] = m.sc[...]
        for cp in sc_copies(m, YES):
            start(cp)

    def stats2_end(m):
        for cp in sc_copies(m, NO):
            cp.wait_recv()

    def stats3(m):
        tot = m.slots2[0, 0:1, :]
        for q in range(1, EVERY):
            tot = tot + m.slots2[q, 0:1, :]
        den = jnp.maximum(1.0, jnp.sqrt(tot / (float(m.width) * float(m.ktot))))[0:1, 0:1]
        mom_load(m).wait()

        def body(t, carry):
            rr = pl.multiple_of(t * 16, 16)
            for s0, w in lane_chunks(m.k):
                u = m.gn[pl.ds(rr, 16), s0:s0 + w] / den
                mn = (0.9 * m.mv[pl.ds(rr, 16), s0:s0 + w].astype(F32) + 0.1 * u).astype(BF16)
                m.mv[pl.ds(rr, 16), s0:s0 + w] = mn
                m.gn[pl.ds(rr, 16), s0:s0 + w] = mn.astype(F32)
            return carry

        lax.fori_loop(0, sh // 16, body, 0)
        mom_store(m).start()
        from_gn(m)

    def mom_load(m):
        return pltpu.make_async_copy(m.mom, m.mv, m.loc_s.at[0])

    def mom_store(m):
        return pltpu.make_async_copy(m.mv, m.mom_new, m.loc_s.at[1])

    def own_copy(m):
        return pltpu.make_async_copy(m.p.at[chip], m.ag.at[dp], m.loc_s.at[2])

    lane0 = jnp.minimum(lax.div(sh * dp, LANES), DP)
    off = sh * dp - lane0 * LANES

    def w_load(m, i, b):
        r0, n = m.ch[i]
        return pltpu.make_async_copy(m.w.at[:, pl.ds(r0, n), pl.ds(pl.multiple_of(lane0 * LANES, LANES), WINDOW)], wst.at[b, :, pl.ds(0, n), :], w_sem.at[b])

    def new_weights(m, sent):
        lr, wd = lr_ref[0], wd_ref[0]
        w_load(m, 0, 0).start()
        for i in range(NCH):
            r0, n = m.ch[i]
            b = i % 2
            if i + 1 < NCH:
                w_load(m, i + 1, 1 - b).start()
            w_load(m, i, b).wait()

            def body(t, carry):
                rs = pl.multiple_of(t * SUB, SUB)
                rd = pl.multiple_of(r0 + t * SUB, SUB)
                heads, tails = [], []
                for k in range(DP):
                    w = pltpu.roll(wst[b, k, pl.ds(rs, SUB), :], lax.rem(WINDOW - off, WINDOW), 1)[:, 0:sh]
                    mt = m.gt[pl.ds(pl.multiple_of(k * m.r + r0 + t * SUB, SUB), DP), 0:sh]
                    new = w - lr * mt - lr * wd * w
                    heads.append(pltpu.roll(new[:, 0:LANES], lax.rem(sh * dp, LANES), 1))
                    tails.append(new[:, LANES:sh])
                m.p[chip, pl.ds(rd, SUB), :] = jnp.concatenate(heads + tails, axis=1)
                return carry

            lax.fori_loop(0, n // SUB, body, 0)
            if i < sent:
                ag_own(m, i)

    def agrow(m, q, i):
        r0, n = m.ch[i]
        return m.ag.at[q, pl.ds(r0, n), :]

    def kept(m, i):
        r0, n = m.ch[i]
        return m.far[i // 2].at[pl.ds(r0 - m.cut[i // 2], n), :]

    def xrow(m, q, i):
        return kept(m, i) if m.keep and i < 4 else agrow(m, q, i)

    def yrow(m, q, i):
        return kept(m, i) if m.keep and i >= 4 else agrow(m, q, i)

    def ag_own(m, i):
        start(rcopy(pview(m, chip, i), xrow(m, dp, i), (m.agx_s, i), xn))
        start(rcopy(pview(m, chip, i), yrow(m, dp, i), (m.agy_s, i), yn))

    def ag_sib_own(m, i):
        start(rcopy(pview(m, chip, i), agrow(m, dp, i), (m.ags_s, 0, i), sib))

    def ag_sib(m, which, src, q, i):
        start(rcopy(src, agrow(m, q, i), (m.ags_s, which, i), sib))

    def ag_xy(m, i):
        fx, fy = xrow(m, qx, i), yrow(m, qy, i)
        rcopy(fx, fx, (m.agx_s, i), xn).wait_recv()
        rcopy(fy, fy, (m.agy_s, i), yn).wait_recv()
        if not m.keep:
            if i < 4:
                start(rcopy(fx, fx, (m.agd_s, i), yn))
            else:
                start(rcopy(fy, fy, (m.agd_s, i), xn))
        ag_sib(m, 1, fx, qx, i)
        ag_sib(m, 2, fy, qy, i)

    def ag_d(m, i):
        rcopy(agrow(m, qd, i), agrow(m, qd, i), (m.agd_s, i), xn).wait_recv()
        ag_sib(m, 3, agrow(m, qd, i), qd, i)

    def ag_end(m):
        blocks = (qs, qx + 1 - 2 * c, qy + 1 - 2 * c, qd + 1 - 2 * c)
        for which, q in enumerate(blocks[0:3] if m.keep else blocks):
            for i in range(NCH):
                rcopy(agrow(m, q, i), agrow(m, q, i), (m.ags_s, which, i), sib).wait_recv()

    a, o = mats
    for i in ORDER:
        start(d2d_copy(a, i))
    rs_pack(a, YES)
    for i in ORDER[4:]:
        rs_free(a, i)
    for i in ORDER:
        start(d2d_copy(o, i))
    for m in mats:
        mom_load(m).start()
        for cp in vec_loads(m):
            cp.start()
    rs_dep(a, ORDER)
    rs_pack(o, NO)
    for m in mats:
        vec_prepare(m)
    for i in ORDER[0:6]:
        start(rs1_copy(o, i))
    acc_own(a, ORDER)
    start(ex_copy(a))
    for i in ORDER[6:]:
        start(rs1_copy(o, i))
    for i in ORDER[0:2]:
        rs_free(o, i)
    ex_wait(a)
    to_gn(a)
    stats1(a)
    for i in ORDER[2:4]:
        rs_free(o, i)
    stats2(a)
    for i in ORDER[4:6]:
        rs_free(o, i)
    stats2_end(a)
    for i in ORDER[6:]:
        rs_free(o, i)
    rs_dep(o, ORDER)
    stats3(a)
    new_weights(a, 3)
    vec_finish(a)
    own_copy(a).start()
    for i in range(NCH):
        ag_sib_own(a, i)
    acc_own(o, ORDER)
    start(ex_copy(o))
    ex_wait(o)
    to_gn(o)
    stats1(o)
    for i in range(3, 5):
        ag_own(a, i)
    stats2(o)
    ag_own(a, 5)
    stats2_end(o)
    for i in range(6, NCH):
        ag_own(a, i)
    stats3(o)
    new_weights(o, 0)
    vec_finish(o)
    own_copy(o).start()
    for i in range(NCH):
        ag_sib_own(o, i)
    for i in range(NCH):
        ag_xy(a, i)
    for i in range(NCH):
        ag_own(o, i)
    for i in range(NCH):
        ag_d(a, i)
    for i in range(NCH):
        ag_xy(o, i)
    for m in mats:
        ag_end(m)
        own_copy(m).wait()
        mom_store(m).wait()
        for cp in vec_stores(m):
            cp.wait()
    for cp in sends:
        cp.wait_send()


def split_rows(rows, parts):
    tiles = rows // SUB
    inner = tiles - 4
    out, start = [], 0
    for n in [2] + [inner // parts + (1 if i < inner % parts else 0) for i in range(parts)] + [2]:
        out.append((SUB * start, SUB * n))
        start += n
    return out


def turn_rows(sh, src, dst, row, rows):
    extra = sh - LANES
    tiles = DP * sh // LANES

    def tile(t):
        return pl.ds(LANES * t, LANES)

    def body(t, carry):
        lane = lax.broadcasted_iota(jnp.int32, (SUB, LANES), 1)
        rs = pl.ds(pl.multiple_of(row + t * SUB, SUB), SUB)
        rd = pl.ds(pl.multiple_of(t * SUB, SUB), SUB)
        ends = [[src[q, rs, tile(e)] for e in range(DP, tiles)] for q in range(DP)]
        for k in range(DP):
            out = [None] * tiles

            def place(v, lo, hi):
                for e in range(lo // LANES, (hi - 1) // LANES + 1):
                    at = max(lo - LANES * e, 0)
                    out[e] = v if out[e] is None else jnp.where(lane >= at, v, out[e])

            first, last = extra * k // LANES, (extra * (k + 1) - 1) // LANES
            for q in range(DP):
                place(src[q, rs, tile(k)], sh * q, sh * q + LANES)
                v = ends[q][first]
                if last > first:
                    v = jnp.where(lane >= extra * k % LANES, v, ends[q][last])
                turn = extra * (q - k) % LANES
                if turn:
                    v = pltpu.roll(v, turn, 1)
                place(v, sh * q + LANES, sh * (q + 1))
            for e in range(tiles):
                dst[k, rd, tile(e)] = out[e]
        return carry

    lax.fori_loop(0, rows // SUB, body, 0)


def unpack_in_kernel(sh, work, count, src, *refs):
    small, dst, small_out = refs[0:count], refs[count], refs[count + 1:2 * count + 1]
    src_v, dst_v, in_sem, out_sem, small_sem, *small_v = refs[2 * count + 1:]
    ins, outs = src_v.shape[0], dst_v.shape[0]

    def load(s):
        r0, n = work[s]
        return pltpu.make_async_copy(src.at[:, pl.ds(r0, n), :], src_v.at[s % ins, :, pl.ds(0, n), :], in_sem.at[s % ins])

    def store(s):
        r0, n = work[s]
        return pltpu.make_async_copy(dst_v.at[s % outs, :, pl.ds(0, n), :], dst.at[:, pl.ds(r0, n), :], out_sem.at[s % outs])

    def small_in(k):
        return pltpu.make_async_copy(small[k], small_v[k], small_sem.at[0, k])

    def small_back(k):
        return pltpu.make_async_copy(small_v[k], small_out[k], small_sem.at[1, k])

    for s in range(ins - 1):
        load(s).start()
    for k in range(count):
        small_in(k).start()
    for s, (r0, n) in enumerate(work):
        if s + ins - 1 < len(work):
            load(s + ins - 1).start()
        load(s).wait()
        if s >= outs:
            store(s - outs).wait()
        turn_rows(sh, src_v.at[s % ins], dst_v.at[s % outs], 0, n)
        store(s).start()
        if s == ins:
            for k in range(count):
                small_in(k).wait()
                small_back(k).start()
    for s in range(len(work) - outs, len(work)):
        store(s).wait()
    for k in range(count):
        small_back(k).wait()


def early_kernel(cut, ag, *refs):
    far, hold, sem = refs[0:4], refs[4], refs[5]
    dp, c, chip, *chips = places()
    qx, qy, _ = (2 * j + c for j in chips)
    other = 1 - 2 * c
    rows = [pl.ds(lo, hi - lo) for lo, hi in zip(cut, cut[1:])]
    copies = [(ag.at[q], hold.at[q]) for q in (dp, dp + other, qx + other, qy + other)]
    for e, part in enumerate(rows):
        for q, near in ((qx, e >= 2), (qy, e < 2)):
            copies.append((ag.at[q, part, :] if near else far[e], hold.at[q, part, :]))
    copies = [pltpu.make_async_copy(v, w, sem.at[e]) for e, (v, w) in enumerate(copies)]
    for cp in copies:
        cp.start()
    for cp in copies:
        cp.wait()


def late_kernel(sh, work, firsts, *refs):
    late, (dst, hold, dst_v, in_sem, out_sem) = refs[1:5], refs[-5:]
    *_, c, _, _, _, jd = places()
    outs = dst_v.shape[0]

    def loads(s):
        r0, n = work[s]
        half = int(r0 >= firsts[1])
        blocks = 2 * jd + c, 2 * jd + 1 - c
        part = pl.ds(r0 - firsts[half], n)
        return [pltpu.make_async_copy(late[2 * e + half].at[part, :], hold.at[q, pl.ds(r0, n), :], in_sem.at[s, e]) for e, q in enumerate(blocks)]

    def store(s):
        r0, n = work[s]
        return pltpu.make_async_copy(dst_v.at[s % outs, :, pl.ds(0, n), :], dst.at[:, pl.ds(r0, n), :], out_sem.at[s % outs])

    for s in range(len(work)):
        for cp in loads(s):
            cp.start()
    for s, (r0, n) in enumerate(work):
        for cp in loads(s):
            cp.wait()
        if s >= outs:
            store(s - outs).wait()
        turn_rows(sh, hold, dst_v.at[s % outs], r0, n)
        store(s).start()
    for s in range(len(work) - outs, len(work)):
        store(s).wait()


IN_HBM = pl.BlockSpec(memory_space=pl.ANY)
IN_VMEM = pl.BlockSpec(memory_space=pltpu.VMEM)


def costing(size):
    return pl.CostEstimate(flops=1000 * size, bytes_accessed=DP * size, transcendentals=0)


def unpack_in(packed, small, sh):
    work = split_rows(packed.shape[1], 13)
    nmax = max(n for _, n in work)
    count = len(small)
    dma = pltpu.SemaphoreType.DMA
    buf = (DP, nmax, packed.shape[2])
    return pl.pallas_call(
        lambda *refs: unpack_in_kernel(sh, work, count, *refs),
        in_specs=[IN_HBM] * (1 + count),
        out_specs=[IN_HBM] * (1 + count),
        out_shape=[jax.ShapeDtypeStruct(v.shape, v.dtype) for v in (packed, *small)],
        scratch_shapes=[pltpu.VMEM((4, *buf), F32), pltpu.VMEM((3, *buf), F32), dma((4,)), dma((3,)), dma((2, count))]
        + [pltpu.VMEM(v.shape, v.dtype) for v in small],
        compiler_params=pltpu.CompilerParams(vmem_limit_bytes=ALL_VMEM),
        cost_estimate=costing(packed.size),
        name='unpack_in',
    )(packed, *small)


def early_out(ag, far, cut):
    return pl.pallas_call(
        lambda *refs: early_kernel(cut, *refs),
        in_specs=[IN_HBM] * (1 + len(far)),
        out_specs=IN_VMEM,
        out_shape=pltpu.VMEM(ag.shape, F32),
        scratch_shapes=[pltpu.SemaphoreType.DMA((12,))],
        compiler_params=pltpu.CompilerParams(vmem_limit_bytes=BESIDE_HOLD),
        cost_estimate=costing(ag.size),
        name='early_out',
    )(ag, *far)


def late_out(hold, late, firsts, sh, before=()):
    shape = hold.shape
    work = [(lo + r0, n) for lo, v in zip(firsts, late) for r0, n in split_rows(v.shape[0], 2)]
    nmax = max(n for _, n in work)
    dma = pltpu.SemaphoreType.DMA
    aliases = {0: 1, 5: 0} if before else {0: 1}
    return pl.pallas_call(
        lambda *refs: late_kernel(sh, work, firsts, *refs),
        in_specs=[IN_VMEM] + [IN_HBM] * (len(late) + len(before)),
        out_specs=[IN_HBM, IN_VMEM],
        out_shape=[jax.ShapeDtypeStruct(shape, F32), pltpu.VMEM(shape, F32)],
        input_output_aliases=aliases,
        scratch_shapes=[pltpu.VMEM((4, DP, nmax, shape[2]), F32), dma((len(work), 2)), dma((4,))],
        compiler_params=pltpu.CompilerParams(vmem_limit_bytes=BESIDE_HOLD),
        cost_estimate=costing(hold.size),
    )(hold, *late, *before)


def solution(mesh):
    tp_devs = mesh.shape['tp']

    def body(w_in, w_out, g_in, g_out, m_in, m_out, r_in, c_in, r_out, c_out, learn_rate, weight_decay, beta_two):
        width = w_in.shape[1]
        sh = width // DP
        mats = (Mat(w_in.shape[2], width, tp_devs, YES), Mat(w_out.shape[1], width, tp_devs, NO))
        a, o = mats

        def grouped(v, m):
            return v.reshape(DP, m.r, width)

        scal = [v.reshape(1) for v in (learn_rate, weight_decay, beta_two)]
        args = list(scal)
        args += [grouped(g_in[0, 0].T, a), grouped(w_in[0].T, a), m_in[0], r_in, c_in]
        args += [grouped(g_out[0, 0], o), grouped(w_out[0], o), m_out[0].T, c_out, r_out]
        sspec = pl.BlockSpec(memory_space=pltpu.SMEM)
        in_specs = [sspec] * 3 + [IN_HBM] * 10
        out_shape, out_specs = [], []
        for m in mats:
            big = jax.ShapeDtypeStruct((m.r, width), F32)
            out_shape += [jax.ShapeDtypeStruct((DP, m.r, width), F32), jax.ShapeDtypeStruct((sh, m.k), BF16),
                          jax.ShapeDtypeStruct((1, sh), F32), jax.ShapeDtypeStruct((1, m.k), F32),
                          jax.ShapeDtypeStruct((4, m.r, width), F32), big, big, big,
                          *(jax.ShapeDtypeStruct((hi - lo, width), F32) for lo, hi in zip(m.cut, m.cut[1:]))]
            out_specs += [IN_HBM] * 12
        nmax = max(m.nmax for m in mats)
        dma = pltpu.SemaphoreType.DMA
        scratch = [pltpu.VMEM((2, 2, 4, nmax, width), F32), pltpu.VMEM((2, DP, nmax, WINDOW), F32), pltpu.VMEM((SUB, LANES), F32), pltpu.VMEM((SUB, LANES), F32), dma((2, 2)), dma((2,))]
        for m in mats:
            gt_rows = 12 * m.r
            scratch += [pltpu.VMEM((4, m.r, width), F32), pltpu.VMEM((gt_rows, 256), F32), pltpu.VMEM((sh, LANES * m.tiles), F32),
                        pltpu.VMEM((sh, m.k), BF16), pltpu.VMEM((SUB, LANES * m.tiles), F32), pltpu.VMEM((m.kr, LANES), F32),
                        pltpu.VMEM((EVERY, m.kr, LANES), F32), pltpu.VMEM((sh, LANES), F32), pltpu.VMEM((sh, LANES), F32),
                        pltpu.VMEM((SUB, LANES), F32), pltpu.VMEM((EVERY, SUB, LANES), F32),
                        pltpu.VMEM((SUB, sh), F32), pltpu.VMEM((SUB, m.k), F32), pltpu.VMEM((sh, LANES), F32), pltpu.VMEM((sh, LANES), F32),
                        pltpu.VMEM((m.kr, LANES), F32), pltpu.VMEM((m.kr, LANES), F32)]
            scratch += [dma((2, NCH)), dma((2, NCH)), dma((2, NCH)), dma((2, NCH)), dma((2,)), dma((2, EVERY)), dma((2,)), dma((2, EVERY)),
                        dma((2, NCH)), dma((2, NCH)), dma((2, NCH)), dma((2, 4, NCH)), dma((5,))]
        outs = pl.pallas_call(
            lambda *refs: main_kernel(mats, sh, *refs),
            in_specs=in_specs,
            out_specs=out_specs,
            out_shape=out_shape,
            scratch_shapes=scratch,
            compiler_params=pltpu.CompilerParams(has_side_effects=YES, vmem_limit_bytes=ALL_VMEM),
            name='step',
        )(*args)
        first, second, far = outs[0:4], outs[12:16], outs[20:]
        chips = mesh.shape['dp'] // 2

        def swap(v, bit):
            return lax.ppermute(v, 'dp', [(q, q ^ bit) for q in range(2 * chips)])

        over = []
        for e in range(2):
            over.append((swap(far[e], 4), swap(far[2 + e], 2)))
        done = unpack_in(first[0], (*first[1:], *second[1:]), sh)
        *both, small = lax.optimization_barrier((*over[0], *far, done[2]))
        early, far = both[0:2], both[2:]
        across = [swap(v, 1) for v in early]
        hold = early_out(second[0], far, o.cut)
        *last, hold = lax.optimization_barrier((*over[1], hold))
        part, hold = late_out(hold, (*early, *across), (o.cut[0], o.cut[2]), sh)
        across = [swap(v, 1) for v in last]
        new_out, _ = late_out(hold, (*last, *across), (o.cut[1], o.cut[3]), sh, (part,))
        new_in = done[0].reshape(a.k, width).T[None]
        new_out = new_out.reshape(o.k, width)[None]
        mom_in, _, col_in, mom_out, row_out, col_out = done[1:]
        return (new_in, new_out, mom_in[None], mom_out.T[None], small, col_in, col_out, row_out)

    free = None
    rows_tp, cols_tp = P(free, 'tp', free), P(free, free, 'tp')
    on_dp, on_tp, whole = P(free, 'dp'), P(free, 'tp'), P()
    state_in, state_out = P(free, 'dp', 'tp'), P(free, 'tp', 'dp')
    in_specs = (cols_tp, rows_tp, P('dp', free, free, 'tp'), P('dp', free, 'tp', free), state_in, state_out, on_dp, on_tp, on_tp, on_dp, whole, whole, whole)
    out_specs = (cols_tp, rows_tp, state_in, state_out, on_dp, on_tp, on_tp, on_dp)
    return jax.shard_map(body, mesh=mesh, in_specs=in_specs, out_specs=out_specs, check_vma=NO)
```

```python
import jax
import jax.numpy as jnp
from jax import lax
from jax.experimental import pallas as pl
from jax.experimental.pallas import tpu as pltpu
from jax.sharding import PartitionSpec as P


F32 = jnp.float32
LANES = 128
SUB = 8
DP = 8
EVERY = 16
ALL_VMEM = 67043328
BESIDE_HOLD = 45500000
YES, NO = True, False
BF16 = jnp.bfloat16
MESH = pl.DeviceIdType.MESH
NCH = 8
WINDOW = 384
ORDER = (0, 4, 1, 5, 2, 6, 3, 7)


def chunk_rows(rows, small_last):
    tiles = rows // SUB
    out, start = [], 0
    for part in ((tiles + 1) // 2, tiles // 2):
        sizes = [part // 10, part // 2 - part // 10, part // 4 + 1] if small_last else [part // 20, part * 9 // 40, part * 3 // 8]
        sizes.append(part - sum(sizes))
        for n in sizes[::-1] if small_last and out else sizes:
            out.append((SUB * start, SUB * n))
            start += n
    return out


def lane_chunks(total):
    width = SUB * LANES
    out = [(s, width) for s in range(0, total - width, width)]
    last = len(out) * width
    if total - last < width // 4:
        s, n = out.pop()
        return out + [(s, n + total - last)]
    return out + [(last, total - last)]


class Mat:
    def __init__(self, kloc, width, tp, row_is_r):
        self.k, self.width, self.sh = kloc, width, width // DP
        self.r = kloc // DP
        self.ktot = kloc * tp
        self.row_is_r = row_is_r
        self.ch = chunk_rows(self.r, not row_is_r)
        self.tiles = (kloc + 127) // LANES
        self.kr = (self.tiles + SUB) // SUB * SUB
        self.nmax = max(n for _, n in self.ch)
        self.cut = [self.ch[i][0] for i in range(0, NCH, 2)] + [self.r]
        self.keep = not row_is_r


def rcopy(src, dst, sems, dev):
    if sems[0].shape:
        ref, *at = sems
        sems = ref.at[(0, *at)], ref.at[(1, *at)]
    return pltpu.make_async_remote_copy(src_ref=src, dst_ref=dst, send_sem=sems[0], recv_sem=sems[1], device_id=dev, device_id_type=MESH)


def places():
    dp = lax.axis_index('dp')
    c, chip = lax.rem(dp, 2), lax.div(dp, 2)
    x, y = lax.rem(chip, 2), lax.div(chip, 2)
    return dp, c, chip, chip + 1 - 2 * x, chip + 2 - 4 * y, 3 - chip


def main_kernel(mats, sh, *refs):
    it = iter(refs)
    lr_ref, wd_ref, b2_ref = next(it), next(it), next(it)
    for m in mats:
        m.g, m.w, m.mom, m.row_arg, m.col_arg = (next(it) for _ in range(5))
    for m in mats:
        (m.ag, m.mom_new, m.row_out, m.col_out, m.d2d, m.xy1, m.x2, m.y2, *m.far) = (next(it) for _ in range(12))
    stage, wst, usq, ucol = next(it), next(it), next(it), next(it)
    ld_sem, w_sem = next(it), next(it)
    for m in mats:
        (m.p, m.gt, m.gn, m.mv, m.colacc, m.msg, m.slots, m.rp, m.rz, m.sc, m.slots2, m.row_raw, m.col_raw, m.row_old, m.row_new, m.col_old, m.col_new) = (next(it) for _ in range(17))
        (m.d2d_s, m.rs1_s, m.x2_s, m.y2_s, m.ex_s, m.msg_s, m.z_s, m.sc_s, m.agx_s, m.agy_s, m.agd_s, m.ags_s, m.loc_s) = (next(it) for _ in range(13))
    tp = lax.axis_index('tp')
    dp, c, chip, jx, jy, jd = places()
    qx, qy, qd, qs = 2 * jx + c, 2 * jy + c, 2 * jd + c, dp + 1 - 2 * c
    sib, xn, yn = {'tp': tp, 'dp': qs}, {'tp': tp, 'dp': qx}, {'tp': tp, 'dp': qy}
    zn = {'tp': 1 - tp, 'dp': dp}
    me16 = tp * DP + dp

    sends = []

    def start(cp):
        cp.start()
        sends.append(cp)

    def direct(m, i):
        return m is mats[0] and i % 4 == 0

    def d2d_copy(m, i):
        r0, n = m.ch[i]
        dst = stage.at[i // 4, 1, :, pl.ds(0, n), :] if direct(m, i) else m.d2d.at[:, pl.ds(r0, n), :]
        return rcopy(m.g.at[pl.ds(4 * (1 - c), 4), pl.ds(r0, n), :], dst, (m.d2d_s, i), sib)

    def own_load(m, i, b):
        r0, n = m.ch[i]
        return pltpu.make_async_copy(m.g.at[pl.ds(4 * c, 4), pl.ds(r0, n), :], stage.at[b, 0, :, pl.ds(0, n), :], ld_sem.at[b, 0])

    def got_load(m, i, b):
        r0, n = m.ch[i]
        return pltpu.make_async_copy(m.d2d.at[:, pl.ds(r0, n), :], stage.at[b, 1, :, pl.ds(0, n), :], ld_sem.at[b, 1])

    def pack_chunk(m, i, b):
        r0, n = m.ch[i]
        own_load(m, i, b).wait()
        if not direct(m, i):
            got_load(m, i, b).wait()

        def body(t, carry):
            rs = pl.multiple_of(t * SUB, SUB)
            rd = pl.multiple_of(r0 + t * SUB, SUB)
            xs = [stage[b, 0, k, pl.ds(rs, SUB), :] + stage[b, 1, k, pl.ds(rs, SUB), :] for k in range(4)]
            for j in range(4):
                parts = [xs[k][:, sh * (2 * j + cc):sh * (2 * j + cc + 1)] for cc in range(2) for k in range(4)]
                m.p[j, pl.ds(rd, SUB), :] = jnp.concatenate(parts, axis=1)
            return carry

        lax.fori_loop(0, n // SUB, body, 0)

    def pview(m, j, i):
        r0, n = m.ch[i]
        return m.p.at[j, pl.ds(r0, n), :]

    def hview(ref, m, i):
        r0, n = m.ch[i]
        return ref.at[pl.ds(r0, n), :]

    def rs1_copy(m, i):
        dev = xn if i < 4 else yn
        return rcopy(pview(m, jd, i), hview(m.xy1, m, i), (m.rs1_s, i), dev)

    def x2_copy(m, i):
        return rcopy(pview(m, jx, i), hview(m.x2, m, i), (m.x2_s, i), xn)

    def y2_copy(m, i):
        return rcopy(pview(m, jy, i), hview(m.y2, m, i), (m.y2_s, i), yn)

    def rs_free(m, i):
        start(x2_copy(m, i) if i < 4 else y2_copy(m, i))

    def rs_pack(m, send):
        own_load(m, ORDER[0], 0).start()
        for s, i in enumerate(ORDER):
            d2d_copy(m, i).wait_recv()
            if not direct(m, i):
                got_load(m, i, s % 2).start()
            if s + 1 < NCH:
                own_load(m, ORDER[s + 1], (s + 1) % 2).start()
            pack_chunk(m, i, s % 2)
            if send:
                start(rs1_copy(m, i))
                if s < 4:
                    rs_free(m, i)

    def rs_dep(m, ids):
        def load(s):
            i = ids[s]
            _, n = m.ch[i]
            return pltpu.make_async_copy(hview(m.xy1, m, i), stage.at[s % 2, 0, 0, pl.ds(0, n), :], ld_sem.at[s % 2, 0])

        for s, i in enumerate(ids):
            r0, n = m.ch[i]
            rs1_copy(m, i).wait_recv()
            load(s).start()
            load(s).wait()
            j = jy if i < 4 else jx

            def body(t, carry):
                rs = pl.multiple_of(t * SUB, SUB)
                rd = pl.multiple_of(r0 + t * SUB, SUB)
                m.p[j, pl.ds(rd, SUB), :] = m.p[j, pl.ds(rd, SUB), :] + stage[s % 2, 0, 0, pl.ds(rs, SUB), :]
                return carry

            lax.fori_loop(0, n // SUB, body, 0)
            start(y2_copy(m, i) if i < 4 else x2_copy(m, i))

    def acc_own(m, ids):
        base = (2 * c * (4 * m.r), (2 - c) * (4 * m.r))

        def loads(s):
            i = ids[s]
            _, n = m.ch[i]
            b = s % 2
            return (pltpu.make_async_copy(hview(m.x2, m, i), stage.at[b, 0, 0, pl.ds(0, n), :], ld_sem.at[b, 0]),
                    pltpu.make_async_copy(hview(m.y2, m, i), stage.at[b, 0, 1, pl.ds(0, n), :], ld_sem.at[b, 1]))

        for s, i in enumerate(ids):
            r0, n = m.ch[i]
            b = s % 2
            x2_copy(m, i).wait_recv()
            y2_copy(m, i).wait_recv()
            la, lb = loads(s)
            la.start()
            lb.start()
            la.wait()
            lb.wait()

            def body(t, carry):
                rs = pl.multiple_of(t * SUB, SUB)
                rd = pl.multiple_of(r0 + t * SUB, SUB)
                v = m.p[chip, pl.ds(rd, SUB), :] + stage[b, 0, 0, pl.ds(rs, SUB), :] + stage[b, 0, 1, pl.ds(rs, SUB), :]
                for cc in range(2):
                    for k in range(4):
                        row = pl.multiple_of(base[cc] + k * m.r + r0 + t * SUB, SUB)
                        m.gt[pl.ds(row, SUB), 0:sh] = v[:, sh * (4 * cc + k):sh * (4 * cc + k + 1)]
                return carry

            lax.fori_loop(0, n // SUB, body, 0)

    def ex_copy(m):
        h = 4 * m.r
        return rcopy(m.gt.at[pl.ds(2 * h, h), :], m.gt.at[pl.ds(c * h, h), :], (m.ex_s,), sib)

    def ex_wait(m):
        h = 4 * m.r
        rcopy(m.gt.at[pl.ds(2 * h, h), :], m.gt.at[pl.ds((1 - c) * h, h), :], (m.ex_s,), sib).wait_recv()

    def to_gn(m):
        full = m.k // LANES

        def body(t, carry):
            o = pl.multiple_of(t * LANES, LANES)
            m.gn[:, pl.ds(o, LANES)] = m.gt[pl.ds(o, LANES), :].T[0:sh, :]
            return carry

        lax.fori_loop(0, full, body, 0)
        rest = m.k - full * LANES
        if rest:
            m.gn[:, full * LANES:m.k] = m.gt[full * LANES:full * LANES + LANES, :].T[0:sh, 0:rest]

    def from_gn(m):
        full = m.k // LANES
        pad = m.gt.shape[1] - sh

        def turn(v):
            return jnp.concatenate([v, jnp.zeros((pad, LANES), F32)], axis=0).T

        def body(t, carry):
            o = pl.multiple_of(t * LANES, LANES)
            m.gt[pl.ds(o, LANES), :] = turn(m.gn[:, pl.ds(o, LANES)])
            return carry

        lax.fori_loop(0, full, body, 0)
        rest = m.k - full * LANES
        if rest:
            v = jnp.concatenate([m.gn[:, full * LANES:m.k], jnp.zeros((sh, LANES - rest), F32)], axis=1)
            m.gt[full * LANES:m.k, :] = turn(v)[0:rest, :]

    def vec_loads(m):
        return (pltpu.make_async_copy(m.row_arg, m.row_raw.at[pl.ds(0, 1), :], m.loc_s.at[3]),
                pltpu.make_async_copy(m.col_arg, m.col_raw.at[pl.ds(0, 1), :], m.loc_s.at[4]))

    def vec_stores(m):
        return (pltpu.make_async_copy(m.row_raw.at[pl.ds(0, 1), :], m.row_out, m.loc_s.at[3]),
                pltpu.make_async_copy(m.col_raw.at[pl.ds(0, 1), :], m.col_out, m.loc_s.at[4]))

    def vec_prepare(m):
        for cp in vec_loads(m):
            cp.wait()
        pad = m.gt.shape[1] - sh
        row = jnp.concatenate([m.row_raw[0:1, :], jnp.zeros((1, pad), F32)], axis=1)
        m.row_old[...] = jnp.broadcast_to(row, (LANES, sh + pad)).T[0:sh, :]
        m.col_old[...] = jnp.zeros_like(m.col_old)
        for t in range(m.tiles):
            w = min(LANES, m.k - LANES * t)
            m.col_old[t:t + 1, 0:w] = m.col_raw[0:1, LANES * t:LANES * t + w]

    def vec_finish(m):
        pad = m.gt.shape[1] - sh
        m.row_raw[...] = jnp.concatenate([m.row_new[...], jnp.zeros((pad, LANES), F32)], axis=0).T[0:SUB, 0:sh]
        for t in range(m.tiles):
            w = min(LANES, m.k - LANES * t)
            m.col_raw[0:1, LANES * t:LANES * t + w] = m.col_new[t:t + 1, 0:w]
        for cp in vec_stores(m):
            cp.start()

    def peers():
        out = []
        for d in range(1, DP):
            q = lax.rem(dp + d, DP)
            out.append((YES, tp, q))
        for d in range(DP):
            q = lax.rem(dp + d, DP)
            out.append((NO, 1 - tp, q))
        return out

    def msg_copies(m, sending):
        out = []
        for n, (same, t, q) in enumerate(peers()):
            slot = me16 if sending else t * SUB + q
            dev = {'tp': t, 'dp': q}
            sems = m.msg_s.at[0, n], m.msg_s.at[1, slot]
            rows = pl.ds(0, m.tiles + 1) if same else pl.ds(m.tiles, 1)
            out.append(rcopy(m.msg.at[rows, :], m.slots.at[slot, rows, :], sems, dev))
        return out

    def z_copy(m):
        return rcopy(m.rp, m.rz, (m.z_s,), zn)

    def sc_copies(m, sending):
        out = []
        for n, (same, t, q) in enumerate(peers()):
            slot = me16 if sending else t * SUB + q
            out.append(rcopy(m.sc.at[pl.ds(0, 1), :], m.slots2.at[slot, pl.ds(0, 1), :], (m.sc_s.at[0, n], m.sc_s.at[1, slot]), {'tp': t, 'dp': q}))
        return out

    def stats1(m):
        b2 = b2_ref[0]
        m.colacc[...] = jnp.zeros_like(m.colacc)

        def body(t, carry):
            rr = pl.multiple_of(t * SUB, SUB)
            rsum = jnp.zeros((DP, 1), F32)
            for s0, w in lane_chunks(m.k):
                g = m.gn[pl.ds(rr, SUB), s0:s0 + w]
                sq = g * g + 1e-30
                m.colacc[:, s0:s0 + w] = m.colacc[:, s0:s0 + w] + sq
                rsum = rsum + jnp.sum(sq, axis=1, keepdims=YES)
            m.rp[pl.ds(rr, SUB), :] = jnp.broadcast_to(rsum, (SUB, LANES))
            return carry

        lax.fori_loop(0, sh // SUB, body, 0)
        for i in range(m.tiles):
            w = min(LANES, m.k - LANES * i)
            m.msg[i:i + 1, 0:w] = jnp.sum(m.colacc[:, LANES * i:LANES * i + w], axis=0, keepdims=YES)
        mean_s = jnp.sum(m.rp[...] * (1.0 / m.ktot), axis=0, keepdims=YES) * (1.0 / m.width)
        if m.row_is_r:
            old = jnp.sum(m.row_old[...], axis=0, keepdims=YES) * (0.5 / m.width)
        else:
            old = jnp.sum(jnp.sum(m.col_old[...], axis=0, keepdims=YES), axis=1, keepdims=YES) * (0.125 / m.ktot)
        m.msg[m.tiles:m.tiles + 1, :] = jnp.broadcast_to(b2 * old + (1.0 - b2) * mean_s, (1, LANES))
        m.slots[me16, :, :] = m.msg[...]
        for cp in msg_copies(m, YES):
            start(cp)
        start(z_copy(m))

    def stats2(m):
        b2 = b2_ref[0]
        for cp in msg_copies(m, NO):
            cp.wait_recv()
        z_copy(m).wait_recv()
        tot = m.slots[tp * DP, 0:m.kr, :]
        for q in range(1, DP):
            tot = tot + m.slots[tp * DP + q, 0:m.kr, :]
        m.col_new[...] = b2 * m.col_old[...] + (1.0 - b2) * (tot / float(m.width))
        m.row_new[...] = b2 * m.row_old[...] + (1.0 - b2) * ((m.rp[...] + m.rz[...]) / float(m.ktot))
        mean_r = m.slots[0, m.tiles:m.tiles + 1, :]
        for q in range(1, EVERY):
            mean_r = mean_r + m.slots[q, m.tiles:m.tiles + 1, :]
        mean_r = mean_r[:, 0:1]
        usq[...] = jnp.zeros_like(usq)
        ucol[...] = jnp.zeros_like(ucol)

        def body(t, carry):
            rr = pl.multiple_of(t * SUB, SUB)
            rv = m.row_new[pl.ds(rr, SUB), 0:1]
            acc = jnp.zeros((DP, 1), F32)
            for i in range(m.tiles):
                s0, w = LANES * i, min(LANES, m.k - LANES * i)
                second = rv * m.col_new[i:i + 1, 0:w] / mean_r
                u = m.gn[pl.ds(rr, SUB), s0:s0 + w] / jnp.sqrt(second)
                m.gn[pl.ds(rr, SUB), s0:s0 + w] = u
                if w == LANES:
                    usq[...] = usq[...] + u * u
                else:
                    acc = acc + jnp.sum(u * u, axis=1, keepdims=YES)
            ucol[...] = ucol[...] + jnp.broadcast_to(acc, (SUB, LANES))
            return carry

        lax.fori_loop(0, sh // SUB, body, 0)
        usum = jnp.sum(jnp.sum(usq[...], axis=1, keepdims=YES), axis=0, keepdims=YES)
        usum = usum + jnp.sum(ucol[:, 0:1], axis=0, keepdims=YES)
        m.sc[...] = jnp.broadcast_to(usum, (SUB, LANES))
        m.slots2[me16, :, :] = m.sc[...]
        for cp in sc_copies(m, YES):
            start(cp)

    def stats2_end(m):
        for cp in sc_copies(m, NO):
            cp.wait_recv()

    def stats3(m):
        tot = m.slots2[0, 0:1, :]
        for q in range(1, EVERY):
            tot = tot + m.slots2[q, 0:1, :]
        den = jnp.maximum(1.0, jnp.sqrt(tot / (float(m.width) * float(m.ktot))))[0:1, 0:1]
        mom_load(m).wait()

        def body(t, carry):
            rr = pl.multiple_of(t * 16, 16)
            for s0, w in lane_chunks(m.k):
                u = m.gn[pl.ds(rr, 16), s0:s0 + w] / den
                mn = (0.9 * m.mv[pl.ds(rr, 16), s0:s0 + w].astype(F32) + 0.1 * u).astype(BF16)
                m.mv[pl.ds(rr, 16), s0:s0 + w] = mn
                m.gn[pl.ds(rr, 16), s0:s0 + w] = mn.astype(F32)
            return carry

        lax.fori_loop(0, sh // 16, body, 0)
        mom_store(m).start()
        from_gn(m)

    def mom_load(m):
        return pltpu.make_async_copy(m.mom, m.mv, m.loc_s.at[0])

    def mom_store(m):
        return pltpu.make_async_copy(m.mv, m.mom_new, m.loc_s.at[1])

    def own_copy(m):
        return pltpu.make_async_copy(m.p.at[chip], m.ag.at[dp], m.loc_s.at[2])

    lane0 = jnp.minimum(lax.div(sh * dp, LANES), DP)
    off = sh * dp - lane0 * LANES

    def w_load(m, i, b):
        r0, n = m.ch[i]
        return pltpu.make_async_copy(m.w.at[:, pl.ds(r0, n), pl.ds(pl.multiple_of(lane0 * LANES, LANES), WINDOW)], wst.at[b, :, pl.ds(0, n), :], w_sem.at[b])

    def new_weights(m, sent):
        lr, wd = lr_ref[0], wd_ref[0]
        w_load(m, 0, 0).start()
        for i in range(NCH):
            r0, n = m.ch[i]
            b = i % 2
            if i + 1 < NCH:
                w_load(m, i + 1, 1 - b).start()
            w_load(m, i, b).wait()

            def body(t, carry):
                rs = pl.multiple_of(t * SUB, SUB)
                rd = pl.multiple_of(r0 + t * SUB, SUB)
                heads, tails = [], []
                for k in range(DP):
                    w = pltpu.roll(wst[b, k, pl.ds(rs, SUB), :], lax.rem(WINDOW - off, WINDOW), 1)[:, 0:sh]
                    mt = m.gt[pl.ds(pl.multiple_of(k * m.r + r0 + t * SUB, SUB), DP), 0:sh]
                    new = w - lr * mt - lr * wd * w
                    heads.append(pltpu.roll(new[:, 0:LANES], lax.rem(sh * dp, LANES), 1))
                    tails.append(new[:, LANES:sh])
                m.p[chip, pl.ds(rd, SUB), :] = jnp.concatenate(heads + tails, axis=1)
                return carry

            lax.fori_loop(0, n // SUB, body, 0)
            if i < sent:
                ag_own(m, i)

    def agrow(m, q, i):
        r0, n = m.ch[i]
        return m.ag.at[q, pl.ds(r0, n), :]

    def kept(m, i):
        r0, n = m.ch[i]
        return m.far[i // 2].at[pl.ds(r0 - m.cut[i // 2], n), :]

    def xrow(m, q, i):
        return kept(m, i) if m.keep and i < 4 else agrow(m, q, i)

    def yrow(m, q, i):
        return kept(m, i) if m.keep and i >= 4 else agrow(m, q, i)

    def ag_own(m, i):
        start(rcopy(pview(m, chip, i), xrow(m, dp, i), (m.agx_s, i), xn))
        start(rcopy(pview(m, chip, i), yrow(m, dp, i), (m.agy_s, i), yn))

    def ag_sib_own(m, i):
        start(rcopy(pview(m, chip, i), agrow(m, dp, i), (m.ags_s, 0, i), sib))

    def ag_sib(m, which, src, q, i):
        start(rcopy(src, agrow(m, q, i), (m.ags_s, which, i), sib))

    def ag_xy(m, i):
        fx, fy = xrow(m, qx, i), yrow(m, qy, i)
        rcopy(fx, fx, (m.agx_s, i), xn).wait_recv()
        rcopy(fy, fy, (m.agy_s, i), yn).wait_recv()
        if not m.keep:
            if i < 4:
                start(rcopy(fx, fx, (m.agd_s, i), yn))
            else:
                start(rcopy(fy, fy, (m.agd_s, i), xn))
        ag_sib(m, 1, fx, qx, i)
        ag_sib(m, 2, fy, qy, i)

    def ag_d(m, i):
        rcopy(agrow(m, qd, i), agrow(m, qd, i), (m.agd_s, i), xn).wait_recv()
        ag_sib(m, 3, agrow(m, qd, i), qd, i)

    def ag_end(m):
        blocks = (qs, qx + 1 - 2 * c, qy + 1 - 2 * c, qd + 1 - 2 * c)
        for which, q in enumerate(blocks[0:3] if m.keep else blocks):
            for i in range(NCH):
                rcopy(agrow(m, q, i), agrow(m, q, i), (m.ags_s, which, i), sib).wait_recv()

    a, o = mats
    for i in ORDER:
        start(d2d_copy(a, i))
    rs_pack(a, YES)
    for i in ORDER[4:]:
        rs_free(a, i)
    for i in ORDER:
        start(d2d_copy(o, i))
    for m in mats:
        mom_load(m).start()
        for cp in vec_loads(m):
            cp.start()
    rs_dep(a, ORDER)
    rs_pack(o, NO)
    for m in mats:
        vec_prepare(m)
    for i in ORDER[0:6]:
        start(rs1_copy(o, i))
    acc_own(a, ORDER)
    start(ex_copy(a))
    for i in ORDER[6:]:
        start(rs1_copy(o, i))
    for i in ORDER[0:2]:
        rs_free(o, i)
    ex_wait(a)
    to_gn(a)
    stats1(a)
    for i in ORDER[2:4]:
        rs_free(o, i)
    stats2(a)
    for i in ORDER[4:6]:
        rs_free(o, i)
    stats2_end(a)
    for i in ORDER[6:]:
        rs_free(o, i)
    rs_dep(o, ORDER)
    stats3(a)
    new_weights(a, 3)
    vec_finish(a)
    own_copy(a).start()
    for i in range(NCH):
        ag_sib_own(a, i)
    acc_own(o, ORDER)
    start(ex_copy(o))
    ex_wait(o)
    to_gn(o)
    stats1(o)
    for i in range(3, 5):
        ag_own(a, i)
    stats2(o)
    ag_own(a, 5)
    stats2_end(o)
    for i in range(6, NCH):
        ag_own(a, i)
    stats3(o)
    new_weights(o, 0)
    vec_finish(o)
    own_copy(o).start()
    for i in range(NCH):
        ag_sib_own(o, i)
    for i in range(NCH):
        ag_xy(a, i)
    for i in range(NCH):
        ag_own(o, i)
    for i in range(NCH):
        ag_d(a, i)
    for i in range(NCH):
        ag_xy(o, i)
    for m in mats:
        ag_end(m)
        own_copy(m).wait()
        mom_store(m).wait()
        for cp in vec_stores(m):
            cp.wait()
    for cp in sends:
        cp.wait_send()


def split_rows(rows, parts):
    tiles = rows // SUB
    inner = tiles - 4
    out, start = [], 0
    for n in [2] + [inner // parts + (1 if i < inner % parts else 0) for i in range(parts)] + [2]:
        out.append((SUB * start, SUB * n))
        start += n
    return out


def turn_rows(sh, src, dst, row, rows):
    extra = sh - LANES
    tiles = DP * sh // LANES

    def tile(t):
        return pl.ds(LANES * t, LANES)

    def body(t, carry):
        lane = lax.broadcasted_iota(jnp.int32, (SUB, LANES), 1)
        rs = pl.ds(pl.multiple_of(row + t * SUB, SUB), SUB)
        rd = pl.ds(pl.multiple_of(t * SUB, SUB), SUB)
        ends = [[src[q, rs, tile(e)] for e in range(DP, tiles)] for q in range(DP)]
        for k in range(DP):
            out = [None] * tiles

            def place(v, lo, hi):
                for e in range(lo // LANES, (hi - 1) // LANES + 1):
                    at = max(lo - LANES * e, 0)
                    out[e] = v if out[e] is None else jnp.where(lane >= at, v, out[e])

            first, last = extra * k // LANES, (extra * (k + 1) - 1) // LANES
            for q in range(DP):
                place(src[q, rs, tile(k)], sh * q, sh * q + LANES)
                v = ends[q][first]
                if last > first:
                    v = jnp.where(lane >= extra * k % LANES, v, ends[q][last])
                turn = extra * (q - k) % LANES
                if turn:
                    v = pltpu.roll(v, turn, 1)
                place(v, sh * q + LANES, sh * (q + 1))
            for e in range(tiles):
                dst[k, rd, tile(e)] = out[e]
        return carry

    lax.fori_loop(0, rows // SUB, body, 0)


def unpack_in_kernel(sh, work, count, src, *refs):
    small, dst, small_out = refs[0:count], refs[count], refs[count + 1:2 * count + 1]
    src_v, dst_v, in_sem, out_sem, small_sem, *small_v = refs[2 * count + 1:]
    ins, outs = src_v.shape[0], dst_v.shape[0]

    def load(s):
        r0, n = work[s]
        return pltpu.make_async_copy(src.at[:, pl.ds(r0, n), :], src_v.at[s % ins, :, pl.ds(0, n), :], in_sem.at[s % ins])

    def store(s):
        r0, n = work[s]
        return pltpu.make_async_copy(dst_v.at[s % outs, :, pl.ds(0, n), :], dst.at[:, pl.ds(r0, n), :], out_sem.at[s % outs])

    def small_in(k):
        return pltpu.make_async_copy(small[k], small_v[k], small_sem.at[0, k])

    def small_back(k):
        return pltpu.make_async_copy(small_v[k], small_out[k], small_sem.at[1, k])

    for s in range(ins - 1):
        load(s).start()
    for k in range(count):
        small_in(k).start()
    for s, (r0, n) in enumerate(work):
        if s + ins - 1 < len(work):
            load(s + ins - 1).start()
        load(s).wait()
        if s >= outs:
            store(s - outs).wait()
        turn_rows(sh, src_v.at[s % ins], dst_v.at[s % outs], 0, n)
        store(s).start()
        if s == ins:
            for k in range(count):
                small_in(k).wait()
                small_back(k).start()
    for s in range(len(work) - outs, len(work)):
        store(s).wait()
    for k in range(count):
        small_back(k).wait()


def early_kernel(cut, ag, *refs):
    far, hold, sem = refs[0:4], refs[4], refs[5]
    dp, c, chip, *chips = places()
    qx, qy, _ = (2 * j + c for j in chips)
    other = 1 - 2 * c
    rows = [pl.ds(lo, hi - lo) for lo, hi in zip(cut, cut[1:])]
    copies = [(ag.at[q], hold.at[q]) for q in (dp, dp + other, qx + other, qy + other)]
    for e, part in enumerate(rows):
        for q, near in ((qx, e >= 2), (qy, e < 2)):
            copies.append((ag.at[q, part, :] if near else far[e], hold.at[q, part, :]))
    copies = [pltpu.make_async_copy(v, w, sem.at[e]) for e, (v, w) in enumerate(copies)]
    for cp in copies:
        cp.start()
    for cp in copies:
        cp.wait()


def late_kernel(sh, work, firsts, *refs):
    late, (dst, hold, dst_v, in_sem, out_sem) = refs[1:5], refs[-5:]
    *_, c, _, _, _, jd = places()
    outs = dst_v.shape[0]

    def loads(s):
        r0, n = work[s]
        half = int(r0 >= firsts[1])
        blocks = 2 * jd + c, 2 * jd + 1 - c
        part = pl.ds(r0 - firsts[half], n)
        return [pltpu.make_async_copy(late[2 * e + half].at[part, :], hold.at[q, pl.ds(r0, n), :], in_sem.at[s, e]) for e, q in enumerate(blocks)]

    def store(s):
        r0, n = work[s]
        return pltpu.make_async_copy(dst_v.at[s % outs, :, pl.ds(0, n), :], dst.at[:, pl.ds(r0, n), :], out_sem.at[s % outs])

    for s in range(len(work)):
        for cp in loads(s):
            cp.start()
    for s, (r0, n) in enumerate(work):
        for cp in loads(s):
            cp.wait()
        if s >= outs:
            store(s - outs).wait()
        turn_rows(sh, hold, dst_v.at[s % outs], r0, n)
        store(s).start()
    for s in range(len(work) - outs, len(work)):
        store(s).wait()


IN_HBM = pl.BlockSpec(memory_space=pl.ANY)
IN_VMEM = pl.BlockSpec(memory_space=pltpu.VMEM)


def costing(size):
    return pl.CostEstimate(flops=1000 * size, bytes_accessed=DP * size, transcendentals=0)


def unpack_in(packed, small, sh):
    work = split_rows(packed.shape[1], 13)
    nmax = max(n for _, n in work)
    count = len(small)
    dma = pltpu.SemaphoreType.DMA
    buf = (DP, nmax, packed.shape[2])
    return pl.pallas_call(
        lambda *refs: unpack_in_kernel(sh, work, count, *refs),
        in_specs=[IN_HBM] * (1 + count),
        out_specs=[IN_HBM] * (1 + count),
        out_shape=[jax.ShapeDtypeStruct(v.shape, v.dtype) for v in (packed, *small)],
        scratch_shapes=[pltpu.VMEM((6, *buf), F32), pltpu.VMEM((5, *buf), F32), dma((6,)), dma((5,)), dma((2, count))]
        + [pltpu.VMEM(v.shape, v.dtype) for v in small],
        compiler_params=pltpu.CompilerParams(vmem_limit_bytes=ALL_VMEM),
        cost_estimate=costing(packed.size),
        name='unpack_in',
    )(packed, *small)


def early_out(ag, far, cut):
    return pl.pallas_call(
        lambda *refs: early_kernel(cut, *refs),
        in_specs=[IN_HBM] * (1 + len(far)),
        out_specs=IN_VMEM,
        out_shape=pltpu.VMEM(ag.shape, F32),
        scratch_shapes=[pltpu.SemaphoreType.DMA((12,))],
        compiler_params=pltpu.CompilerParams(vmem_limit_bytes=BESIDE_HOLD),
        cost_estimate=costing(ag.size),
        name='early_out',
    )(ag, *far)


def late_out(hold, late, firsts, sh, before=()):
    shape = hold.shape
    work = [(lo + r0, n) for lo, v in zip(firsts, late) for r0, n in split_rows(v.shape[0], 2)]
    nmax = max(n for _, n in work)
    dma = pltpu.SemaphoreType.DMA
    aliases = {0: 1, 5: 0} if before else {0: 1}
    return pl.pallas_call(
        lambda *refs: late_kernel(sh, work, firsts, *refs),
        in_specs=[IN_VMEM] + [IN_HBM] * (len(late) + len(before)),
        out_specs=[IN_HBM, IN_VMEM],
        out_shape=[jax.ShapeDtypeStruct(shape, F32), pltpu.VMEM(shape, F32)],
        input_output_aliases=aliases,
        scratch_shapes=[pltpu.VMEM((4, DP, nmax, shape[2]), F32), dma((len(work), 2)), dma((4,))],
        compiler_params=pltpu.CompilerParams(vmem_limit_bytes=BESIDE_HOLD),
        cost_estimate=costing(hold.size),
    )(hold, *late, *before)


def solution(mesh):
    tp_devs = mesh.shape['tp']

    def body(w_in, w_out, g_in, g_out, m_in, m_out, r_in, c_in, r_out, c_out, learn_rate, weight_decay, beta_two):
        width = w_in.shape[1]
        sh = width // DP
        mats = (Mat(w_in.shape[2], width, tp_devs, YES), Mat(w_out.shape[1], width, tp_devs, NO))
        a, o = mats

        def grouped(v, m):
            return v.reshape(DP, m.r, width)

        scal = [v.reshape(1) for v in (learn_rate, weight_decay, beta_two)]
        args = list(scal)
        args += [grouped(g_in[0, 0].T, a), grouped(w_in[0].T, a), m_in[0], r_in, c_in]
        args += [grouped(g_out[0, 0], o), grouped(w_out[0], o), m_out[0].T, c_out, r_out]
        sspec = pl.BlockSpec(memory_space=pltpu.SMEM)
        in_specs = [sspec] * 3 + [IN_HBM] * 10
        out_shape, out_specs = [], []
        for m in mats:
            big = jax.ShapeDtypeStruct((m.r, width), F32)
            out_shape += [jax.ShapeDtypeStruct((DP, m.r, width), F32), jax.ShapeDtypeStruct((sh, m.k), BF16),
                          jax.ShapeDtypeStruct((1, sh), F32), jax.ShapeDtypeStruct((1, m.k), F32),
                          jax.ShapeDtypeStruct((4, m.r, width), F32), big, big, big,
                          *(jax.ShapeDtypeStruct((hi - lo, width), F32) for lo, hi in zip(m.cut, m.cut[1:]))]
            out_specs += [IN_HBM] * 12
        nmax = max(m.nmax for m in mats)
        dma = pltpu.SemaphoreType.DMA
        scratch = [pltpu.VMEM((2, 2, 4, nmax, width), F32), pltpu.VMEM((2, DP, nmax, WINDOW), F32), pltpu.VMEM((SUB, LANES), F32), pltpu.VMEM((SUB, LANES), F32), dma((2, 2)), dma((2,))]
        for m in mats:
            gt_rows = 12 * m.r
            scratch += [pltpu.VMEM((4, m.r, width), F32), pltpu.VMEM((gt_rows, 256), F32), pltpu.VMEM((sh, LANES * m.tiles), F32),
                        pltpu.VMEM((sh, m.k), BF16), pltpu.VMEM((SUB, LANES * m.tiles), F32), pltpu.VMEM((m.kr, LANES), F32),
                        pltpu.VMEM((EVERY, m.kr, LANES), F32), pltpu.VMEM((sh, LANES), F32), pltpu.VMEM((sh, LANES), F32),
                        pltpu.VMEM((SUB, LANES), F32), pltpu.VMEM((EVERY, SUB, LANES), F32),
                        pltpu.VMEM((SUB, sh), F32), pltpu.VMEM((SUB, m.k), F32), pltpu.VMEM((sh, LANES), F32), pltpu.VMEM((sh, LANES), F32),
                        pltpu.VMEM((m.kr, LANES), F32), pltpu.VMEM((m.kr, LANES), F32)]
            scratch += [dma((2, NCH)), dma((2, NCH)), dma((2, NCH)), dma((2, NCH)), dma((2,)), dma((2, EVERY)), dma((2,)), dma((2, EVERY)),
                        dma((2, NCH)), dma((2, NCH)), dma((2, NCH)), dma((2, 4, NCH)), dma((5,))]
        outs = pl.pallas_call(
            lambda *refs: main_kernel(mats, sh, *refs),
            in_specs=in_specs,
            out_specs=out_specs,
            out_shape=out_shape,
            scratch_shapes=scratch,
            compiler_params=pltpu.CompilerParams(has_side_effects=YES, vmem_limit_bytes=ALL_VMEM),
            name='step',
        )(*args)
        first, second, far = outs[0:4], outs[12:16], outs[20:]
        chips = mesh.shape['dp'] // 2

        def swap(v, bit):
            return lax.ppermute(v, 'dp', [(q, q ^ bit) for q in range(2 * chips)])

        over = []
        for e in range(2):
            over.append((swap(far[e], 4), swap(far[2 + e], 2)))
        done = unpack_in(first[0], (*first[1:], *second[1:]), sh)
        *both, small = lax.optimization_barrier((*over[0], *far, done[2]))
        early, far = both[0:2], both[2:]
        across = [swap(v, 1) for v in early]
        hold = early_out(second[0], far, o.cut)
        *last, hold = lax.optimization_barrier((*over[1], hold))
        part, hold = late_out(hold, (*early, *across), (o.cut[0], o.cut[2]), sh)
        across = [swap(v, 1) for v in last]
        new_out, _ = late_out(hold, (*last, *across), (o.cut[1], o.cut[3]), sh, (part,))
        new_in = done[0].reshape(a.k, width).T[None]
        new_out = new_out.reshape(o.k, width)[None]
        mom_in, _, col_in, mom_out, row_out, col_out = done[1:]
        return (new_in, new_out, mom_in[None], mom_out.T[None], small, col_in, col_out, row_out)

    free = None
    rows_tp, cols_tp = P(free, 'tp', free), P(free, free, 'tp')
    on_dp, on_tp, whole = P(free, 'dp'), P(free, 'tp'), P()
    state_in, state_out = P(free, 'dp', 'tp'), P(free, 'tp', 'dp')
    in_specs = (cols_tp, rows_tp, P('dp', free, free, 'tp'), P('dp', free, 'tp', free), state_in, state_out, on_dp, on_tp, on_tp, on_dp, whole, whole, whole)
    out_specs = (cols_tp, rows_tp, state_in, state_out, on_dp, on_tp, on_tp, on_dp)
    return jax.shard_map(body, mesh=mesh, in_specs=in_specs, out_specs=out_specs, check_vma=NO)
```

```python
import jax
import jax.numpy as jnp
from jax import lax
from jax.experimental import pallas as pl
from jax.experimental.pallas import tpu as pltpu
from jax.sharding import PartitionSpec as P


F32 = jnp.float32
LANES = 128
SUB = 8
DP = 8
EVERY = 16
ALL_VMEM = 67043328
BESIDE_HOLD = 45500000
YES, NO = True, False
BF16 = jnp.bfloat16
MESH = pl.DeviceIdType.MESH
NCH = 8
WINDOW = 384
ORDER = (0, 4, 1, 5, 2, 6, 3, 7)


def chunk_rows(rows, small_last):
    tiles = rows // SUB
    out, start = [], 0
    for part in ((tiles + 1) // 2, tiles // 2):
        sizes = [part // 10, part // 2 - part // 10, part // 4 + 1] if small_last else [part // 20, part * 9 // 40, part * 3 // 8]
        sizes.append(part - sum(sizes))
        for n in sizes[::-1] if small_last and out else sizes:
            out.append((SUB * start, SUB * n))
            start += n
    return out


def lane_chunks(total):
    width = SUB * LANES
    out = [(s, width) for s in range(0, total - width, width)]
    last = len(out) * width
    if total - last < width // 4:
        s, n = out.pop()
        return out + [(s, n + total - last)]
    return out + [(last, total - last)]


class Mat:
    def __init__(self, kloc, width, tp, row_is_r):
        self.k, self.width, self.sh = kloc, width, width // DP
        self.r = kloc // DP
        self.ktot = kloc * tp
        self.row_is_r = row_is_r
        self.ch = chunk_rows(self.r, not row_is_r)
        self.tiles = (kloc + 127) // LANES
        self.kr = (self.tiles + SUB) // SUB * SUB
        self.nmax = max(n for _, n in self.ch)
        self.cut = [self.ch[i][0] for i in range(0, NCH, 2)] + [self.r]
        self.keep = not row_is_r


def rcopy(src, dst, sems, dev):
    if sems[0].shape:
        ref, *at = sems
        sems = ref.at[(0, *at)], ref.at[(1, *at)]
    return pltpu.make_async_remote_copy(src_ref=src, dst_ref=dst, send_sem=sems[0], recv_sem=sems[1], device_id=dev, device_id_type=MESH)


def places():
    dp = lax.axis_index('dp')
    c, chip = lax.rem(dp, 2), lax.div(dp, 2)
    x, y = lax.rem(chip, 2), lax.div(chip, 2)
    return dp, c, chip, chip + 1 - 2 * x, chip + 2 - 4 * y, 3 - chip


def main_kernel(mats, sh, *refs):
    it = iter(refs)
    lr_ref, wd_ref, b2_ref = next(it), next(it), next(it)
    for m in mats:
        m.g, m.w, m.mom, m.row_arg, m.col_arg = (next(it) for _ in range(5))
    for m in mats:
        (m.ag, m.mom_new, m.row_out, m.col_out, m.d2d, m.xy1, m.x2, m.y2, *m.far) = (next(it) for _ in range(12))
    stage, wst, usq, ucol = next(it), next(it), next(it), next(it)
    ld_sem, w_sem = next(it), next(it)
    for m in mats:
        (m.p, m.gt, m.gn, m.mv, m.colacc, m.msg, m.slots, m.rp, m.rz, m.sc, m.slots2, m.row_raw, m.col_raw, m.row_old, m.row_new, m.col_old, m.col_new) = (next(it) for _ in range(17))
        (m.d2d_s, m.rs1_s, m.x2_s, m.y2_s, m.ex_s, m.msg_s, m.z_s, m.sc_s, m.agx_s, m.agy_s, m.agd_s, m.ags_s, m.loc_s) = (next(it) for _ in range(13))
    tp = lax.axis_index('tp')
    dp, c, chip, jx, jy, jd = places()
    qx, qy, qd, qs = 2 * jx + c, 2 * jy + c, 2 * jd + c, dp + 1 - 2 * c
    sib, xn, yn = {'tp': tp, 'dp': qs}, {'tp': tp, 'dp': qx}, {'tp': tp, 'dp': qy}
    zn = {'tp': 1 - tp, 'dp': dp}
    me16 = tp * DP + dp

    sends = []

    def start(cp):
        cp.start()
        sends.append(cp)

    def direct(m, i):
        return m is mats[0] and i % 4 == 0

    def d2d_copy(m, i):
        r0, n = m.ch[i]
        dst = stage.at[i // 4, 1, :, pl.ds(0, n), :] if direct(m, i) else m.d2d.at[:, pl.ds(r0, n), :]
        return rcopy(m.g.at[pl.ds(4 * (1 - c), 4), pl.ds(r0, n), :], dst, (m.d2d_s, i), sib)

    def own_load(m, i, b):
        r0, n = m.ch[i]
        return pltpu.make_async_copy(m.g.at[pl.ds(4 * c, 4), pl.ds(r0, n), :], stage.at[b, 0, :, pl.ds(0, n), :], ld_sem.at[b, 0])

    def got_load(m, i, b):
        r0, n = m.ch[i]
        return pltpu.make_async_copy(m.d2d.at[:, pl.ds(r0, n), :], stage.at[b, 1, :, pl.ds(0, n), :], ld_sem.at[b, 1])

    def pack_chunk(m, i, b):
        r0, n = m.ch[i]
        own_load(m, i, b).wait()
        if not direct(m, i):
            got_load(m, i, b).wait()

        def body(t, carry):
            rs = pl.multiple_of(t * SUB, SUB)
            rd = pl.multiple_of(r0 + t * SUB, SUB)
            xs = [stage[b, 0, k, pl.ds(rs, SUB), :] + stage[b, 1, k, pl.ds(rs, SUB), :] for k in range(4)]
            for j in range(4):
                parts = [xs[k][:, sh * (2 * j + cc):sh * (2 * j + cc + 1)] for cc in range(2) for k in range(4)]
                m.p[j, pl.ds(rd, SUB), :] = jnp.concatenate(parts, axis=1)
            return carry

        lax.fori_loop(0, n // SUB, body, 0)

    def pview(m, j, i):
        r0, n = m.ch[i]
        return m.p.at[j, pl.ds(r0, n), :]

    def hview(ref, m, i):
        r0, n = m.ch[i]
        return ref.at[pl.ds(r0, n), :]

    def rs1_copy(m, i):
        dev = xn if i < 4 else yn
        return rcopy(pview(m, jd, i), hview(m.xy1, m, i), (m.rs1_s, i), dev)

    def x2_copy(m, i):
        return rcopy(pview(m, jx, i), hview(m.x2, m, i), (m.x2_s, i), xn)

    def y2_copy(m, i):
        return rcopy(pview(m, jy, i), hview(m.y2, m, i), (m.y2_s, i), yn)

    def rs_free(m, i):
        start(x2_copy(m, i) if i < 4 else y2_copy(m, i))

    def rs_pack(m, send):
        own_load(m, ORDER[0], 0).start()
        for s, i in enumerate(ORDER):
            d2d_copy(m, i).wait_recv()
            if not direct(m, i):
                got_load(m, i, s % 2).start()
            if s + 1 < NCH:
                own_load(m, ORDER[s + 1], (s + 1) % 2).start()
            pack_chunk(m, i, s % 2)
            if send:
                start(rs1_copy(m, i))
                if s < 4:
                    rs_free(m, i)

    def rs_dep(m, ids):
        def load(s):
            i = ids[s]
            _, n = m.ch[i]
            return pltpu.make_async_copy(hview(m.xy1, m, i), stage.at[s % 2, 0, 0, pl.ds(0, n), :], ld_sem.at[s % 2, 0])

        for s, i in enumerate(ids):
            r0, n = m.ch[i]
            rs1_copy(m, i).wait_recv()
            load(s).start()
            load(s).wait()
            j = jy if i < 4 else jx

            def body(t, carry):
                rs = pl.multiple_of(t * SUB, SUB)
                rd = pl.multiple_of(r0 + t * SUB, SUB)
                m.p[j, pl.ds(rd, SUB), :] = m.p[j, pl.ds(rd, SUB), :] + stage[s % 2, 0, 0, pl.ds(rs, SUB), :]
                return carry

            lax.fori_loop(0, n // SUB, body, 0)
            start(y2_copy(m, i) if i < 4 else x2_copy(m, i))

    def acc_own(m, ids):
        base = (2 * c * (4 * m.r), (2 - c) * (4 * m.r))

        def loads(s):
            i = ids[s]
            _, n = m.ch[i]
            b = s % 2
            return (pltpu.make_async_copy(hview(m.x2, m, i), stage.at[b, 0, 0, pl.ds(0, n), :], ld_sem.at[b, 0]),
                    pltpu.make_async_copy(hview(m.y2, m, i), stage.at[b, 0, 1, pl.ds(0, n), :], ld_sem.at[b, 1]))

        for s, i in enumerate(ids):
            r0, n = m.ch[i]
            b = s % 2
            x2_copy(m, i).wait_recv()
            y2_copy(m, i).wait_recv()
            la, lb = loads(s)
            la.start()
            lb.start()
            la.wait()
            lb.wait()

            def body(t, carry):
                rs = pl.multiple_of(t * SUB, SUB)
                rd = pl.multiple_of(r0 + t * SUB, SUB)
                v = m.p[chip, pl.ds(rd, SUB), :] + stage[b, 0, 0, pl.ds(rs, SUB), :] + stage[b, 0, 1, pl.ds(rs, SUB), :]
                for cc in range(2):
                    for k in range(4):
                        row = pl.multiple_of(base[cc] + k * m.r + r0 + t * SUB, SUB)
                        m.gt[pl.ds(row, SUB), 0:sh] = v[:, sh * (4 * cc + k):sh * (4 * cc + k + 1)]
                return carry

            lax.fori_loop(0, n // SUB, body, 0)

    def ex_copy(m):
        h = 4 * m.r
        return rcopy(m.gt.at[pl.ds(2 * h, h), :], m.gt.at[pl.ds(c * h, h), :], (m.ex_s,), sib)

    def ex_wait(m):
        h = 4 * m.r
        rcopy(m.gt.at[pl.ds(2 * h, h), :], m.gt.at[pl.ds((1 - c) * h, h), :], (m.ex_s,), sib).wait_recv()

    def to_gn(m):
        full = m.k // LANES

        def body(t, carry):
            o = pl.multiple_of(t * LANES, LANES)
            m.gn[:, pl.ds(o, LANES)] = m.gt[pl.ds(o, LANES), :].T[0:sh, :]
            return carry

        lax.fori_loop(0, full, body, 0)
        rest = m.k - full * LANES
        if rest:
            m.gn[:, full * LANES:m.k] = m.gt[full * LANES:full * LANES + LANES, :].T[0:sh, 0:rest]

    def from_gn(m):
        full = m.k // LANES
        pad = m.gt.shape[1] - sh

        def turn(v):
            return jnp.concatenate([v, jnp.zeros((pad, LANES), F32)], axis=0).T

        def body(t, carry):
            o = pl.multiple_of(t * LANES, LANES)
            m.gt[pl.ds(o, LANES), :] = turn(m.gn[:, pl.ds(o, LANES)])
            return carry

        lax.fori_loop(0, full, body, 0)
        rest = m.k - full * LANES
        if rest:
            v = jnp.concatenate([m.gn[:, full * LANES:m.k], jnp.zeros((sh, LANES - rest), F32)], axis=1)
            m.gt[full * LANES:m.k, :] = turn(v)[0:rest, :]

    def vec_loads(m):
        return (pltpu.make_async_copy(m.row_arg, m.row_raw.at[pl.ds(0, 1), :], m.loc_s.at[3]),
                pltpu.make_async_copy(m.col_arg, m.col_raw.at[pl.ds(0, 1), :], m.loc_s.at[4]))

    def vec_stores(m):
        return (pltpu.make_async_copy(m.row_raw.at[pl.ds(0, 1), :], m.row_out, m.loc_s.at[3]),
                pltpu.make_async_copy(m.col_raw.at[pl.ds(0, 1), :], m.col_out, m.loc_s.at[4]))

    def vec_prepare(m):
        for cp in vec_loads(m):
            cp.wait()
        pad = m.gt.shape[1] - sh
        row = jnp.concatenate([m.row_raw[0:1, :], jnp.zeros((1, pad), F32)], axis=1)
        m.row_old[...] = jnp.broadcast_to(row, (LANES, sh + pad)).T[0:sh, :]
        m.col_old[...] = jnp.zeros_like(m.col_old)
        for t in range(m.tiles):
            w = min(LANES, m.k - LANES * t)
            m.col_old[t:t + 1, 0:w] = m.col_raw[0:1, LANES * t:LANES * t + w]

    def vec_finish(m):
        pad = m.gt.shape[1] - sh
        m.row_raw[...] = jnp.concatenate([m.row_new[...], jnp.zeros((pad, LANES), F32)], axis=0).T[0:SUB, 0:sh]
        for t in range(m.tiles):
            w = min(LANES, m.k - LANES * t)
            m.col_raw[0:1, LANES * t:LANES * t + w] = m.col_new[t:t + 1, 0:w]
        for cp in vec_stores(m):
            cp.start()

    def peers():
        out = []
        for d in range(1, DP):
            q = lax.rem(dp + d, DP)
            out.append((YES, tp, q))
        for d in range(DP):
            q = lax.rem(dp + d, DP)
            out.append((NO, 1 - tp, q))
        return out

    def msg_copies(m, sending):
        out = []
        for n, (same, t, q) in enumerate(peers()):
            slot = me16 if sending else t * SUB + q
            dev = {'tp': t, 'dp': q}
            sems = m.msg_s.at[0, n], m.msg_s.at[1, slot]
            rows = pl.ds(0, m.tiles + 1) if same else pl.ds(m.tiles, 1)
            out.append(rcopy(m.msg.at[rows, :], m.slots.at[slot, rows, :], sems, dev))
        return out

    def z_copy(m):
        return rcopy(m.rp, m.rz, (m.z_s,), zn)

    def sc_copies(m, sending):
        out = []
        for n, (same, t, q) in enumerate(peers()):
            slot = me16 if sending else t * SUB + q
            out.append(rcopy(m.sc.at[pl.ds(0, 1), :], m.slots2.at[slot, pl.ds(0, 1), :], (m.sc_s.at[0, n], m.sc_s.at[1, slot]), {'tp': t, 'dp': q}))
        return out

    def stats1(m):
        b2 = b2_ref[0]
        m.colacc[...] = jnp.zeros_like(m.colacc)

        def body(t, carry):
            rr = pl.multiple_of(t * SUB, SUB)
            rsum = jnp.zeros((DP, 1), F32)
            for s0, w in lane_chunks(m.k):
                g = m.gn[pl.ds(rr, SUB), s0:s0 + w]
                sq = g * g + 1e-30
                m.colacc[:, s0:s0 + w] = m.colacc[:, s0:s0 + w] + sq
                rsum = rsum + jnp.sum(sq, axis=1, keepdims=YES)
            m.rp[pl.ds(rr, SUB), :] = jnp.broadcast_to(rsum, (SUB, LANES))
            return carry

        lax.fori_loop(0, sh // SUB, body, 0)
        for i in range(m.tiles):
            w = min(LANES, m.k - LANES * i)
            m.msg[i:i + 1, 0:w] = jnp.sum(m.colacc[:, LANES * i:LANES * i + w], axis=0, keepdims=YES)
        mean_s = jnp.sum(m.rp[...] * (1.0 / m.ktot), axis=0, keepdims=YES) * (1.0 / m.width)
        if m.row_is_r:
            old = jnp.sum(m.row_old[...], axis=0, keepdims=YES) * (0.5 / m.width)
        else:
            old = jnp.sum(jnp.sum(m.col_old[...], axis=0, keepdims=YES), axis=1, keepdims=YES) * (0.125 / m.ktot)
        m.msg[m.tiles:m.tiles + 1, :] = jnp.broadcast_to(b2 * old + (1.0 - b2) * mean_s, (1, LANES))
        m.slots[me16, :, :] = m.msg[...]
        for cp in msg_copies(m, YES):
            start(cp)
        start(z_copy(m))

    def stats2(m):
        b2 = b2_ref[0]
        for cp in msg_copies(m, NO):
            cp.wait_recv()
        z_copy(m).wait_recv()
        tot = m.slots[tp * DP, 0:m.kr, :]
        for q in range(1, DP):
            tot = tot + m.slots[tp * DP + q, 0:m.kr, :]
        m.col_new[...] = b2 * m.col_old[...] + (1.0 - b2) * (tot / float(m.width))
        m.row_new[...] = b2 * m.row_old[...] + (1.0 - b2) * ((m.rp[...] + m.rz[...]) / float(m.ktot))
        mean_r = m.slots[0, m.tiles:m.tiles + 1, :]
        for q in range(1, EVERY):
            mean_r = mean_r + m.slots[q, m.tiles:m.tiles + 1, :]
        mean_r = mean_r[:, 0:1]
        usq[...] = jnp.zeros_like(usq)
        ucol[...] = jnp.zeros_like(ucol)

        def body(t, carry):
            rr = pl.multiple_of(t * SUB, SUB)
            rv = m.row_new[pl.ds(rr, SUB), 0:1]
            acc = jnp.zeros((DP, 1), F32)
            for i in range(m.tiles):
                s0, w = LANES * i, min(LANES, m.k - LANES * i)
                second = rv * m.col_new[i:i + 1, 0:w] / mean_r
                u = m.gn[pl.ds(rr, SUB), s0:s0 + w] / jnp.sqrt(second)
                m.gn[pl.ds(rr, SUB), s0:s0 + w] = u
                if w == LANES:
                    usq[...] = usq[...] + u * u
                else:
                    acc = acc + jnp.sum(u * u, axis=1, keepdims=YES)
            ucol[...] = ucol[...] + jnp.broadcast_to(acc, (SUB, LANES))
            return carry

        lax.fori_loop(0, sh // SUB, body, 0)
        usum = jnp.sum(jnp.sum(usq[...], axis=1, keepdims=YES), axis=0, keepdims=YES)
        usum = usum + jnp.sum(ucol[:, 0:1], axis=0, keepdims=YES)
        m.sc[...] = jnp.broadcast_to(usum, (SUB, LANES))
        m.slots2[me16, :, :] = m.sc[...]
        for cp in sc_copies(m, YES):
            start(cp)

    def stats2_end(m):
        for cp in sc_copies(m, NO):
            cp.wait_recv()

    def stats3(m):
        tot = m.slots2[0, 0:1, :]
        for q in range(1, EVERY):
            tot = tot + m.slots2[q, 0:1, :]
        den = jnp.maximum(1.0, jnp.sqrt(tot / (float(m.width) * float(m.ktot))))[0:1, 0:1]
        mom_load(m).wait()

        def body(t, carry):
            rr = pl.multiple_of(t * 16, 16)
            for s0, w in lane_chunks(m.k):
                u = m.gn[pl.ds(rr, 16), s0:s0 + w] / den
                mn = (0.9 * m.mv[pl.ds(rr, 16), s0:s0 + w].astype(F32) + 0.1 * u).astype(BF16)
                m.mv[pl.ds(rr, 16), s0:s0 + w] = mn
                m.gn[pl.ds(rr, 16), s0:s0 + w] = mn.astype(F32)
            return carry

        lax.fori_loop(0, sh // 16, body, 0)
        mom_store(m).start()
        from_gn(m)

    def mom_load(m):
        return pltpu.make_async_copy(m.mom, m.mv, m.loc_s.at[0])

    def mom_store(m):
        return pltpu.make_async_copy(m.mv, m.mom_new, m.loc_s.at[1])

    def own_copy(m):
        return pltpu.make_async_copy(m.p.at[chip], m.ag.at[dp], m.loc_s.at[2])

    lane0 = jnp.minimum(lax.div(sh * dp, LANES), DP)
    off = sh * dp - lane0 * LANES

    def w_load(m, i, b):
        r0, n = m.ch[i]
        return pltpu.make_async_copy(m.w.at[:, pl.ds(r0, n), pl.ds(pl.multiple_of(lane0 * LANES, LANES), WINDOW)], wst.at[b, :, pl.ds(0, n), :], w_sem.at[b])

    def new_weights(m, sent):
        lr, wd = lr_ref[0], wd_ref[0]
        w_load(m, 0, 0).start()
        for i in range(NCH):
            r0, n = m.ch[i]
            b = i % 2
            if i + 1 < NCH:
                w_load(m, i + 1, 1 - b).start()
            w_load(m, i, b).wait()

            def body(t, carry):
                rs = pl.multiple_of(t * SUB, SUB)
                rd = pl.multiple_of(r0 + t * SUB, SUB)
                heads, tails = [], []
                for k in range(DP):
                    w = pltpu.roll(wst[b, k, pl.ds(rs, SUB), :], lax.rem(WINDOW - off, WINDOW), 1)[:, 0:sh]
                    mt = m.gt[pl.ds(pl.multiple_of(k * m.r + r0 + t * SUB, SUB), DP), 0:sh]
                    new = w - lr * mt - lr * wd * w
                    heads.append(pltpu.roll(new[:, 0:LANES], lax.rem(sh * dp, LANES), 1))
                    tails.append(new[:, LANES:sh])
                m.p[chip, pl.ds(rd, SUB), :] = jnp.concatenate(heads + tails, axis=1)
                return carry

            lax.fori_loop(0, n // SUB, body, 0)
            if i < sent:
                ag_own(m, i)

    def agrow(m, q, i):
        r0, n = m.ch[i]
        return m.ag.at[q, pl.ds(r0, n), :]

    def kept(m, i):
        r0, n = m.ch[i]
        return m.far[i // 2].at[pl.ds(r0 - m.cut[i // 2], n), :]

    def xrow(m, q, i):
        return kept(m, i) if m.keep and i < 4 else agrow(m, q, i)

    def yrow(m, q, i):
        return kept(m, i) if m.keep and i >= 4 else agrow(m, q, i)

    def ag_own(m, i):
        start(rcopy(pview(m, chip, i), xrow(m, dp, i), (m.agx_s, i), xn))
        start(rcopy(pview(m, chip, i), yrow(m, dp, i), (m.agy_s, i), yn))

    def ag_sib_own(m, i):
        start(rcopy(pview(m, chip, i), agrow(m, dp, i), (m.ags_s, 0, i), sib))

    def ag_sib(m, which, src, q, i):
        start(rcopy(src, agrow(m, q, i), (m.ags_s, which, i), sib))

    def ag_xy(m, i):
        fx, fy = xrow(m, qx, i), yrow(m, qy, i)
        rcopy(fx, fx, (m.agx_s, i), xn).wait_recv()
        rcopy(fy, fy, (m.agy_s, i), yn).wait_recv()
        if not m.keep:
            if i < 4:
                start(rcopy(fx, fx, (m.agd_s, i), yn))
            else:
                start(rcopy(fy, fy, (m.agd_s, i), xn))
        ag_sib(m, 1, fx, qx, i)
        ag_sib(m, 2, fy, qy, i)

    def ag_d(m, i):
        rcopy(agrow(m, qd, i), agrow(m, qd, i), (m.agd_s, i), xn).wait_recv()
        ag_sib(m, 3, agrow(m, qd, i), qd, i)

    def ag_end(m):
        blocks = (qs, qx + 1 - 2 * c, qy + 1 - 2 * c, qd + 1 - 2 * c)
        for which, q in enumerate(blocks[0:3] if m.keep else blocks):
            for i in range(NCH):
                rcopy(agrow(m, q, i), agrow(m, q, i), (m.ags_s, which, i), sib).wait_recv()

    a, o = mats
    barrier = pltpu.get_barrier_semaphore()
    for _, t, q in peers():
        pl.semaphore_signal(barrier, inc=1, device_id={'tp': t, 'dp': q}, device_id_type=MESH)
    pl.semaphore_wait(barrier, EVERY - 1)
    for i in ORDER:
        start(d2d_copy(a, i))
    rs_pack(a, YES)
    for i in ORDER[4:]:
        rs_free(a, i)
    for i in ORDER:
        start(d2d_copy(o, i))
    for m in mats:
        mom_load(m).start()
        for cp in vec_loads(m):
            cp.start()
    rs_dep(a, ORDER)
    rs_pack(o, NO)
    for m in mats:
        vec_prepare(m)
    for i in ORDER[0:6]:
        start(rs1_copy(o, i))
    acc_own(a, ORDER)
    start(ex_copy(a))
    for i in ORDER[6:]:
        start(rs1_copy(o, i))
    for i in ORDER[0:2]:
        rs_free(o, i)
    ex_wait(a)
    to_gn(a)
    stats1(a)
    for i in ORDER[2:4]:
        rs_free(o, i)
    stats2(a)
    for i in ORDER[4:6]:
        rs_free(o, i)
    stats2_end(a)
    for i in ORDER[6:]:
        rs_free(o, i)
    rs_dep(o, ORDER)
    stats3(a)
    new_weights(a, 3)
    vec_finish(a)
    own_copy(a).start()
    for i in range(NCH):
        ag_sib_own(a, i)
    acc_own(o, ORDER)
    start(ex_copy(o))
    ex_wait(o)
    to_gn(o)
    stats1(o)
    for i in range(3, 5):
        ag_own(a, i)
    stats2(o)
    ag_own(a, 5)
    stats2_end(o)
    for i in range(6, NCH):
        ag_own(a, i)
    stats3(o)
    new_weights(o, 0)
    vec_finish(o)
    own_copy(o).start()
    for i in range(NCH):
        ag_sib_own(o, i)
    for i in range(NCH):
        ag_xy(a, i)
    for i in range(NCH):
        ag_own(o, i)
    for i in range(NCH):
        ag_d(a, i)
    for i in range(NCH):
        ag_xy(o, i)
    for m in mats:
        ag_end(m)
        own_copy(m).wait()
        mom_store(m).wait()
        for cp in vec_stores(m):
            cp.wait()
    for cp in sends:
        cp.wait_send()


def split_rows(rows, parts):
    tiles = rows // SUB
    inner = tiles - 4
    out, start = [], 0
    for n in [2] + [inner // parts + (1 if i < inner % parts else 0) for i in range(parts)] + [2]:
        out.append((SUB * start, SUB * n))
        start += n
    return out


def turn_rows(sh, src, dst, row, rows):
    extra = sh - LANES
    tiles = DP * sh // LANES

    def tile(t):
        return pl.ds(LANES * t, LANES)

    def body(t, carry):
        lane = lax.broadcasted_iota(jnp.int32, (SUB, LANES), 1)
        rs = pl.ds(pl.multiple_of(row + t * SUB, SUB), SUB)
        rd = pl.ds(pl.multiple_of(t * SUB, SUB), SUB)
        ends = [[src[q, rs, tile(e)] for e in range(DP, tiles)] for q in range(DP)]
        for k in range(DP):
            out = [None] * tiles

            def place(v, lo, hi):
                for e in range(lo // LANES, (hi - 1) // LANES + 1):
                    at = max(lo - LANES * e, 0)
                    out[e] = v if out[e] is None else jnp.where(lane >= at, v, out[e])

            first, last = extra * k // LANES, (extra * (k + 1) - 1) // LANES
            for q in range(DP):
                place(src[q, rs, tile(k)], sh * q, sh * q + LANES)
                v = ends[q][first]
                if last > first:
                    v = jnp.where(lane >= extra * k % LANES, v, ends[q][last])
                turn = extra * (q - k) % LANES
                if turn:
                    v = pltpu.roll(v, turn, 1)
                place(v, sh * q + LANES, sh * (q + 1))
            for e in range(tiles):
                dst[k, rd, tile(e)] = out[e]
        return carry

    lax.fori_loop(0, rows // SUB, body, 0)


def unpack_in_kernel(sh, work, count, src, *refs):
    small, dst, small_out = refs[0:count], refs[count], refs[count + 1:2 * count + 1]
    src_v, dst_v, in_sem, out_sem, small_sem, *small_v = refs[2 * count + 1:]
    ins, outs = src_v.shape[0], dst_v.shape[0]

    def load(s):
        r0, n = work[s]
        return pltpu.make_async_copy(src.at[:, pl.ds(r0, n), :], src_v.at[s % ins, :, pl.ds(0, n), :], in_sem.at[s % ins])

    def store(s):
        r0, n = work[s]
        return pltpu.make_async_copy(dst_v.at[s % outs, :, pl.ds(0, n), :], dst.at[:, pl.ds(r0, n), :], out_sem.at[s % outs])

    def small_in(k):
        return pltpu.make_async_copy(small[k], small_v[k], small_sem.at[0, k])

    def small_back(k):
        return pltpu.make_async_copy(small_v[k], small_out[k], small_sem.at[1, k])

    for s in range(ins - 1):
        load(s).start()
    for k in range(count):
        small_in(k).start()
    for s, (r0, n) in enumerate(work):
        if s + ins - 1 < len(work):
            load(s + ins - 1).start()
        load(s).wait()
        if s >= outs:
            store(s - outs).wait()
        turn_rows(sh, src_v.at[s % ins], dst_v.at[s % outs], 0, n)
        store(s).start()
        if s == ins:
            for k in range(count):
                small_in(k).wait()
                small_back(k).start()
    for s in range(len(work) - outs, len(work)):
        store(s).wait()
    for k in range(count):
        small_back(k).wait()


def early_kernel(cut, ag, *refs):
    far, hold, sem = refs[0:4], refs[4], refs[5]
    dp, c, chip, *chips = places()
    qx, qy, _ = (2 * j + c for j in chips)
    other = 1 - 2 * c
    rows = [pl.ds(lo, hi - lo) for lo, hi in zip(cut, cut[1:])]
    copies = [(ag.at[q], hold.at[q]) for q in (dp, dp + other, qx + other, qy + other)]
    for e, part in enumerate(rows):
        for q, near in ((qx, e >= 2), (qy, e < 2)):
            copies.append((ag.at[q, part, :] if near else far[e], hold.at[q, part, :]))
    copies = [pltpu.make_async_copy(v, w, sem.at[e]) for e, (v, w) in enumerate(copies)]
    for cp in copies:
        cp.start()
    for cp in copies:
        cp.wait()


def late_kernel(sh, work, firsts, *refs):
    late, (dst, hold, dst_v, in_sem, out_sem) = refs[1:5], refs[-5:]
    *_, c, _, _, _, jd = places()
    outs = dst_v.shape[0]

    def loads(s):
        r0, n = work[s]
        half = int(r0 >= firsts[1])
        blocks = 2 * jd + c, 2 * jd + 1 - c
        part = pl.ds(r0 - firsts[half], n)
        return [pltpu.make_async_copy(late[2 * e + half].at[part, :], hold.at[q, pl.ds(r0, n), :], in_sem.at[s, e]) for e, q in enumerate(blocks)]

    def store(s):
        r0, n = work[s]
        return pltpu.make_async_copy(dst_v.at[s % outs, :, pl.ds(0, n), :], dst.at[:, pl.ds(r0, n), :], out_sem.at[s % outs])

    for s in range(len(work)):
        for cp in loads(s):
            cp.start()
    for s, (r0, n) in enumerate(work):
        for cp in loads(s):
            cp.wait()
        if s >= outs:
            store(s - outs).wait()
        turn_rows(sh, hold, dst_v.at[s % outs], r0, n)
        store(s).start()
    for s in range(len(work) - outs, len(work)):
        store(s).wait()


IN_HBM = pl.BlockSpec(memory_space=pl.ANY)
IN_VMEM = pl.BlockSpec(memory_space=pltpu.VMEM)


def costing(size):
    return pl.CostEstimate(flops=1000 * size, bytes_accessed=DP * size, transcendentals=0)


def unpack_in(packed, small, sh):
    work = split_rows(packed.shape[1], 13)
    nmax = max(n for _, n in work)
    count = len(small)
    dma = pltpu.SemaphoreType.DMA
    buf = (DP, nmax, packed.shape[2])
    return pl.pallas_call(
        lambda *refs: unpack_in_kernel(sh, work, count, *refs),
        in_specs=[IN_HBM] * (1 + count),
        out_specs=[IN_HBM] * (1 + count),
        out_shape=[jax.ShapeDtypeStruct(v.shape, v.dtype) for v in (packed, *small)],
        scratch_shapes=[pltpu.VMEM((6, *buf), F32), pltpu.VMEM((5, *buf), F32), dma((6,)), dma((5,)), dma((2, count))]
        + [pltpu.VMEM(v.shape, v.dtype) for v in small],
        compiler_params=pltpu.CompilerParams(vmem_limit_bytes=ALL_VMEM),
        cost_estimate=costing(packed.size),
        name='unpack_in',
    )(packed, *small)


def early_out(ag, far, cut):
    return pl.pallas_call(
        lambda *refs: early_kernel(cut, *refs),
        in_specs=[IN_HBM] * (1 + len(far)),
        out_specs=IN_VMEM,
        out_shape=pltpu.VMEM(ag.shape, F32),
        scratch_shapes=[pltpu.SemaphoreType.DMA((12,))],
        compiler_params=pltpu.CompilerParams(vmem_limit_bytes=BESIDE_HOLD),
        cost_estimate=costing(ag.size),
        name='early_out',
    )(ag, *far)


def late_out(hold, late, firsts, sh, before=()):
    shape = hold.shape
    work = [(lo + r0, n) for lo, v in zip(firsts, late) for r0, n in split_rows(v.shape[0], 2)]
    nmax = max(n for _, n in work)
    dma = pltpu.SemaphoreType.DMA
    aliases = {0: 1, 5: 0} if before else {0: 1}
    return pl.pallas_call(
        lambda *refs: late_kernel(sh, work, firsts, *refs),
        in_specs=[IN_VMEM] + [IN_HBM] * (len(late) + len(before)),
        out_specs=[IN_HBM, IN_VMEM],
        out_shape=[jax.ShapeDtypeStruct(shape, F32), pltpu.VMEM(shape, F32)],
        input_output_aliases=aliases,
        scratch_shapes=[pltpu.VMEM((4, DP, nmax, shape[2]), F32), dma((len(work), 2)), dma((4,))],
        compiler_params=pltpu.CompilerParams(vmem_limit_bytes=BESIDE_HOLD),
        cost_estimate=costing(hold.size),
    )(hold, *late, *before)


def solution(mesh):
    tp_devs = mesh.shape['tp']

    def body(w_in, w_out, g_in, g_out, m_in, m_out, r_in, c_in, r_out, c_out, learn_rate, weight_decay, beta_two):
        width = w_in.shape[1]
        sh = width // DP
        mats = (Mat(w_in.shape[2], width, tp_devs, YES), Mat(w_out.shape[1], width, tp_devs, NO))
        a, o = mats

        def grouped(v, m):
            return v.reshape(DP, m.r, width)

        scal = [v.reshape(1) for v in (learn_rate, weight_decay, beta_two)]
        args = list(scal)
        args += [grouped(g_in[0, 0].T, a), grouped(w_in[0].T, a), m_in[0], r_in, c_in]
        args += [grouped(g_out[0, 0], o), grouped(w_out[0], o), m_out[0].T, c_out, r_out]
        sspec = pl.BlockSpec(memory_space=pltpu.SMEM)
        in_specs = [sspec] * 3 + [IN_HBM] * 10
        out_shape, out_specs = [], []
        for m in mats:
            big = jax.ShapeDtypeStruct((m.r, width), F32)
            out_shape += [jax.ShapeDtypeStruct((DP, m.r, width), F32), jax.ShapeDtypeStruct((sh, m.k), BF16),
                          jax.ShapeDtypeStruct((1, sh), F32), jax.ShapeDtypeStruct((1, m.k), F32),
                          jax.ShapeDtypeStruct((4, m.r, width), F32), big, big, big,
                          *(jax.ShapeDtypeStruct((hi - lo, width), F32) for lo, hi in zip(m.cut, m.cut[1:]))]
            out_specs += [IN_HBM] * 12
        nmax = max(m.nmax for m in mats)
        dma = pltpu.SemaphoreType.DMA
        scratch = [pltpu.VMEM((2, 2, 4, nmax, width), F32), pltpu.VMEM((2, DP, nmax, WINDOW), F32), pltpu.VMEM((SUB, LANES), F32), pltpu.VMEM((SUB, LANES), F32), dma((2, 2)), dma((2,))]
        for m in mats:
            gt_rows = 12 * m.r
            scratch += [pltpu.VMEM((4, m.r, width), F32), pltpu.VMEM((gt_rows, 256), F32), pltpu.VMEM((sh, LANES * m.tiles), F32),
                        pltpu.VMEM((sh, m.k), BF16), pltpu.VMEM((SUB, LANES * m.tiles), F32), pltpu.VMEM((m.kr, LANES), F32),
                        pltpu.VMEM((EVERY, m.kr, LANES), F32), pltpu.VMEM((sh, LANES), F32), pltpu.VMEM((sh, LANES), F32),
                        pltpu.VMEM((SUB, LANES), F32), pltpu.VMEM((EVERY, SUB, LANES), F32),
                        pltpu.VMEM((SUB, sh), F32), pltpu.VMEM((SUB, m.k), F32), pltpu.VMEM((sh, LANES), F32), pltpu.VMEM((sh, LANES), F32),
                        pltpu.VMEM((m.kr, LANES), F32), pltpu.VMEM((m.kr, LANES), F32)]
            scratch += [dma((2, NCH)), dma((2, NCH)), dma((2, NCH)), dma((2, NCH)), dma((2,)), dma((2, EVERY)), dma((2,)), dma((2, EVERY)),
                        dma((2, NCH)), dma((2, NCH)), dma((2, NCH)), dma((2, 4, NCH)), dma((5,))]
        outs = pl.pallas_call(
            lambda *refs: main_kernel(mats, sh, *refs),
            in_specs=in_specs,
            out_specs=out_specs,
            out_shape=out_shape,
            scratch_shapes=scratch,
            compiler_params=pltpu.CompilerParams(has_side_effects=YES, collective_id=0, vmem_limit_bytes=ALL_VMEM),
            name='step',
        )(*args)
        first, second, far = outs[0:4], outs[12:16], outs[20:]
        chips = mesh.shape['dp'] // 2

        def swap(v, bit):
            return lax.ppermute(v, 'dp', [(q, q ^ bit) for q in range(2 * chips)])

        over = []
        for e in range(2):
            over.append((swap(far[e], 4), swap(far[2 + e], 2)))
        done = unpack_in(first[0], (*first[1:], *second[1:]), sh)
        *both, small = lax.optimization_barrier((*over[0], *far, done[2]))
        early, far = both[0:2], both[2:]
        across = [swap(v, 1) for v in early]
        hold = early_out(second[0], far, o.cut)
        *last, hold = lax.optimization_barrier((*over[1], hold))
        part, hold = late_out(hold, (*early, *across), (o.cut[0], o.cut[2]), sh)
        across = [swap(v, 1) for v in last]
        new_out, _ = late_out(hold, (*last, *across), (o.cut[1], o.cut[3]), sh, (part,))
        new_in = done[0].reshape(a.k, width).T[None]
        new_out = new_out.reshape(o.k, width)[None]
        mom_in, _, col_in, mom_out, row_out, col_out = done[1:]
        return (new_in, new_out, mom_in[None], mom_out.T[None], small, col_in, col_out, row_out)

    free = None
    rows_tp, cols_tp = P(free, 'tp', free), P(free, free, 'tp')
    on_dp, on_tp, whole = P(free, 'dp'), P(free, 'tp'), P()
    state_in, state_out = P(free, 'dp', 'tp'), P(free, 'tp', 'dp')
    in_specs = (cols_tp, rows_tp, P('dp', free, free, 'tp'), P('dp', free, 'tp', free), state_in, state_out, on_dp, on_tp, on_tp, on_dp, whole, whole, whole)
    out_specs = (cols_tp, rows_tp, state_in, state_out, on_dp, on_tp, on_tp, on_dp)
    return jax.shard_map(body, mesh=mesh, in_specs=in_specs, out_specs=out_specs, check_vma=NO)
```
